32 devices in a mesh: kgrp: 2 (over y), band: 4 (over z), fft: 4 (over x, core).
Axes of the slice: x: 2, y: 2, z: 4, core: 2. Of those that a mesh axis runs over, the one named last changes fastest.
Arguments:
- orbitals: float32 [8, 64, 64, 128], P(('kgrp', 'band'), 'fft'), parts along dimension 0, may hold values from -6 to 6
- partners: float32 [8, 64, 64, 128], P(('kgrp', 'band'), 'fft'), parts along dimension 0, may hold values from -6 to 6
- shift_table: float32 [8, 3], replicated, may hold values from -0.5 to 0.5
- shift_index: int32 [8], P('kgrp'), parts along dimension 0, may hold values from 0 to 7
Outputs:
- potential: float32 [8, 64, 64, 128], P(('kgrp', 'band'), 'fft'), parts along dimension 0
- projector: float32 [8, 64, 64, 128], P(('kgrp', 'band'), 'fft'), parts along dimension 0
The draws below stay inside these ranges and needn't reach their ends.
There are 2 independent parts, one for each index of `kgrp`. The reference program is written for one: setup_inputs(seed, part) draws one part's arguments, and reference() takes and returns one part's arrays. A program takes and returns all parts, laid end to end along the dimension named above; an argument that names none is the same for every part. Nothing has to cross between parts.
All inputs are finite; a program needn't handle non-finite values.
Results may differ from the reference program's by a relative error of at most 0.0001.
Values sent between devices are 32-bit elements; how exact they have to be, the bound alone decides.
A program may use at most 64 MiB of HBM per device.

```python
import math
import jax
import jax.numpy as jnp
from jax import lax

GRID = 64
NQ = 8
BANDS = 4
PARTNERS = 4


def touch_ends(drawn, rng, least, top_value):
    longest = drawn.shape.index(max(drawn.shape))
    spots = []
    for shift in (0, 1):
        where = [jax.random.randint(jax.random.fold_in(rng, axis), (), 0, length) for axis, length in enumerate(drawn.shape)]
        where[longest] = (where[longest] + shift) % drawn.shape[longest]
        spots.append(tuple(where))
    return drawn.at[spots[0]].set(least).at[spots[1]].set(top_value)


def block_levels(stream_key, dims, pieces, low, high):
    loudness = 1.0
    for dim, parts in pieces:
        heights = jax.random.uniform(jax.random.fold_in(jax.random.fold_in(stream_key, 6), dim), (parts,), jnp.float32, low / len(pieces), high / len(pieces))
        loudness = loudness * jnp.repeat(jnp.exp(heights), dims[dim] // parts).reshape((-1,) + (1,) * (len(dims) - 1 - dim))
    return loudness


def noise(stream_key, shape, scale, bound, split=(), kind=jnp.bfloat16):
    result = jax.random.normal(stream_key, shape, jnp.float32) * scale
    if len(split) > 0:
        result = block_levels(stream_key, shape, split, -0.22, 0.18) * result
    return jnp.clip(result, min=-bound, max=bound).astype(kind)


def setup_inputs(seed: int = 0, part: int = 0) -> dict:
    arg_keys = jax.random.split(jax.random.key(seed), 5)
    part_keys = jax.random.split(jax.random.fold_in(arg_keys[4], part), 5)
    orbitals = noise(part_keys[0], (BANDS, GRID, GRID, 2 * GRID), 0.7, 6.0, ((0, 4), (1, 4)), jnp.float32)
    partners = noise(part_keys[1], (PARTNERS, GRID, GRID, 2 * GRID), 0.7, 6.0, ((0, 4), (1, 4)), jnp.float32)
    shift_table = jnp.clip(jax.random.uniform(arg_keys[2], (NQ, 3), jnp.float32, -0.5, 0.5), -0.5, 0.5)
    shift_index = touch_ends(jax.random.randint(part_keys[3], (PARTNERS,), 0, NQ), jax.random.fold_in(part_keys[3], 1), 0, NQ - 1).astype(jnp.int32)
    return {"orbitals": orbitals, "partners": partners, "shift_table": shift_table, "shift_index": shift_index}


HIGHEST = lax.Precision.HIGHEST
SCREEN_SQUARE = 0.25
FOUR_PI = 4.0 * math.pi

def frequency(positions, extent):
    return jnp.where(positions < extent // 2, positions, positions - extent).astype(jnp.float32)

def rotate(field):
    extent = field.shape[-1] // 2
    return jnp.concatenate([field[..., extent:], -field[..., :extent]], axis=-1)

def factor_inverse(over_real, over_imag):
    matrix_order = over_real.shape[0]
    positions = jnp.arange(matrix_order, dtype=jnp.int32)
    zero_start = jnp.zeros_like(over_real)

    def chol_step(column, lowers):
        lower_real, lower_imag = lowers
        row_real = lower_real[column]
        row_imag = lower_imag[column]
        resid_real = over_real[:, column] - (jnp.dot(lower_real, row_real, precision=HIGHEST) + jnp.dot(lower_imag, row_imag, precision=HIGHEST))
        resid_imag = over_imag[:, column] - (jnp.dot(lower_imag, row_real, precision=HIGHEST) - jnp.dot(lower_real, row_imag, precision=HIGHEST))
        pivot_value = jnp.sqrt(resid_real[column])
        below_diag = positions > column
        at_diag = positions == column
        new_real = jnp.where(below_diag, resid_real / pivot_value, jnp.where(at_diag, pivot_value, 0.0))
        new_imag = jnp.where(below_diag, resid_imag / pivot_value, 0.0)
        chosen = positions[None, :] == column
        return (jnp.where(chosen, new_real[:, None], lower_real), jnp.where(chosen, new_imag[:, None], lower_imag))
    lower_real, lower_imag = lax.fori_loop(0, matrix_order, chol_step, (zero_start, zero_start))

    def solve_step(row_index, inverses):
        inv_real, inv_imag = inverses
        row_real = lower_real[row_index]
        row_imag = lower_imag[row_index]
        sum_real = jnp.dot(row_real, inv_real, precision=HIGHEST) - jnp.dot(row_imag, inv_imag, precision=HIGHEST)
        sum_imag = jnp.dot(row_real, inv_imag, precision=HIGHEST) + jnp.dot(row_imag, inv_real, precision=HIGHEST)
        unit_row = (positions == row_index).astype(over_real.dtype)
        pivot_value = lower_real[row_index, row_index]
        new_real = (unit_row - sum_real) / pivot_value
        new_imag = -sum_imag / pivot_value
        chosen = positions[:, None] == row_index
        return (jnp.where(chosen, new_real[None, :], inv_real), jnp.where(chosen, new_imag[None, :], inv_imag))
    return lax.fori_loop(0, matrix_order, solve_step, (zero_start, zero_start))

def reference(orbitals, partners, shift_table, shift_index):
    extent = orbitals.shape[1]
    orbital_field = orbitals[..., :extent] + 1j * orbitals[..., extent:]
    partner_field = partners[..., :extent] + 1j * partners[..., extent:]
    grid_freq = frequency(jnp.arange(extent, dtype=jnp.int32), extent).astype(orbitals.dtype)

    def partner_term(running, member):
        single, chosen_index = member
        qvector = shift_table[chosen_index]
        denominator = (grid_freq[:, None, None] + qvector[0]) ** 2 + (grid_freq[None, :, None] + qvector[1]) ** 2 + (grid_freq[None, None, :] + qvector[2]) ** 2 + SCREEN_SQUARE
        kernel = FOUR_PI / denominator
        density = jnp.conj(single)[None] * orbital_field
        field = jnp.fft.ifftn(jnp.fft.fftn(density, axes=(1, 2, 3)) * kernel[None], axes=(1, 2, 3))
        return (running + single[None] * field, None)
    start_field = jnp.zeros(orbital_field.shape, orbital_field.dtype)
    exchange_field, _ = lax.scan(partner_term, start_field, (partner_field, shift_index))
    potential = jnp.concatenate([exchange_field.real, exchange_field.imag], axis=-1).astype(orbitals.dtype)
    total_bands = potential.shape[0]
    turned = rotate(potential)
    flat_orbitals = orbitals.reshape(total_bands, -1)
    flat_pot = potential.reshape(total_bands, -1)
    flat_turned = turned.reshape(total_bands, -1)
    volume = float(extent ** 3)
    over_real = jnp.einsum('ik,jk->ij', flat_orbitals, flat_pot, precision=HIGHEST) / volume
    over_imag = jnp.einsum('ik,jk->ij', flat_orbitals, flat_turned, precision=HIGHEST) / volume
    inv_real, inv_imag = factor_inverse(over_real, over_imag)
    projector = jnp.dot(inv_real, flat_pot, precision=HIGHEST) + jnp.dot(inv_imag, flat_turned, precision=HIGHEST)
    return (potential, projector.reshape(potential.shape))
```

```python
import functools
import math

import jax
import jax.numpy as jnp
import numpy as np
from jax import lax
from jax.experimental import pallas as pl
from jax.experimental.pallas import tpu as pltpu
from jax.sharding import PartitionSpec as P

HIGHEST = lax.Precision.HIGHEST
HIGH = lax.Precision.HIGH
MESH = pl.DeviceIdType.MESH
GROUP = 8
SCREEN_SQUARE = 0.25
FOUR_PI = 4.0 * math.pi


def angle_pair(extent, sign):
    positions = jnp.arange(extent, dtype=jnp.int32)
    product = positions[:, None] * positions[None, :] % extent
    angle = 2.0 * math.pi / extent * product.astype(jnp.float32)
    return (jnp.cos(angle), sign * jnp.sin(angle))


def last_table(extent, sign):
    cosine, sine = angle_pair(extent, sign)
    upper = jnp.concatenate([cosine, sine], axis=1)
    lower = jnp.concatenate([-sine, cosine], axis=1)
    return jnp.concatenate([upper, lower], axis=0)


def middle_table(extent, sign):
    cosine, sine = angle_pair(extent, sign)
    return jnp.stack([jnp.stack([cosine, -sine], -1), jnp.stack([sine, cosine], -1)], 1)


def along_last(field, table):
    shape = field.shape
    flat = field.reshape(-1, shape[-1])
    return jnp.dot(flat, table, precision=HIGH).reshape(shape)


def along_axis(field, table, axis_number):
    shape = field.shape
    extent = shape[-1] // 2
    split = field.reshape(shape[0], shape[1], shape[2], 2, extent)
    if axis_number == 1:
        result = jnp.einsum("kcnd,pnbdz->pkbcz", table, split, precision=HIGH)
    else:
        result = jnp.einsum("kcnd,pandz->pakcz", table, split, precision=HIGH)
    return result.reshape(shape)


def times_conj(left, right):
    extent = left.shape[-1] // 2
    left_real, left_imag = (left[..., :extent], left[..., extent:])
    right_real, right_imag = (right[..., :extent], right[..., extent:])
    return jnp.concatenate(
        [
            left_real * right_real + left_imag * right_imag,
            left_real * right_imag - left_imag * right_real,
        ],
        axis=-1,
    )


def times(left, right):
    extent = left.shape[-1] // 2
    left_real, left_imag = (left[..., :extent], left[..., extent:])
    right_real, right_imag = (right[..., :extent], right[..., extent:])
    return jnp.concatenate(
        [
            left_real * right_real - left_imag * right_imag,
            left_real * right_imag + left_imag * right_real,
        ],
        axis=-1,
    )


def rotate(field):
    extent = field.shape[-1] // 2
    return jnp.concatenate([field[..., extent:], -field[..., :extent]], axis=-1)


def frequency(positions, extent):
    return jnp.where(positions < extent // 2, positions, positions - extent).astype(jnp.float32)


def kernel_block(qvectors, y_count, extent):
    first_freq = frequency(jnp.arange(extent, dtype=jnp.int32), extent)
    second_freq = frequency(jnp.arange(y_count, dtype=jnp.int32), extent)
    third_freq = frequency(jnp.arange(2 * extent, dtype=jnp.int32) % extent, extent)
    first_part = (first_freq[None, :] + qvectors[:, 0:1]) ** 2
    second_part = (second_freq[None, :] + qvectors[:, 1:2]) ** 2
    third_part = (third_freq[None, :] + qvectors[:, 2:3]) ** 2
    denominator = (
        first_part[:, :, None, None]
        + second_part[:, None, :, None]
        + third_part[:, None, None, :]
        + SCREEN_SQUARE
    )
    return FOUR_PI / extent**3 / denominator


def shifts_for(shift_table, shift_index, start_at, length):
    picked = lax.dynamic_slice_in_dim(shift_index, start_at, length)
    onehot = (picked[:, None] == jnp.arange(shift_table.shape[0], dtype=jnp.int32)[None, :]).astype(
        jnp.float32
    )
    return jnp.dot(onehot, shift_table, precision=HIGHEST)


def factor_inverse(over_real, over_imag):
    matrix_order = over_real.shape[0]
    positions = jnp.arange(matrix_order, dtype=jnp.int32)
    zero_start = jnp.zeros_like(over_real)

    def chol_step(column, lowers):
        lower_real, lower_imag = lowers
        row_real = lower_real[column]
        row_imag = lower_imag[column]
        resid_real = over_real[:, column] - (
            jnp.dot(lower_real, row_real, precision=HIGHEST)
            + jnp.dot(lower_imag, row_imag, precision=HIGHEST)
        )
        resid_imag = over_imag[:, column] - (
            jnp.dot(lower_imag, row_real, precision=HIGHEST)
            - jnp.dot(lower_real, row_imag, precision=HIGHEST)
        )
        pivot_value = jnp.sqrt(resid_real[column])
        below_diag = positions > column
        at_diag = positions == column
        new_real = jnp.where(
            below_diag, resid_real / pivot_value, jnp.where(at_diag, pivot_value, 0.0)
        )
        new_imag = jnp.where(below_diag, resid_imag / pivot_value, 0.0)
        chosen = positions[None, :] == column
        return (
            jnp.where(chosen, new_real[:, None], lower_real),
            jnp.where(chosen, new_imag[:, None], lower_imag),
        )

    lower_real, lower_imag = lax.fori_loop(0, matrix_order, chol_step, (zero_start, zero_start))

    def solve_step(row_index, inverses):
        inv_real, inv_imag = inverses
        row_real = lower_real[row_index]
        row_imag = lower_imag[row_index]
        sum_real = jnp.dot(row_real, inv_real, precision=HIGHEST) - jnp.dot(
            row_imag, inv_imag, precision=HIGHEST
        )
        sum_imag = jnp.dot(row_real, inv_imag, precision=HIGHEST) + jnp.dot(
            row_imag, inv_real, precision=HIGHEST
        )
        unit_row = (positions == row_index).astype(over_real.dtype)
        pivot_value = lower_real[row_index, row_index]
        new_real = (unit_row - sum_real) / pivot_value
        new_imag = -sum_imag / pivot_value
        chosen = positions[:, None] == row_index
        return (
            jnp.where(chosen, new_real[None, :], inv_real),
            jnp.where(chosen, new_imag[None, :], inv_imag),
        )

    return lax.fori_loop(0, matrix_order, solve_step, (zero_start, zero_start))


def general_body(orbitals, partners, shift_table, shift_index):
    extent = orbitals.shape[2]
    band_count = orbitals.shape[0]
    tables = (
        last_table(extent, -1.0),
        middle_table(extent, -1.0),
        last_table(extent, 1.0),
        middle_table(extent, 1.0),
    )
    my_band = lax.axis_index("band")
    forward_last, forward_mid, inverse_last, inverse_mid = tables
    full_orbitals = lax.all_gather(orbitals, "fft", axis=1, tiled=True)
    every_slab = lax.all_gather(partners, "band", axis=0, tiled=True)
    own_grids = lax.all_to_all(every_slab, "fft", split_axis=0, concat_axis=1, tiled=True)
    own_count = own_grids.shape[0]
    qvectors = shifts_for(shift_table, shift_index, lax.axis_index("fft") * own_count, own_count)

    def one_partner(member, running):
        single = lax.dynamic_slice_in_dim(own_grids, member, 1, 0)
        kernel = kernel_block(lax.dynamic_slice_in_dim(qvectors, member, 1, 0), extent, extent)
        density = times_conj(single, full_orbitals)
        spectrum = (
            along_axis(
                along_axis(along_last(density, forward_last), forward_mid, 2), forward_mid, 1
            )
            * kernel
        )
        field = along_last(
            along_axis(along_axis(spectrum, inverse_mid, 1), inverse_mid, 2), inverse_last
        )
        return running + times(single, field)

    partial_value = lax.fori_loop(
        0, own_count, one_partner, jnp.zeros(full_orbitals.shape, jnp.float32)
    )
    potential = lax.psum_scatter(partial_value, "fft", scatter_dimension=1, tiled=True)
    every_pot = lax.all_gather(potential, "band", axis=0, tiled=True)
    turned = rotate(every_pot)
    total_bands = every_pot.shape[0]
    flat_orbitals = orbitals.reshape(band_count, -1)
    flat_pot = every_pot.reshape(total_bands, -1)
    flat_turned = turned.reshape(total_bands, -1)
    volume = float(extent**3)
    rows_real = jnp.einsum("ik,jk->ij", flat_orbitals, flat_pot, precision=HIGHEST) / volume
    rows_imag = jnp.einsum("ik,jk->ij", flat_orbitals, flat_turned, precision=HIGHEST) / volume
    start_row = my_band * band_count
    summed_real, summed_imag = lax.psum((rows_real, rows_imag), "fft")
    over_real, over_imag = (
        lax.all_gather(summed_real, "band", axis=0, tiled=True),
        lax.all_gather(summed_imag, "band", axis=0, tiled=True),
    )
    inv_real, inv_imag = factor_inverse(over_real, over_imag)
    coef_real = lax.dynamic_slice_in_dim(inv_real, start_row, band_count, 0)
    coef_imag = lax.dynamic_slice_in_dim(inv_imag, start_row, band_count, 0)
    projector = jnp.dot(coef_real, flat_pot, precision=HIGHEST) + jnp.dot(
        coef_imag, flat_turned, precision=HIGHEST
    )
    return (potential, projector.reshape(orbitals.shape))


def remote(source, target, send_sem, recv_sem, where):
    return pltpu.make_async_remote_copy(
        src_ref=source,
        dst_ref=target,
        send_sem=send_sem,
        recv_sem=recv_sem,
        device_id=where,
        device_id_type=MESH,
    )


def greet(others):
    barrier = pltpu.get_barrier_semaphore()
    for other in others:
        pl.semaphore_signal(barrier, inc=1, device_id=other, device_id_type=MESH)
    pl.semaphore_wait(barrier, len(others))


def turn(block):
    lanes = block.shape[-1]
    swapped = pltpu.roll(block, lanes // 2, block.ndim - 1)
    position = lax.broadcasted_iota(jnp.int32, block.shape, block.ndim - 1)
    return jnp.where(position < lanes // 2, swapped, -swapped)


def small_factor_inverse(matrix):
    order = len(matrix)
    lower = [[None] * order for _ in range(order)]
    for column in range(order):
        residual = []
        for row in range(column, order):
            real, imag = matrix[row][column]
            for k in range(column):
                a, b = lower[row][k]
                c, d = lower[column][k]
                real = real - (a * c + b * d)
                imag = imag - (b * c - a * d)
            residual.append((real, imag))
        pivot = jnp.sqrt(residual[0][0])
        lower[column][column] = (pivot, jnp.zeros_like(pivot))
        for row in range(column + 1, order):
            real, imag = residual[row - column]
            lower[row][column] = (real / pivot, imag / pivot)
    inverse = [[None] * order for _ in range(order)]
    for row in range(order):
        pivot = lower[row][row][0]
        inverse[row][row] = (1.0 / pivot, jnp.zeros_like(pivot))
        for column in range(row):
            real = jnp.zeros_like(pivot)
            imag = jnp.zeros_like(pivot)
            for k in range(column, row):
                a, b = lower[row][k]
                c, d = inverse[k][column]
                real = real - (a * c - b * d)
                imag = imag - (a * d + b * c)
            inverse[row][column] = (real / pivot, imag / pivot)
    return inverse


def split_table(table):
    high = table.astype(jnp.bfloat16)
    low = (table - high.astype(np.float64)).astype(jnp.bfloat16)
    return high, low


def right_table(extent, sign):
    grid = np.outer(np.arange(extent), np.arange(extent)) % extent
    angle = 2.0 * math.pi / extent * grid
    cosine, sine = np.cos(angle), sign * np.sin(angle)
    table = np.block([[cosine, sine], [-sine, cosine]])
    high, low = split_table(table)
    upper = np.concatenate([high, low], axis=1)
    lower = np.concatenate([high, np.zeros_like(low)], axis=1)
    return np.concatenate([upper, lower], axis=0)


def left_table(extent, sign):
    grid = np.outer(np.arange(extent), np.arange(extent)) % extent
    angle = 2.0 * math.pi / extent * grid
    high, low = split_table(np.concatenate([np.cos(angle), sign * np.sin(angle)], axis=0))
    return np.concatenate([high, high, low], axis=1)


def halves(value):
    high = value.astype(jnp.bfloat16)
    low = (value - high.astype(jnp.float32)).astype(jnp.bfloat16)
    return high, low


def right_product(value, table):
    lanes = value.shape[-1]
    high, low = halves(value)
    both = jnp.dot(
        jnp.concatenate([high, low], axis=1), table, preferred_element_type=jnp.float32
    )
    return both[:, :lanes] + both[:, lanes:]


def left_product(first, second, table):
    rows, lanes = first.shape
    high, low = halves(jnp.concatenate([first, second], axis=1))
    stacked = jnp.concatenate([high, low, high], axis=0)
    both = jnp.dot(table, stacked, preferred_element_type=jnp.float32)
    return tuple(
        both[:rows, cut : cut + lanes] - turn(both[rows:, cut : cut + lanes])
        for cut in (0, lanes)
    )


def spread_parts(value):
    lanes = value.shape[-1]
    swapped = pltpu.roll(value, lanes // 2, value.ndim - 1)
    lower = lax.broadcasted_iota(jnp.int32, value.shape, value.ndim - 1) < lanes // 2
    return jnp.where(lower, value, swapped), jnp.where(lower, swapped, value)


def forward_group(group, orbital_grid, partner_grid, work, right, left):
    rows, lanes = orbital_grid.shape[1:]
    span = pl.ds(group * GROUP, GROUP)
    orbital = orbital_grid[span].reshape(GROUP * rows, lanes)
    real, imag = spread_parts(partner_grid[span].reshape(GROUP * rows, lanes))
    density = real * orbital + imag * turn(orbital)
    lines = right_product(density, right[...])
    planes = []
    for pair in range(GROUP // 2):
        start = 2 * pair * rows
        planes += left_product(
            lines[start : start + rows], lines[start + rows : start + 2 * rows], left[...]
        )
    stacked = jnp.stack(planes, axis=0)
    work[:, span, :] = jnp.swapaxes(stacked, 0, 1)


def backward_group(group, partner_grid, partial, work, right, left):
    rows, lanes = partner_grid.shape[1:]
    span = pl.ds(group * GROUP, GROUP)
    planes = jnp.swapaxes(work[:, span, :], 0, 1)
    lines = []
    for pair in range(GROUP // 2):
        lines += left_product(planes[2 * pair], planes[2 * pair + 1], left[...])
    field = right_product(jnp.concatenate(lines, axis=0), right[...])
    real, imag = spread_parts(partner_grid[span].reshape(GROUP * rows, lanes))
    partial[span] = (real * field - imag * turn(field)).reshape(GROUP, rows, lanes)


def middle_pairs(shift, work, forward, inverse):
    columns, extent, lanes = work.shape
    first = frequency(lax.broadcasted_iota(jnp.int32, (extent, lanes), 0), extent)
    third_place = lax.broadcasted_iota(jnp.int32, (extent, lanes), 1)
    third_place = jnp.where(third_place < lanes // 2, third_place, third_place - lanes // 2)
    third = frequency(third_place, extent)
    base = (first + shift[0]) ** 2 + (third + shift[2]) ** 2 + SCREEN_SQUARE
    scale = FOUR_PI / (float(extent) * float(columns) * float(lanes // 2))

    def one_pair(pair, carry):
        spectra = left_product(work[2 * pair], work[2 * pair + 1], forward[...])
        scaled = []
        for which in range(2):
            column = 2 * pair + which
            second = jnp.where(column < columns // 2, column, column - columns)
            offset = (second.astype(jnp.float32) + shift[1]) ** 2
            scaled.append(spectra[which] * (scale / (base + offset)))
        fields = left_product(scaled[0], scaled[1], inverse[...])
        work[2 * pair] = fields[0]
        work[2 * pair + 1] = fields[1]
        return carry

    lax.fori_loop(0, columns // 2, one_pair, 0, unroll=4)


def exchange_kernel(
    bands,
    ranks,
    shift_table,
    shift_index,
    orbital_home,
    partner_home,
    right_forward_home,
    right_inverse_home,
    left_forward_home,
    left_inverse_home,
    potential,
    projector,
    orbital_grid,
    partner_grid,
    work,
    partial,
    partner,
    detour,
    near,
    outgoing,
    arriving,
    passed,
    others,
    tallies,
    own_sums,
    all_sums,
    right_forward,
    right_inverse,
    left_forward,
    left_inverse,
    load_sem,
    gather_send,
    detour_send,
    detour_recv,
    onward_send,
    chain_send,
    partner_recv,
    grid_send,
    grid_recv,
    other_send,
    other_recv,
    near_send,
    near_recv,
    far_send,
    far_recv,
    up_send,
    up_recv,
    sum_send,
    sum_recv,
):
    planes, rows, lanes = potential.shape
    chunks = bands
    piece = planes // chunks
    per_group = GROUP // piece
    halves_count = planes // GROUP
    last = bands - 1
    direct = chunks // 2
    band = lax.axis_index("band")
    rank = lax.axis_index("fft")
    beside = rank + 1 - 2 * (rank % 2)
    across = (rank + 2) % ranks
    beside_across = (beside + 2) % ranks
    slabs = (rank, beside, across, beside_across)
    home = 2 * (rank % 2) + (rank // 2 + rank % 2) % 2
    keeper = 2 * ((band // 2 + band % 2) % 2) + band // 2

    def both(*conditions):
        return functools.reduce(jnp.logical_and, conditions)

    def either(*conditions):
        return functools.reduce(jnp.logical_or, conditions)

    at_home = band == home
    at_end = either(band == 0, band == last)
    early = either(at_home, band == 1, band == last - 1)
    low_side = rank < ranks // 2
    takes_detour = both(at_end, low_side)
    gives_detour = both(jnp.logical_not(at_end), low_side)

    def span(index):
        return pl.ds(index * piece, piece)

    def slab(index):
        return pl.ds(index * planes, planes)

    def window(index, chunk):
        return pl.ds(index * planes + chunk * piece, piece)

    own_slab = pltpu.make_async_copy(orbital_home, orbital_grid.at[slab(rank)], load_sem.at[1])
    partner_load = pltpu.make_async_copy(partner_home, partner, load_sem.at[0])
    home_load = pltpu.make_async_copy(partner_home, partner_grid.at[slab(rank)], load_sem.at[2])
    table_loads = [
        pltpu.make_async_copy(source, here, load_sem.at[3 + number])
        for number, (source, here) in enumerate(
            (
                (right_forward_home, right_forward),
                (left_forward_home, left_forward),
                (right_inverse_home, right_inverse),
                (left_inverse_home, left_inverse),
            )
        )
    ]
    partner_load.start()

    @pl.when(at_home)
    def _():
        home_load.start()

    own_slab.start()
    for load in table_loads:
        load.start()
    greet(
        [
            {"band": (band + step) % bands, "fft": (rank + turn_by) % ranks}
            for step in range(bands)
            for turn_by in range(ranks)
            if step or turn_by
        ]
    )

    def gather_copy(chunk):
        return remote(
            partner.at[span(chunk)],
            partner_grid.at[window(rank, chunk)],
            gather_send.at[chunk],
            partner_recv.at[rank, chunk],
            {"fft": keeper},
        )

    def detour_copy(chunk):
        return remote(
            partner.at[span(chunk)],
            detour.at[chunk],
            detour_send.at[chunk],
            detour_recv.at[chunk],
            {"band": last * (band - 1)},
        )

    def onward_copy(chunk):
        return remote(
            detour.at[chunk],
            partner_grid.at[window(rank, chunk)],
            onward_send.at[chunk],
            partner_recv.at[rank, chunk],
            {"fft": ranks // 2 + band // last},
        )

    def chain_copy(way, turn_to, chunk):
        place = partner_grid.at[window(slabs[turn_to], chunk)]
        return remote(
            place,
            place,
            chain_send.at[way, turn_to, chunk],
            partner_recv.at[slabs[turn_to], chunk],
            {"band": band + 1 - 2 * way},
        )

    def passes(way, turn_to):
        if way == 0:
            go = both(band >= home, band < last)
            short = both(band == last - 1, rank == ranks - 1)
        else:
            go = both(band <= home, band > 0)
            short = both(band == 1, rank == ranks // 2)
        return both(go, jnp.logical_not(short)) if turn_to > 1 else go

    def arrive(turn_to, chunk):
        def wait():
            chain_copy(0, turn_to, chunk).wait_recv()

        if turn_to:
            wait()
        else:
            pl.when(jnp.logical_not(at_home))(wait)

    def step(turn_to, chunk):
        arrive(turn_to, chunk)
        for way in (0, 1):

            @pl.when(passes(way, turn_to))
            def _():
                chain_copy(way, turn_to, chunk).start()

    tail = [(turn_to, half) for half in range(halves_count) for turn_to in (2, 3)]

    def of_half(half):
        return range(half * per_group, (half + 1) * per_group)

    partner_load.wait()
    for chunk in range(chunks):

        @pl.when(jnp.logical_not(at_home))
        def _():
            gather_copy(chunk).start()

        @pl.when(gives_detour)
        def _():
            detour_copy(chunk).start()

    @pl.when(at_home)
    def _():
        home_load.wait()

    own_slab.wait()
    own_orbital = orbital_grid.at[slab(rank)]
    to_across = remote(own_orbital, own_orbital, grid_send.at[0], grid_recv.at[0], {"fft": across})
    to_beside = remote(own_orbital, own_orbital, grid_send.at[1], grid_recv.at[1], {"fft": beside})
    other_orbital = orbital_grid.at[slab(across)]
    onward = remote(
        other_orbital, other_orbital, grid_send.at[2], grid_recv.at[2], {"fft": beside}
    )
    to_across.start()
    to_beside.start()

    def take_detour(condition, chunk):
        @pl.when(both(takes_detour, condition))
        def _():
            detour_copy(chunk).wait_recv()
            onward_copy(chunk).start()

    for turn_to in (0, 1):
        for chunk in range(chunks):
            step(turn_to, chunk)
            if turn_to == 1:
                take_detour(jnp.logical_not(at_home), chunk)

    def other_copy(which, slot, where, source=own_orbital):
        return remote(
            source,
            others.at[slot],
            other_send.at[which],
            other_recv.at[slot],
            {"band": where},
        )

    @pl.when(early)
    def _():
        for turn_to, half in tail:
            for chunk in of_half(half):
                if turn_to == 2:
                    take_detour(at_home, chunk)
            for chunk in of_half(half):
                step(turn_to, chunk)

    @pl.when(band == 0)
    def _():
        other_copy(0, 0, 1).start()

    @pl.when(band == last)
    def _():
        other_copy(0, 1, last - 1).start()

    to_across.wait_recv()
    onward.start()
    for load in table_loads:
        load.wait()
    to_beside.wait_recv()
    onward.wait_recv()

    def forward(group):
        forward_group(group, orbital_grid, partner_grid, work, right_forward, left_forward)

    def forward_near(index, carry):
        forward(
            (rank + index // halves_count * (beside - rank)) * halves_count + index % halves_count
        )
        return carry

    lax.fori_loop(0, 2 * halves_count, forward_near, 0)
    for turn_to, half in tail:

        @pl.when(jnp.logical_not(early))
        def _():
            for chunk in of_half(half):
                arrive(turn_to, chunk)

        forward(slabs[turn_to] * halves_count + half)

    chosen = shift_index[home]
    shift = [shift_table[axis, chosen] for axis in range(3)]
    middle_pairs(shift, work, left_forward, left_inverse)

    @pl.when(band == last)
    def _():
        other_copy(1, 1, 0).start()

    @pl.when(band == 1)
    def _():
        other_copy(0, 0, 0).wait_recv()
        other_copy(0, 0, 2, others.at[0]).start()

    def backward(index, half):
        backward_group(
            index * halves_count + half, partner_grid, partial, work, right_inverse, left_inverse
        )

    def near_copy(which, index, half):
        return remote(
            partial.at[pl.ds(index * planes + half * GROUP, GROUP)],
            near.at[which, pl.ds(half * GROUP, GROUP)],
            near_send.at[which, half],
            near_recv.at[which, half],
            {"fft": beside},
        )

    def far_copy(chunk):
        return remote(
            outgoing.at[chunk],
            arriving.at[chunk],
            far_send.at[chunk],
            far_recv.at[chunk],
            {"fft": across},
        )

    def up_copy(owner, chunk, own=False):
        held = passed.at[owner, span(chunk)]
        return remote(
            potential.at[span(chunk)] if own else held,
            held,
            up_send.at[owner, chunk],
            up_recv.at[owner, chunk],
            {"band": band + 1},
        )

    for half in range(halves_count):
        backward(beside_across, half)
        near_copy(1, beside_across, half).start()
        backward(across, half)
        near_copy(1, beside_across, half).wait_recv()
        for chunk in of_half(half):
            outgoing[chunk] = partial[window(across, chunk)] + near[1, span(chunk)]
            far_copy(chunk).start()
    for half in range(halves_count):
        backward(beside, half)
        near_copy(0, beside, half).start()
    for half in range(halves_count):
        backward(rank, half)

    zero = jnp.zeros((8, lanes), jnp.float32)
    for number in range(tallies.shape[0]):
        tallies[number] = zero

    def inner(slot, left, right, chunk):
        def accumulate(plane, sums):
            straight = right(plane)
            value = left(plane)
            return tuple(
                running + jnp.sum((value * other).reshape(rows // 8, 8, lanes), axis=0)
                for running, other in zip(sums, (straight, turn(straight)))
            )

        sums = lax.fori_loop(
            chunk * piece,
            (chunk + 1) * piece,
            accumulate,
            (tallies[2 * slot], tallies[2 * slot + 1]),
        )
        tallies[2 * slot] = sums[0]
        tallies[2 * slot + 1] = sums[1]

    def own_potential(plane):
        return potential[plane]

    def own_values(plane):
        return orbital_grid[rank * planes + plane]

    holds_first = either(band == 1, band == 2)
    holds_last = either(band == 0, band == 2)

    def with_others(span_of_chunks, wait):
        for slot, held in ((0, holds_first), (1, holds_last)):

            @pl.when(held)
            def _():
                if wait and slot:
                    other_copy(0, 1, 0).wait_recv()
                for chunk in span_of_chunks:
                    inner(1 + slot, lambda plane: others[slot, plane], own_potential, chunk)

    for chunk in range(chunks):
        if chunk % per_group == 0:
            near_copy(0, beside, chunk // per_group).wait_recv()
        far_copy(chunk).wait_recv()
        potential[span(chunk)] = (
            partial[window(rank, chunk)] + near[0, span(chunk)]
        ) + arriving[chunk]

        @pl.when(band < last - 1 if chunk >= direct else band < last)
        def _():
            up_copy(band, chunk, True).start()

        inner(0, own_values, own_potential, chunk)
        if chunk == chunks - 2:

            @pl.when(band == 2)
            def _():
                other_copy(0, 0, 0).wait_recv()

            with_others(range(chunk + 1), True)
    with_others([chunks - 1], False)

    @pl.when(band == 2)
    def _():
        for chunk in range(chunks):
            up_copy(1, chunk).wait_recv()
            if chunk < direct:
                up_copy(1, chunk).start()
            inner(3, own_values, lambda plane: passed[1, plane], chunk)
            inner(4, lambda plane: others[1, plane], lambda plane: passed[1, plane], chunk)

    entries = [(i, l) for i in range(bands) for l in range(i + 1)]
    row_start = band * (band + 1) // 2
    places = (
        row_start + band,
        row_start,
        entries.index((last, 0)) + band,
        entries.index((2, 1)),
        entries.index((last, 1)),
    )
    position = lax.broadcasted_iota(jnp.int32, (8, lanes), 1)
    packed = zero
    for slot, place in enumerate(places):
        for half in range(2):
            value = jnp.sum(tallies[2 * slot + half], axis=1, keepdims=True)
            value = -value if (slot, half) == (1, 1) else value
            packed = packed + jnp.where(position == 2 * place + half, value, 0.0)
    own_sums[...] = packed
    sum_copies = []
    for step_by in range(bands):
        for turn_by in range(ranks):
            if step_by == 0 and turn_by == 0:
                continue
            copy = remote(
                own_sums,
                all_sums.at[band, rank],
                sum_send.at[step_by, turn_by],
                sum_recv.at[step_by, turn_by],
                {"band": (band + step_by) % bands, "fft": (rank + turn_by) % ranks},
            )
            copy.start()
            sum_copies.append(copy)
    all_sums[band, rank] = packed

    @pl.when(either(band == 1, band == 2))
    def _():
        for chunk in range(direct):
            up_copy(0, chunk).wait_recv()
            up_copy(0, chunk).start()

    @pl.when(band == 1)
    def _():
        for chunk in range(direct, chunks):
            up_copy(0, chunk).wait_recv()
            up_copy(0, chunk).start()

    for copy in sum_copies:
        copy.wait()
    total = zero
    for one_band in range(bands):
        for one_rank in range(ranks):
            total = total + all_sums[one_band, one_rank]
    total = jnp.broadcast_to(jnp.sum(total, axis=0, keepdims=True), (8, lanes))
    volume = float(lanes // 2) * float(rows) * float(planes * ranks)
    matrix = [[None] * bands for _ in range(bands)]
    for number, (i, l) in enumerate(entries):
        values = [
            jnp.broadcast_to(
                jnp.sum(jnp.where(position == 2 * number + half, total, 0.0), axis=1, keepdims=True),
                (8, lanes),
            )
            / volume
            for half in range(2)
        ]
        matrix[i][l] = (values[0], values[1])
    inverse = small_factor_inverse(matrix)

    def combine(row, own, members, start, stop, put):
        def one_plane(plane, carry):
            sum_straight = jnp.zeros((rows, lanes), jnp.float32)
            sum_turned = jnp.zeros((rows, lanes), jnp.float32)
            for m in members:
                block = potential[plane] if m is None else passed[m, plane]
                real, imag = inverse[row][own if m is None else m]
                sum_straight = sum_straight + real[:1] * block
                sum_turned = sum_turned + imag[:1] * block
            put(plane, sum_straight + turn(sum_turned))
            return carry

        lax.fori_loop(start, stop, one_plane, 0)

    def put_whole(plane, value):
        projector[plane] = value

    def put_more(plane, value):
        projector[plane] = projector[plane] + value

    def put_lifted(plane, value):
        passed[2, plane] = value

    for row in range(2):

        @pl.when(band == row)
        def _():
            combine(row, row, [None, 0][: row + 1], 0, planes, put_whole)

    @pl.when(band == 2)
    def _():
        for chunk in range(direct, chunks):
            up_copy(0, chunk).wait_recv()
            combine(last, 2, (0, 1, None), chunk * piece, (chunk + 1) * piece, put_lifted)
            up_copy(2, chunk).start()
        combine(2, 2, (0, 1, None), 0, planes, put_whole)

    @pl.when(band == last)
    def _():
        for member in (2, 1):
            for chunk in range(direct):
                up_copy(member, chunk).wait_recv()
        combine(last, last, (1, 2, None), 0, direct * piece, put_whole)
        combine(last, last, (None,), direct * piece, planes, put_whole)
        for chunk in range(direct):
            up_copy(0, chunk).wait_recv()
            combine(last, last, (0,), chunk * piece, (chunk + 1) * piece, put_more)
        for chunk in range(direct, chunks):
            up_copy(2, chunk).wait_recv()
            projector[span(chunk)] = projector[span(chunk)] + passed[2, span(chunk)]

    for chunk in range(chunks):

        @pl.when(jnp.logical_not(at_home))
        def _():
            gather_copy(chunk).wait_send()

        @pl.when(gives_detour)
        def _():
            detour_copy(chunk).wait_send()

        @pl.when(takes_detour)
        def _():
            onward_copy(chunk).wait_send()

        for turn_to in range(len(slabs)):
            for way in (0, 1):

                @pl.when(passes(way, turn_to))
                def _():
                    chain_copy(way, turn_to, chunk).wait_send()

        far_copy(chunk).wait_send()

        @pl.when(band < last)
        def _():
            up_copy(band, chunk, True).wait_send()

        if chunk < direct:

            @pl.when(band == 2)
            def _():
                up_copy(1, chunk).wait_send()

        @pl.when(band == 1 if chunk >= direct else either(band == 1, band == 2))
        def _():
            up_copy(0, chunk).wait_send()

    @pl.when(band != 2)
    def _():
        other_copy(0, 0, 1).wait_send()

    @pl.when(band == last)
    def _():
        other_copy(1, 1, 0).wait_send()

    for half in range(halves_count):
        near_copy(0, beside, half).wait_send()
        near_copy(1, beside_across, half).wait_send()
    to_across.wait_send()
    to_beside.wait_send()
    onward.wait_send()


def exchange(bands, ranks, orbital, partner, shift_table, shift_index):
    planes, rows, lanes = orbital.shape
    chunks = bands
    halves_count = planes // GROUP
    vmem = pl.BlockSpec(memory_space=pltpu.VMEM)
    smem = pl.BlockSpec(memory_space=pltpu.SMEM)
    out = jax.ShapeDtypeStruct((planes, rows, lanes), jnp.float32)
    grid = pltpu.VMEM((ranks * planes, rows, lanes), jnp.float32)
    slab = pltpu.VMEM((planes, rows, lanes), jnp.float32)
    quarters = pltpu.VMEM((chunks, planes // chunks, rows, lanes), jnp.float32)

    def slab_list(count):
        return pltpu.VMEM((count, planes, rows, lanes), jnp.float32)

    dma = pltpu.SemaphoreType.DMA
    tables = [
        jnp.asarray(table)
        for table in (
            right_table(rows, -1.0),
            right_table(rows, 1.0),
            left_table(rows, -1.0),
            left_table(rows, 1.0),
        )
    ]
    return pl.pallas_call(
        functools.partial(exchange_kernel, bands, ranks),
        name="exchange",
        out_shape=(out, out),
        in_specs=[smem, smem] + [pl.BlockSpec(memory_space=pl.ANY)] * 6,
        out_specs=(vmem, vmem),
        scratch_shapes=[
            grid,
            grid,
            grid,
            grid,
            slab,
            quarters,
            slab_list(2),
            quarters,
            quarters,
            slab_list(bands - 1),
            slab_list(2),
            pltpu.VMEM((10, 8, lanes), jnp.float32),
            pltpu.VMEM((8, lanes), jnp.float32),
            pltpu.VMEM((bands, ranks, 8, lanes), jnp.float32),
        ]
        + [pltpu.VMEM(table.shape, table.dtype) for table in tables]
        + [
            dma((7,)),
            dma((chunks,)),
            dma((chunks,)),
            dma((chunks,)),
            dma((chunks,)),
            dma((2, ranks, chunks)),
            dma((ranks, chunks)),
            dma((3,)),
            dma((3,)),
            dma((2,)),
            dma((2,)),
            dma((2, halves_count)),
            dma((2, halves_count)),
            dma((chunks,)),
            dma((chunks,)),
            dma((bands, chunks)),
            dma((bands, chunks)),
            dma((bands, ranks)),
            dma((bands, ranks)),
        ],
        compiler_params=pltpu.CompilerParams(
            collective_id=0, has_side_effects=True, vmem_limit_bytes=60 * 1024 * 1024
        ),
    )(shift_table.T, shift_index, orbital, partner, *tables)


def paired_body(bands, ranks, orbitals, partners, shift_table, shift_index):
    potential, projector = exchange(
        bands, ranks, orbitals[0], partners[0], shift_table, shift_index
    )
    return (potential[None], projector[None])


def body(orbitals, partners, shift_table, shift_index):
    bands = lax.axis_size("band")
    ranks = lax.axis_size("fft")
    count, planes, rows, lanes = orbitals.shape
    grid_bytes = ranks * planes * rows * lanes * 4
    paired = (
        count == 1
        and ranks == 4
        and bands == ranks
        and planes % bands == 0
        and planes % GROUP == 0
        and GROUP % (planes // bands) == 0
        and lanes == 2 * rows
        and lanes == 128
        and grid_bytes <= 2 * 1024 * 1024
    )
    if paired:
        return paired_body(bands, ranks, orbitals, partners, shift_table, shift_index)
    return general_body(orbitals, partners, shift_table, shift_index)


def solution(mesh):
    in_specs = (
        P(("kgrp", "band"), "fft", None, None),
        P(("kgrp", "band"), "fft", None, None),
        P(),
        P("kgrp"),
    )
    out_specs = (P(("kgrp", "band"), "fft", None, None), P(("kgrp", "band"), "fft", None, None))
    return jax.shard_map(body, mesh=mesh, in_specs=in_specs, out_specs=out_specs, check_vma=False)
```

```python
import functools
import math

import jax
import jax.numpy as jnp
import numpy as np
from jax import lax
from jax.experimental import pallas as pl
from jax.experimental.pallas import tpu as pltpu
from jax.sharding import PartitionSpec as P

HIGHEST = lax.Precision.HIGHEST
HIGH = lax.Precision.HIGH
MESH = pl.DeviceIdType.MESH
GROUP = 8
SCREEN_SQUARE = 0.25
FOUR_PI = 4.0 * math.pi


def angle_pair(extent, sign):
    positions = jnp.arange(extent, dtype=jnp.int32)
    product = positions[:, None] * positions[None, :] % extent
    angle = 2.0 * math.pi / extent * product.astype(jnp.float32)
    return (jnp.cos(angle), sign * jnp.sin(angle))


def last_table(extent, sign):
    cosine, sine = angle_pair(extent, sign)
    upper = jnp.concatenate([cosine, sine], axis=1)
    lower = jnp.concatenate([-sine, cosine], axis=1)
    return jnp.concatenate([upper, lower], axis=0)


def middle_table(extent, sign):
    cosine, sine = angle_pair(extent, sign)
    return jnp.stack([jnp.stack([cosine, -sine], -1), jnp.stack([sine, cosine], -1)], 1)


def along_last(field, table):
    shape = field.shape
    flat = field.reshape(-1, shape[-1])
    return jnp.dot(flat, table, precision=HIGH).reshape(shape)


def along_axis(field, table, axis_number):
    shape = field.shape
    extent = shape[-1] // 2
    split = field.reshape(shape[0], shape[1], shape[2], 2, extent)
    if axis_number == 1:
        result = jnp.einsum("kcnd,pnbdz->pkbcz", table, split, precision=HIGH)
    else:
        result = jnp.einsum("kcnd,pandz->pakcz", table, split, precision=HIGH)
    return result.reshape(shape)


def times_conj(left, right):
    extent = left.shape[-1] // 2
    left_real, left_imag = (left[..., :extent], left[..., extent:])
    right_real, right_imag = (right[..., :extent], right[..., extent:])
    return jnp.concatenate(
        [
            left_real * right_real + left_imag * right_imag,
            left_real * right_imag - left_imag * right_real,
        ],
        axis=-1,
    )


def times(left, right):
    extent = left.shape[-1] // 2
    left_real, left_imag = (left[..., :extent], left[..., extent:])
    right_real, right_imag = (right[..., :extent], right[..., extent:])
    return jnp.concatenate(
        [
            left_real * right_real - left_imag * right_imag,
            left_real * right_imag + left_imag * right_real,
        ],
        axis=-1,
    )


def rotate(field):
    extent = field.shape[-1] // 2
    return jnp.concatenate([field[..., extent:], -field[..., :extent]], axis=-1)


def frequency(positions, extent):
    return jnp.where(positions < extent // 2, positions, positions - extent).astype(jnp.float32)


def kernel_block(qvectors, y_count, extent):
    first_freq = frequency(jnp.arange(extent, dtype=jnp.int32), extent)
    second_freq = frequency(jnp.arange(y_count, dtype=jnp.int32), extent)
    third_freq = frequency(jnp.arange(2 * extent, dtype=jnp.int32) % extent, extent)
    first_part = (first_freq[None, :] + qvectors[:, 0:1]) ** 2
    second_part = (second_freq[None, :] + qvectors[:, 1:2]) ** 2
    third_part = (third_freq[None, :] + qvectors[:, 2:3]) ** 2
    denominator = (
        first_part[:, :, None, None]
        + second_part[:, None, :, None]
        + third_part[:, None, None, :]
        + SCREEN_SQUARE
    )
    return FOUR_PI / extent**3 / denominator


def shifts_for(shift_table, shift_index, start_at, length):
    picked = lax.dynamic_slice_in_dim(shift_index, start_at, length)
    onehot = (picked[:, None] == jnp.arange(shift_table.shape[0], dtype=jnp.int32)[None, :]).astype(
        jnp.float32
    )
    return jnp.dot(onehot, shift_table, precision=HIGHEST)


def factor_inverse(over_real, over_imag):
    matrix_order = over_real.shape[0]
    positions = jnp.arange(matrix_order, dtype=jnp.int32)
    zero_start = jnp.zeros_like(over_real)

    def chol_step(column, lowers):
        lower_real, lower_imag = lowers
        row_real = lower_real[column]
        row_imag = lower_imag[column]
        resid_real = over_real[:, column] - (
            jnp.dot(lower_real, row_real, precision=HIGHEST)
            + jnp.dot(lower_imag, row_imag, precision=HIGHEST)
        )
        resid_imag = over_imag[:, column] - (
            jnp.dot(lower_imag, row_real, precision=HIGHEST)
            - jnp.dot(lower_real, row_imag, precision=HIGHEST)
        )
        pivot_value = jnp.sqrt(resid_real[column])
        below_diag = positions > column
        at_diag = positions == column
        new_real = jnp.where(
            below_diag, resid_real / pivot_value, jnp.where(at_diag, pivot_value, 0.0)
        )
        new_imag = jnp.where(below_diag, resid_imag / pivot_value, 0.0)
        chosen = positions[None, :] == column
        return (
            jnp.where(chosen, new_real[:, None], lower_real),
            jnp.where(chosen, new_imag[:, None], lower_imag),
        )

    lower_real, lower_imag = lax.fori_loop(0, matrix_order, chol_step, (zero_start, zero_start))

    def solve_step(row_index, inverses):
        inv_real, inv_imag = inverses
        row_real = lower_real[row_index]
        row_imag = lower_imag[row_index]
        sum_real = jnp.dot(row_real, inv_real, precision=HIGHEST) - jnp.dot(
            row_imag, inv_imag, precision=HIGHEST
        )
        sum_imag = jnp.dot(row_real, inv_imag, precision=HIGHEST) + jnp.dot(
            row_imag, inv_real, precision=HIGHEST
        )
        unit_row = (positions == row_index).astype(over_real.dtype)
        pivot_value = lower_real[row_index, row_index]
        new_real = (unit_row - sum_real) / pivot_value
        new_imag = -sum_imag / pivot_value
        chosen = positions[:, None] == row_index
        return (
            jnp.where(chosen, new_real[None, :], inv_real),
            jnp.where(chosen, new_imag[None, :], inv_imag),
        )

    return lax.fori_loop(0, matrix_order, solve_step, (zero_start, zero_start))


def general_body(orbitals, partners, shift_table, shift_index):
    extent = orbitals.shape[2]
    band_count = orbitals.shape[0]
    tables = (
        last_table(extent, -1.0),
        middle_table(extent, -1.0),
        last_table(extent, 1.0),
        middle_table(extent, 1.0),
    )
    my_band = lax.axis_index("band")
    forward_last, forward_mid, inverse_last, inverse_mid = tables
    full_orbitals = lax.all_gather(orbitals, "fft", axis=1, tiled=True)
    every_slab = lax.all_gather(partners, "band", axis=0, tiled=True)
    own_grids = lax.all_to_all(every_slab, "fft", split_axis=0, concat_axis=1, tiled=True)
    own_count = own_grids.shape[0]
    qvectors = shifts_for(shift_table, shift_index, lax.axis_index("fft") * own_count, own_count)

    def one_partner(member, running):
        single = lax.dynamic_slice_in_dim(own_grids, member, 1, 0)
        kernel = kernel_block(lax.dynamic_slice_in_dim(qvectors, member, 1, 0), extent, extent)
        density = times_conj(single, full_orbitals)
        spectrum = (
            along_axis(
                along_axis(along_last(density, forward_last), forward_mid, 2), forward_mid, 1
            )
            * kernel
        )
        field = along_last(
            along_axis(along_axis(spectrum, inverse_mid, 1), inverse_mid, 2), inverse_last
        )
        return running + times(single, field)

    partial_value = lax.fori_loop(
        0, own_count, one_partner, jnp.zeros(full_orbitals.shape, jnp.float32)
    )
    potential = lax.psum_scatter(partial_value, "fft", scatter_dimension=1, tiled=True)
    every_pot = lax.all_gather(potential, "band", axis=0, tiled=True)
    turned = rotate(every_pot)
    total_bands = every_pot.shape[0]
    flat_orbitals = orbitals.reshape(band_count, -1)
    flat_pot = every_pot.reshape(total_bands, -1)
    flat_turned = turned.reshape(total_bands, -1)
    volume = float(extent**3)
    rows_real = jnp.einsum("ik,jk->ij", flat_orbitals, flat_pot, precision=HIGHEST) / volume
    rows_imag = jnp.einsum("ik,jk->ij", flat_orbitals, flat_turned, precision=HIGHEST) / volume
    start_row = my_band * band_count
    summed_real, summed_imag = lax.psum((rows_real, rows_imag), "fft")
    over_real, over_imag = (
        lax.all_gather(summed_real, "band", axis=0, tiled=True),
        lax.all_gather(summed_imag, "band", axis=0, tiled=True),
    )
    inv_real, inv_imag = factor_inverse(over_real, over_imag)
    coef_real = lax.dynamic_slice_in_dim(inv_real, start_row, band_count, 0)
    coef_imag = lax.dynamic_slice_in_dim(inv_imag, start_row, band_count, 0)
    projector = jnp.dot(coef_real, flat_pot, precision=HIGHEST) + jnp.dot(
        coef_imag, flat_turned, precision=HIGHEST
    )
    return (potential, projector.reshape(orbitals.shape))


def remote(source, target, send_sem, recv_sem, where):
    return pltpu.make_async_remote_copy(
        src_ref=source,
        dst_ref=target,
        send_sem=send_sem,
        recv_sem=recv_sem,
        device_id=where,
        device_id_type=MESH,
    )


def greet(others):
    barrier = pltpu.get_barrier_semaphore()
    for other in others:
        pl.semaphore_signal(barrier, inc=1, device_id=other, device_id_type=MESH)
    pl.semaphore_wait(barrier, len(others))


def turn(block):
    lanes = block.shape[-1]
    swapped = pltpu.roll(block, lanes // 2, block.ndim - 1)
    position = lax.broadcasted_iota(jnp.int32, block.shape, block.ndim - 1)
    return jnp.where(position < lanes // 2, swapped, -swapped)


def small_factor_inverse(matrix):
    order = len(matrix)
    lower = [[None] * order for _ in range(order)]
    for column in range(order):
        residual = []
        for row in range(column, order):
            real, imag = matrix[row][column]
            for k in range(column):
                a, b = lower[row][k]
                c, d = lower[column][k]
                real = real - (a * c + b * d)
                imag = imag - (b * c - a * d)
            residual.append((real, imag))
        pivot = jnp.sqrt(residual[0][0])
        lower[column][column] = (pivot, jnp.zeros_like(pivot))
        for row in range(column + 1, order):
            real, imag = residual[row - column]
            lower[row][column] = (real / pivot, imag / pivot)
    inverse = [[None] * order for _ in range(order)]
    for row in range(order):
        pivot = lower[row][row][0]
        inverse[row][row] = (1.0 / pivot, jnp.zeros_like(pivot))
        for column in range(row):
            real = jnp.zeros_like(pivot)
            imag = jnp.zeros_like(pivot)
            for k in range(column, row):
                a, b = lower[row][k]
                c, d = inverse[k][column]
                real = real - (a * c - b * d)
                imag = imag - (a * d + b * c)
            inverse[row][column] = (real / pivot, imag / pivot)
    return inverse


def split_table(table):
    high = table.astype(jnp.bfloat16)
    low = (table - high.astype(np.float64)).astype(jnp.bfloat16)
    return high, low


def right_table(extent, sign):
    grid = np.outer(np.arange(extent), np.arange(extent)) % extent
    angle = 2.0 * math.pi / extent * grid
    cosine, sine = np.cos(angle), sign * np.sin(angle)
    table = np.block([[cosine, sine], [-sine, cosine]])
    high, low = split_table(table)
    upper = np.concatenate([high, low], axis=1)
    lower = np.concatenate([high, np.zeros_like(low)], axis=1)
    return np.concatenate([upper, lower], axis=0)


def left_table(extent, sign):
    grid = np.outer(np.arange(extent), np.arange(extent)) % extent
    angle = 2.0 * math.pi / extent * grid
    high, low = split_table(np.concatenate([np.cos(angle), sign * np.sin(angle)], axis=0))
    return np.concatenate([high, high, low], axis=1)


def halves(value):
    high = value.astype(jnp.bfloat16)
    low = (value - high.astype(jnp.float32)).astype(jnp.bfloat16)
    return high, low


def right_product(value, table):
    lanes = value.shape[-1]
    high, low = halves(value)
    both = jnp.dot(
        jnp.concatenate([high, low], axis=1), table, preferred_element_type=jnp.float32
    )
    return both[:, :lanes] + both[:, lanes:]


def left_product(first, second, table):
    rows, lanes = first.shape
    high, low = halves(jnp.concatenate([first, second], axis=1))
    stacked = jnp.concatenate([high, low, high], axis=0)
    both = jnp.dot(table, stacked, preferred_element_type=jnp.float32)
    return tuple(
        both[:rows, cut : cut + lanes] - turn(both[rows:, cut : cut + lanes])
        for cut in (0, lanes)
    )


def spread_parts(value):
    lanes = value.shape[-1]
    swapped = pltpu.roll(value, lanes // 2, value.ndim - 1)
    lower = lax.broadcasted_iota(jnp.int32, value.shape, value.ndim - 1) < lanes // 2
    return jnp.where(lower, value, swapped), jnp.where(lower, swapped, value)


def forward_group(group, orbital_grid, partner_grid, work, right, left):
    rows, lanes = orbital_grid.shape[1:]
    span = pl.ds(group * GROUP, GROUP)
    orbital = orbital_grid[span].reshape(GROUP * rows, lanes)
    real, imag = spread_parts(partner_grid[span].reshape(GROUP * rows, lanes))
    density = real * orbital + imag * turn(orbital)
    lines = right_product(density, right[...])
    planes = []
    for pair in range(GROUP // 2):
        start = 2 * pair * rows
        planes += left_product(
            lines[start : start + rows], lines[start + rows : start + 2 * rows], left[...]
        )
    stacked = jnp.stack(planes, axis=0)
    work[:, span, :] = jnp.swapaxes(stacked, 0, 1)


def backward_group(group, partner_grid, partial, work, right, left):
    rows, lanes = partner_grid.shape[1:]
    span = pl.ds(group * GROUP, GROUP)
    planes = jnp.swapaxes(work[:, span, :], 0, 1)
    lines = []
    for pair in range(GROUP // 2):
        lines += left_product(planes[2 * pair], planes[2 * pair + 1], left[...])
    field = right_product(jnp.concatenate(lines, axis=0), right[...])
    real, imag = spread_parts(partner_grid[span].reshape(GROUP * rows, lanes))
    partial[span] = (real * field - imag * turn(field)).reshape(GROUP, rows, lanes)


def fill_screen(shift, screen):
    columns, extent, lanes = screen.shape
    first = frequency(lax.broadcasted_iota(jnp.int32, (extent, lanes), 0), extent)
    third_place = lax.broadcasted_iota(jnp.int32, (extent, lanes), 1)
    third_place = jnp.where(third_place < lanes // 2, third_place, third_place - lanes // 2)
    third = frequency(third_place, extent)
    base = (first + shift[0]) ** 2 + (third + shift[2]) ** 2 + SCREEN_SQUARE
    scale = FOUR_PI / (float(extent) * float(columns) * float(lanes // 2))

    def one_column(column, carry):
        second = jnp.where(column < columns // 2, column, column - columns)
        offset = (second.astype(jnp.float32) + shift[1]) ** 2
        screen[column] = scale / (base + offset)
        return carry

    lax.fori_loop(0, columns, one_column, 0, unroll=2)


def middle_pairs(screen, work, forward, inverse):
    columns = work.shape[0]

    def one_pair(pair, carry):
        spectra = left_product(work[2 * pair], work[2 * pair + 1], forward[...])
        scaled = [spectra[which] * screen[2 * pair + which] for which in range(2)]
        fields = left_product(scaled[0], scaled[1], inverse[...])
        work[2 * pair] = fields[0]
        work[2 * pair + 1] = fields[1]
        return carry

    lax.fori_loop(0, columns // 2, one_pair, 0, unroll=16)


def exchange_kernel(
    bands,
    ranks,
    shift_table,
    shift_index,
    orbital_home,
    partner_home,
    right_forward_home,
    right_inverse_home,
    left_forward_home,
    left_inverse_home,
    potential,
    projector,
    orbital_grid,
    partner_grid,
    work,
    partial,
    partner,
    detour,
    near,
    outgoing,
    arriving,
    passed,
    others,
    tallies,
    own_sums,
    all_sums,
    right_forward,
    right_inverse,
    left_forward,
    left_inverse,
    load_sem,
    gather_send,
    detour_send,
    detour_recv,
    onward_send,
    chain_send,
    partner_recv,
    grid_send,
    grid_recv,
    other_send,
    other_recv,
    near_send,
    near_recv,
    far_send,
    far_recv,
    up_send,
    up_recv,
    sum_send,
    sum_recv,
):
    planes, rows, lanes = potential.shape
    chunks = bands
    piece = planes // chunks
    per_group = GROUP // piece
    halves_count = planes // GROUP
    last = bands - 1
    cuts = 2 * chunks
    slice_size = planes // cuts
    direct = 4 * cuts // 8
    band = lax.axis_index("band")
    rank = lax.axis_index("fft")
    beside = rank + 1 - 2 * (rank % 2)
    across = (rank + 2) % ranks
    beside_across = (beside + 2) % ranks
    slabs = (rank, beside, across, beside_across)
    home = 2 * (rank % 2) + (rank // 2 + rank % 2) % 2
    keeper = 2 * ((band // 2 + band % 2) % 2) + band // 2

    def both(*conditions):
        return functools.reduce(jnp.logical_and, conditions)

    def either(*conditions):
        return functools.reduce(jnp.logical_or, conditions)

    at_home = band == home
    at_end = either(band == 0, band == last)
    early = either(at_home, band == 1, band == last - 1)
    low_side = rank < ranks // 2
    takes_detour = both(at_end, low_side)
    gives_detour = both(jnp.logical_not(at_end), low_side)

    def span(index):
        return pl.ds(index * piece, piece)

    def cut_span(cut):
        return pl.ds(cut * slice_size, slice_size)

    def slab(index):
        return pl.ds(index * planes, planes)

    def window(index, chunk):
        return pl.ds(index * planes + chunk * piece, piece)

    own_slab = pltpu.make_async_copy(orbital_home, orbital_grid.at[slab(rank)], load_sem.at[1])
    partner_load = pltpu.make_async_copy(partner_home, partner, load_sem.at[0])
    home_load = pltpu.make_async_copy(partner_home, partner_grid.at[slab(rank)], load_sem.at[2])
    table_loads = [
        pltpu.make_async_copy(source, here, load_sem.at[3 + number])
        for number, (source, here) in enumerate(
            (
                (right_forward_home, right_forward),
                (left_forward_home, left_forward),
                (right_inverse_home, right_inverse),
                (left_inverse_home, left_inverse),
            )
        )
    ]
    partner_load.start()

    @pl.when(at_home)
    def _():
        home_load.start()

    own_slab.start()
    for load in table_loads:
        load.start()
    greet(
        [
            {"band": (band + step) % bands, "fft": (rank + turn_by) % ranks}
            for step in range(bands)
            for turn_by in range(ranks)
            if step or turn_by
        ]
    )

    def gather_copy(chunk):
        return remote(
            partner.at[span(chunk)],
            partner_grid.at[window(rank, chunk)],
            gather_send.at[chunk],
            partner_recv.at[rank, chunk],
            {"fft": keeper},
        )

    def detour_copy(chunk):
        return remote(
            partner.at[span(chunk)],
            detour.at[chunk],
            detour_send.at[chunk],
            detour_recv.at[chunk],
            {"band": last * (band - 1)},
        )

    def onward_copy(chunk):
        return remote(
            detour.at[chunk],
            partner_grid.at[window(rank, chunk)],
            onward_send.at[chunk],
            partner_recv.at[rank, chunk],
            {"fft": ranks // 2 + band // last},
        )

    def chain_copy(way, turn_to, chunk):
        place = partner_grid.at[window(slabs[turn_to], chunk)]
        return remote(
            place,
            place,
            chain_send.at[way, turn_to, chunk],
            partner_recv.at[slabs[turn_to], chunk],
            {"band": band + 1 - 2 * way},
        )

    def passes(way, turn_to):
        if way == 0:
            go = both(band >= home, band < last)
            short = both(band == last - 1, rank == ranks - 1)
        else:
            go = both(band <= home, band > 0)
            short = both(band == 1, rank == ranks // 2)
        return both(go, jnp.logical_not(short)) if turn_to > 1 else go

    def arrive(turn_to, chunk):
        def wait():
            chain_copy(0, turn_to, chunk).wait_recv()

        if turn_to:
            wait()
        else:
            pl.when(jnp.logical_not(at_home))(wait)

    def step(turn_to, chunk):
        arrive(turn_to, chunk)
        for way in (0, 1):

            @pl.when(passes(way, turn_to))
            def _():
                chain_copy(way, turn_to, chunk).start()

    tail = [(turn_to, half) for half in range(halves_count) for turn_to in (2, 3)]

    def of_half(half):
        return range(half * per_group, (half + 1) * per_group)

    partner_load.wait()
    for chunk in range(chunks):

        @pl.when(jnp.logical_not(at_home))
        def _():
            gather_copy(chunk).start()

        @pl.when(gives_detour)
        def _():
            detour_copy(chunk).start()

    @pl.when(at_home)
    def _():
        home_load.wait()

    own_slab.wait()
    own_orbital = orbital_grid.at[slab(rank)]
    to_across = remote(own_orbital, own_orbital, grid_send.at[0], grid_recv.at[0], {"fft": across})
    to_beside = remote(own_orbital, own_orbital, grid_send.at[1], grid_recv.at[1], {"fft": beside})
    other_orbital = orbital_grid.at[slab(across)]
    onward = remote(
        other_orbital, other_orbital, grid_send.at[2], grid_recv.at[2], {"fft": beside}
    )
    to_across.start()
    to_beside.start()

    def take_detour(condition, chunk):
        @pl.when(both(takes_detour, condition))
        def _():
            detour_copy(chunk).wait_recv()
            onward_copy(chunk).start()

    for turn_to in (0, 1):
        for chunk in range(chunks):
            step(turn_to, chunk)
            if turn_to == 1:
                take_detour(jnp.logical_not(at_home), chunk)

    def other_copy(slot, where, source=own_orbital):
        return remote(
            source,
            others.at[slot],
            other_send.at[slot, where],
            other_recv.at[slot],
            {"band": where},
        )

    def forward(group):
        forward_group(group, orbital_grid, partner_grid, work, right_forward, left_forward)

    def forward_near(index):
        forward(
            (rank + index // halves_count * (beside - rank)) * halves_count + index % halves_count
        )

    for load in table_loads:
        load.wait()
    to_beside.wait_recv()

    @pl.when(early)
    def _():
        for number, (turn_to, half) in enumerate(tail):
            for chunk in of_half(half):
                if turn_to == 2:
                    take_detour(at_home, chunk)
            if number == len(tail) - 1:

                @pl.when(jnp.logical_not(at_home))
                def _():
                    to_across.wait_recv()
                    onward.start()

            for chunk in of_half(half):
                step(turn_to, chunk)
            forward_near(number)

    @pl.when(band == 2)
    def _():
        other_copy(0, 1).start()

    @pl.when(band == last)
    def _():
        other_copy(1, 2).start()

    @pl.when(either(at_home, at_end))
    def _():
        to_across.wait_recv()
        onward.start()

    @pl.when(jnp.logical_not(early))
    def _():
        def one_group(index, carry):
            forward_near(index)
            return carry

        lax.fori_loop(0, 2 * halves_count, one_group, 0)

    onward.wait_recv()
    chosen = shift_index[home]
    fill_screen([shift_table[axis, chosen] for axis in range(3)], partial)
    for turn_to, half in tail:

        @pl.when(jnp.logical_not(early))
        def _():
            for chunk in of_half(half):
                arrive(turn_to, chunk)

        forward(slabs[turn_to] * halves_count + half)

    middle_pairs(partial, work, left_forward, left_inverse)

    @pl.when(band == 2)
    def _():
        other_copy(1, 2).wait_recv()
        other_copy(1, 1, others.at[1]).start()

    def backward(index, half):
        backward_group(
            index * halves_count + half, partner_grid, partial, work, right_inverse, left_inverse
        )

    def near_copy(which, index, half):
        return remote(
            partial.at[pl.ds(index * planes + half * GROUP, GROUP)],
            near.at[which, pl.ds(half * GROUP, GROUP)],
            near_send.at[which, half],
            near_recv.at[which, half],
            {"fft": beside},
        )

    def far_copy(cut):
        return remote(
            outgoing.at[cut_span(cut)],
            arriving.at[cut_span(cut)],
            far_send.at[cut],
            far_recv.at[cut],
            {"fft": across},
        )

    def up_copy(owner, cut, own=False):
        held = passed.at[owner, cut_span(cut)]
        return remote(
            potential.at[cut_span(cut)] if own else held,
            held,
            up_send.at[owner, cut],
            up_recv.at[owner, cut],
            {"band": band + 1},
        )

    def slice_of(index, cut):
        return pl.ds(index * planes + cut * slice_size, slice_size)

    per_half = cuts // halves_count
    for half in range(halves_count):
        backward(beside_across, half)
        near_copy(1, beside_across, half).start()
        backward(across, half)
        near_copy(1, beside_across, half).wait_recv()
        for cut in range(half * per_half, (half + 1) * per_half):
            outgoing[cut_span(cut)] = partial[slice_of(across, cut)] + near[1, cut_span(cut)]
            far_copy(cut).start()
    for half in range(halves_count):
        backward(beside, half)
        near_copy(0, beside, half).start()
    for half in range(halves_count):
        backward(rank, half)

    zero = jnp.zeros((8, lanes), jnp.float32)
    for number in range(tallies.shape[0]):
        tallies[number] = zero

    def inner(pairs, right, start, stop):
        slots = [2 * slot + half for slot, _ in pairs for half in range(2)]

        def accumulate(plane, sums):
            straight = right(plane)
            sides = (straight, turn(straight))
            values = [left(plane) for _, left in pairs]
            return tuple(
                running
                + jnp.sum((values[n // 2] * sides[n % 2]).reshape(rows // 8, 8, lanes), axis=0)
                for n, running in enumerate(sums)
            )

        sums = lax.fori_loop(start, stop, accumulate, tuple(tallies[slot] for slot in slots))
        for slot, value in zip(slots, sums):
            tallies[slot] = value

    def own_potential(plane):
        return potential[plane]

    def first_potential(plane):
        return passed[0, plane]

    def own_values(plane):
        return orbital_grid[rank * planes + plane]

    def other_values(slot):
        return lambda plane: others[slot, plane]

    for cut in range(cuts):
        if cut % per_half == 0:
            near_copy(0, beside, cut // per_half).wait_recv()
        far_copy(cut).wait_recv()
        potential[cut_span(cut)] = (
            partial[slice_of(rank, cut)] + near[0, cut_span(cut)]
        ) + arriving[cut_span(cut)]

        @pl.when(band < last - 1 if cut >= direct else band < last)
        def _():
            up_copy(band, cut, True).start()

        inner([(0, own_values)], own_potential, cut * slice_size, (cut + 1) * slice_size)

    @pl.when(band == 1)
    def _():
        other_copy(0, 1).wait_recv()
        other_copy(1, 1).wait_recv()
        inner([(1, other_values(0)), (2, other_values(1))], own_potential, 0, planes)
        for cut in range(cuts):
            up_copy(0, cut).wait_recv()
            up_copy(0, cut).start()
            inner(
                [(3, own_values), (4, other_values(0)), (5, other_values(1))],
                first_potential,
                cut * slice_size,
                (cut + 1) * slice_size,
            )

    @pl.when(band == 2)
    def _():
        inner([(2, other_values(1))], own_potential, 0, planes)

    entries = [(i, l) for i in range(bands) for l in range(i + 1)]
    places = (
        band * (band + 1) // 2 + band,
        entries.index((2, 1)),
        entries.index((last, 0)) + band,
        entries.index((1, 0)),
        entries.index((2, 0)),
        entries.index((last, 0)),
    )
    position = lax.broadcasted_iota(jnp.int32, (8, lanes), 1)
    packed = zero
    for slot, place in enumerate(places):
        for half in range(2):
            value = jnp.sum(tallies[2 * slot + half], axis=1, keepdims=True)
            packed = packed + jnp.where(position == 2 * place + half, value, 0.0)
    own_sums[...] = packed
    sum_copies = []
    for step_by in range(bands):
        for turn_by in range(ranks):
            if step_by == 0 and turn_by == 0:
                continue
            copy = remote(
                own_sums,
                all_sums.at[band, rank],
                sum_send.at[step_by, turn_by],
                sum_recv.at[step_by, turn_by],
                {"band": (band + step_by) % bands, "fft": (rank + turn_by) % ranks},
            )
            copy.start()
            sum_copies.append(copy)
    all_sums[band, rank] = packed

    @pl.when(band == 2)
    def _():
        for member in (1, 0):
            for cut in range(direct):
                up_copy(member, cut).wait_recv()
                up_copy(member, cut).start()

    for copy in sum_copies:
        copy.wait()
    total = zero
    for one_band in range(bands):
        for one_rank in range(ranks):
            total = total + all_sums[one_band, one_rank]
    total = jnp.broadcast_to(jnp.sum(total, axis=0, keepdims=True), (8, lanes))
    volume = float(lanes // 2) * float(rows) * float(planes * ranks)
    matrix = [[None] * bands for _ in range(bands)]
    for number, (i, l) in enumerate(entries):
        values = [
            jnp.broadcast_to(
                jnp.sum(jnp.where(position == 2 * number + half, total, 0.0), axis=1, keepdims=True),
                (8, lanes),
            )
            / volume
            for half in range(2)
        ]
        matrix[i][l] = (values[0], values[1])
    inverse = small_factor_inverse(matrix)

    def combine(row, own, members, start, stop, put):
        def one_plane(plane, carry):
            sum_straight = jnp.zeros((rows, lanes), jnp.float32)
            sum_turned = jnp.zeros((rows, lanes), jnp.float32)
            for m in members:
                block = potential[plane] if m is None else passed[m, plane]
                real, imag = inverse[row][own if m is None else m]
                sum_straight = sum_straight + real[:1] * block
                sum_turned = sum_turned + imag[:1] * block
            put(plane, sum_straight + turn(sum_turned))
            return carry

        lax.fori_loop(start, stop, one_plane, 0)

    def put_whole(plane, value):
        projector[plane] = value

    def put_more(plane, value):
        projector[plane] = projector[plane] + value

    def put_lifted(plane, value):
        passed[2, plane] = value

    for row in range(2):

        @pl.when(band == row)
        def _():
            combine(row, row, [None, 0][: row + 1], 0, planes, put_whole)

    @pl.when(band == 2)
    def _():
        for cut in range(direct, cuts):
            up_copy(1, cut).wait_recv()
        for cut in range(direct, cuts):
            up_copy(0, cut).wait_recv()
            combine(
                last, 2, (0, 1, None), cut * slice_size, (cut + 1) * slice_size, put_lifted
            )
            up_copy(2, cut).start()
        combine(2, 2, (0, 1, None), 0, planes, put_whole)

    @pl.when(band == last)
    def _():
        for member in (2, 1):
            for cut in range(direct):
                up_copy(member, cut).wait_recv()
        combine(last, last, (1, 2, None), 0, direct * slice_size, put_whole)
        combine(last, last, (None,), direct * slice_size, planes, put_whole)
        for cut in range(direct):
            up_copy(0, cut).wait_recv()
            combine(last, last, (0,), cut * slice_size, (cut + 1) * slice_size, put_more)
        for cut in range(direct, cuts):
            up_copy(2, cut).wait_recv()
            projector[cut_span(cut)] = projector[cut_span(cut)] + passed[2, cut_span(cut)]

    for chunk in range(chunks):

        @pl.when(jnp.logical_not(at_home))
        def _():
            gather_copy(chunk).wait_send()

        @pl.when(gives_detour)
        def _():
            detour_copy(chunk).wait_send()

        @pl.when(takes_detour)
        def _():
            onward_copy(chunk).wait_send()

        for turn_to in range(len(slabs)):
            for way in (0, 1):

                @pl.when(passes(way, turn_to))
                def _():
                    chain_copy(way, turn_to, chunk).wait_send()

    for cut in range(cuts):
        far_copy(cut).wait_send()

        @pl.when(band < last)
        def _():
            up_copy(band, cut, True).wait_send()

        if cut < direct:

            @pl.when(band == 2)
            def _():
                up_copy(1, cut).wait_send()

        @pl.when(band == 1 if cut >= direct else either(band == 1, band == 2))
        def _():
            up_copy(0, cut).wait_send()

    @pl.when(band == 2)
    def _():
        other_copy(0, 1).wait_send()
        other_copy(1, 1).wait_send()

    @pl.when(band == last)
    def _():
        other_copy(1, 2).wait_send()

    for half in range(halves_count):
        near_copy(0, beside, half).wait_send()
        near_copy(1, beside_across, half).wait_send()
    to_across.wait_send()
    to_beside.wait_send()
    onward.wait_send()


def exchange(bands, ranks, orbital, partner, shift_table, shift_index):
    planes, rows, lanes = orbital.shape
    chunks = bands
    halves_count = planes // GROUP
    vmem = pl.BlockSpec(memory_space=pltpu.VMEM)
    smem = pl.BlockSpec(memory_space=pltpu.SMEM)
    out = pltpu.VMEM((planes, rows, lanes), jnp.float32)
    grid = pltpu.VMEM((ranks * planes, rows, lanes), jnp.float32)
    slab = pltpu.VMEM((planes, rows, lanes), jnp.float32)
    quarters = pltpu.VMEM((chunks, planes // chunks, rows, lanes), jnp.float32)

    def slab_list(count):
        return pltpu.VMEM((count, planes, rows, lanes), jnp.float32)

    dma = pltpu.SemaphoreType.DMA
    tables = [
        jnp.asarray(table)
        for table in (
            right_table(rows, -1.0),
            right_table(rows, 1.0),
            left_table(rows, -1.0),
            left_table(rows, 1.0),
        )
    ]
    return pl.pallas_call(
        functools.partial(exchange_kernel, bands, ranks),
        name="exchange",
        out_shape=(out, out),
        in_specs=[smem, smem] + [pl.BlockSpec(memory_space=pl.ANY)] * 6,
        out_specs=(vmem, vmem),
        scratch_shapes=[
            grid,
            grid,
            grid,
            grid,
            slab,
            quarters,
            slab_list(2),
            slab,
            slab,
            slab_list(bands - 1),
            slab_list(2),
            pltpu.VMEM((12, 8, lanes), jnp.float32),
            pltpu.VMEM((8, lanes), jnp.float32),
            pltpu.VMEM((bands, ranks, 8, lanes), jnp.float32),
        ]
        + [pltpu.VMEM(table.shape, table.dtype) for table in tables]
        + [
            dma((7,)),
            dma((chunks,)),
            dma((chunks,)),
            dma((chunks,)),
            dma((chunks,)),
            dma((2, ranks, chunks)),
            dma((ranks, chunks)),
            dma((3,)),
            dma((3,)),
            dma((2, bands)),
            dma((2,)),
            dma((2, halves_count)),
            dma((2, halves_count)),
            dma((2 * chunks,)),
            dma((2 * chunks,)),
            dma((bands, 2 * chunks)),
            dma((bands, 2 * chunks)),
            dma((bands, ranks)),
            dma((bands, ranks)),
        ],
        compiler_params=pltpu.CompilerParams(
            collective_id=0, has_side_effects=True, vmem_limit_bytes=60 * 1024 * 1024
        ),
    )(shift_table.T, shift_index, orbital, partner, *tables)


def paired_body(bands, ranks, orbitals, partners, shift_table, shift_index):
    potential, projector = exchange(
        bands, ranks, orbitals[0], partners[0], shift_table, shift_index
    )
    return (potential[None], projector[None])


def body(orbitals, partners, shift_table, shift_index):
    bands = lax.axis_size("band")
    ranks = lax.axis_size("fft")
    count, planes, rows, lanes = orbitals.shape
    grid_bytes = ranks * planes * rows * lanes * 4
    paired = (
        count == 1
        and ranks == 4
        and bands == ranks
        and planes % (2 * bands) == 0
        and planes % GROUP == 0
        and GROUP % (planes // bands) == 0
        and lanes == 2 * rows
        and lanes == 128
        and grid_bytes <= 2 * 1024 * 1024
    )
    if paired:
        return paired_body(bands, ranks, orbitals, partners, shift_table, shift_index)
    return general_body(orbitals, partners, shift_table, shift_index)


def solution(mesh):
    in_specs = (
        P(("kgrp", "band"), "fft", None, None),
        P(("kgrp", "band"), "fft", None, None),
        P(),
        P("kgrp"),
    )
    out_specs = (P(("kgrp", "band"), "fft", None, None), P(("kgrp", "band"), "fft", None, None))
    return jax.shard_map(body, mesh=mesh, in_specs=in_specs, out_specs=out_specs, check_vma=False)
```

```python
import functools
import math

import jax
import jax.numpy as jnp
import numpy as np
from jax import lax
from jax.experimental import pallas as pl
from jax.experimental.pallas import tpu as pltpu
from jax.sharding import PartitionSpec as P

HIGHEST = lax.Precision.HIGHEST
HIGH = lax.Precision.HIGH
MESH = pl.DeviceIdType.MESH
GROUP = 8
SCREEN_SQUARE = 0.25
FOUR_PI = 4.0 * math.pi


def angle_pair(extent, sign):
    positions = jnp.arange(extent, dtype=jnp.int32)
    product = positions[:, None] * positions[None, :] % extent
    angle = 2.0 * math.pi / extent * product.astype(jnp.float32)
    return (jnp.cos(angle), sign * jnp.sin(angle))


def last_table(extent, sign):
    cosine, sine = angle_pair(extent, sign)
    upper = jnp.concatenate([cosine, sine], axis=1)
    lower = jnp.concatenate([-sine, cosine], axis=1)
    return jnp.concatenate([upper, lower], axis=0)


def middle_table(extent, sign):
    cosine, sine = angle_pair(extent, sign)
    return jnp.stack([jnp.stack([cosine, -sine], -1), jnp.stack([sine, cosine], -1)], 1)


def along_last(field, table):
    shape = field.shape
    flat = field.reshape(-1, shape[-1])
    return jnp.dot(flat, table, precision=HIGH).reshape(shape)


def along_axis(field, table, axis_number):
    shape = field.shape
    extent = shape[-1] // 2
    split = field.reshape(shape[0], shape[1], shape[2], 2, extent)
    if axis_number == 1:
        result = jnp.einsum("kcnd,pnbdz->pkbcz", table, split, precision=HIGH)
    else:
        result = jnp.einsum("kcnd,pandz->pakcz", table, split, precision=HIGH)
    return result.reshape(shape)


def times_conj(left, right):
    extent = left.shape[-1] // 2
    left_real, left_imag = (left[..., :extent], left[..., extent:])
    right_real, right_imag = (right[..., :extent], right[..., extent:])
    return jnp.concatenate(
        [
            left_real * right_real + left_imag * right_imag,
            left_real * right_imag - left_imag * right_real,
        ],
        axis=-1,
    )


def times(left, right):
    extent = left.shape[-1] // 2
    left_real, left_imag = (left[..., :extent], left[..., extent:])
    right_real, right_imag = (right[..., :extent], right[..., extent:])
    return jnp.concatenate(
        [
            left_real * right_real - left_imag * right_imag,
            left_real * right_imag + left_imag * right_real,
        ],
        axis=-1,
    )


def rotate(field):
    extent = field.shape[-1] // 2
    return jnp.concatenate([field[..., extent:], -field[..., :extent]], axis=-1)


def frequency(positions, extent):
    return jnp.where(positions < extent // 2, positions, positions - extent).astype(jnp.float32)


def kernel_block(qvectors, y_count, extent):
    first_freq = frequency(jnp.arange(extent, dtype=jnp.int32), extent)
    second_freq = frequency(jnp.arange(y_count, dtype=jnp.int32), extent)
    third_freq = frequency(jnp.arange(2 * extent, dtype=jnp.int32) % extent, extent)
    first_part = (first_freq[None, :] + qvectors[:, 0:1]) ** 2
    second_part = (second_freq[None, :] + qvectors[:, 1:2]) ** 2
    third_part = (third_freq[None, :] + qvectors[:, 2:3]) ** 2
    denominator = (
        first_part[:, :, None, None]
        + second_part[:, None, :, None]
        + third_part[:, None, None, :]
        + SCREEN_SQUARE
    )
    return FOUR_PI / extent**3 / denominator


def shifts_for(shift_table, shift_index, start_at, length):
    picked = lax.dynamic_slice_in_dim(shift_index, start_at, length)
    onehot = (picked[:, None] == jnp.arange(shift_table.shape[0], dtype=jnp.int32)[None, :]).astype(
        jnp.float32
    )
    return jnp.dot(onehot, shift_table, precision=HIGHEST)


def factor_inverse(over_real, over_imag):
    matrix_order = over_real.shape[0]
    positions = jnp.arange(matrix_order, dtype=jnp.int32)
    zero_start = jnp.zeros_like(over_real)

    def chol_step(column, lowers):
        lower_real, lower_imag = lowers
        row_real = lower_real[column]
        row_imag = lower_imag[column]
        resid_real = over_real[:, column] - (
            jnp.dot(lower_real, row_real, precision=HIGHEST)
            + jnp.dot(lower_imag, row_imag, precision=HIGHEST)
        )
        resid_imag = over_imag[:, column] - (
            jnp.dot(lower_imag, row_real, precision=HIGHEST)
            - jnp.dot(lower_real, row_imag, precision=HIGHEST)
        )
        pivot_value = jnp.sqrt(resid_real[column])
        below_diag = positions > column
        at_diag = positions == column
        new_real = jnp.where(
            below_diag, resid_real / pivot_value, jnp.where(at_diag, pivot_value, 0.0)
        )
        new_imag = jnp.where(below_diag, resid_imag / pivot_value, 0.0)
        chosen = positions[None, :] == column
        return (
            jnp.where(chosen, new_real[:, None], lower_real),
            jnp.where(chosen, new_imag[:, None], lower_imag),
        )

    lower_real, lower_imag = lax.fori_loop(0, matrix_order, chol_step, (zero_start, zero_start))

    def solve_step(row_index, inverses):
        inv_real, inv_imag = inverses
        row_real = lower_real[row_index]
        row_imag = lower_imag[row_index]
        sum_real = jnp.dot(row_real, inv_real, precision=HIGHEST) - jnp.dot(
            row_imag, inv_imag, precision=HIGHEST
        )
        sum_imag = jnp.dot(row_real, inv_imag, precision=HIGHEST) + jnp.dot(
            row_imag, inv_real, precision=HIGHEST
        )
        unit_row = (positions == row_index).astype(over_real.dtype)
        pivot_value = lower_real[row_index, row_index]
        new_real = (unit_row - sum_real) / pivot_value
        new_imag = -sum_imag / pivot_value
        chosen = positions[:, None] == row_index
        return (
            jnp.where(chosen, new_real[None, :], inv_real),
            jnp.where(chosen, new_imag[None, :], inv_imag),
        )

    return lax.fori_loop(0, matrix_order, solve_step, (zero_start, zero_start))


def general_body(orbitals, partners, shift_table, shift_index):
    extent = orbitals.shape[2]
    band_count = orbitals.shape[0]
    tables = (
        last_table(extent, -1.0),
        middle_table(extent, -1.0),
        last_table(extent, 1.0),
        middle_table(extent, 1.0),
    )
    my_band = lax.axis_index("band")
    forward_last, forward_mid, inverse_last, inverse_mid = tables
    full_orbitals = lax.all_gather(orbitals, "fft", axis=1, tiled=True)
    every_slab = lax.all_gather(partners, "band", axis=0, tiled=True)
    own_grids = lax.all_to_all(every_slab, "fft", split_axis=0, concat_axis=1, tiled=True)
    own_count = own_grids.shape[0]
    qvectors = shifts_for(shift_table, shift_index, lax.axis_index("fft") * own_count, own_count)

    def one_partner(member, running):
        single = lax.dynamic_slice_in_dim(own_grids, member, 1, 0)
        kernel = kernel_block(lax.dynamic_slice_in_dim(qvectors, member, 1, 0), extent, extent)
        density = times_conj(single, full_orbitals)
        spectrum = (
            along_axis(
                along_axis(along_last(density, forward_last), forward_mid, 2), forward_mid, 1
            )
            * kernel
        )
        field = along_last(
            along_axis(along_axis(spectrum, inverse_mid, 1), inverse_mid, 2), inverse_last
        )
        return running + times(single, field)

    partial_value = lax.fori_loop(
        0, own_count, one_partner, jnp.zeros(full_orbitals.shape, jnp.float32)
    )
    potential = lax.psum_scatter(partial_value, "fft", scatter_dimension=1, tiled=True)
    every_pot = lax.all_gather(potential, "band", axis=0, tiled=True)
    turned = rotate(every_pot)
    total_bands = every_pot.shape[0]
    flat_orbitals = orbitals.reshape(band_count, -1)
    flat_pot = every_pot.reshape(total_bands, -1)
    flat_turned = turned.reshape(total_bands, -1)
    volume = float(extent**3)
    rows_real = jnp.einsum("ik,jk->ij", flat_orbitals, flat_pot, precision=HIGHEST) / volume
    rows_imag = jnp.einsum("ik,jk->ij", flat_orbitals, flat_turned, precision=HIGHEST) / volume
    start_row = my_band * band_count
    summed_real, summed_imag = lax.psum((rows_real, rows_imag), "fft")
    over_real, over_imag = (
        lax.all_gather(summed_real, "band", axis=0, tiled=True),
        lax.all_gather(summed_imag, "band", axis=0, tiled=True),
    )
    inv_real, inv_imag = factor_inverse(over_real, over_imag)
    coef_real = lax.dynamic_slice_in_dim(inv_real, start_row, band_count, 0)
    coef_imag = lax.dynamic_slice_in_dim(inv_imag, start_row, band_count, 0)
    projector = jnp.dot(coef_real, flat_pot, precision=HIGHEST) + jnp.dot(
        coef_imag, flat_turned, precision=HIGHEST
    )
    return (potential, projector.reshape(orbitals.shape))


def remote(source, target, send_sem, recv_sem, where):
    return pltpu.make_async_remote_copy(
        src_ref=source,
        dst_ref=target,
        send_sem=send_sem,
        recv_sem=recv_sem,
        device_id=where,
        device_id_type=MESH,
    )


def greet(others):
    barrier = pltpu.get_barrier_semaphore()
    for other in others:
        pl.semaphore_signal(barrier, inc=1, device_id=other, device_id_type=MESH)
    pl.semaphore_wait(barrier, len(others))


def turn(block):
    lanes = block.shape[-1]
    swapped = pltpu.roll(block, lanes // 2, block.ndim - 1)
    position = lax.broadcasted_iota(jnp.int32, block.shape, block.ndim - 1)
    return jnp.where(position < lanes // 2, swapped, -swapped)


def small_factor_inverse(matrix):
    order = len(matrix)
    lower = [[None] * order for _ in range(order)]
    for column in range(order):
        residual = []
        for row in range(column, order):
            real, imag = matrix[row][column]
            for k in range(column):
                a, b = lower[row][k]
                c, d = lower[column][k]
                real = real - (a * c + b * d)
                imag = imag - (b * c - a * d)
            residual.append((real, imag))
        pivot = jnp.sqrt(residual[0][0])
        lower[column][column] = (pivot, jnp.zeros_like(pivot))
        for row in range(column + 1, order):
            real, imag = residual[row - column]
            lower[row][column] = (real / pivot, imag / pivot)
    inverse = [[None] * order for _ in range(order)]
    for row in range(order):
        pivot = lower[row][row][0]
        inverse[row][row] = (1.0 / pivot, jnp.zeros_like(pivot))
        for column in range(row):
            real = jnp.zeros_like(pivot)
            imag = jnp.zeros_like(pivot)
            for k in range(column, row):
                a, b = lower[row][k]
                c, d = inverse[k][column]
                real = real - (a * c - b * d)
                imag = imag - (a * d + b * c)
            inverse[row][column] = (real / pivot, imag / pivot)
    return inverse


def split_table(table):
    high = table.astype(jnp.bfloat16)
    low = (table - high.astype(np.float64)).astype(jnp.bfloat16)
    return high, low


def right_table(extent, sign):
    grid = np.outer(np.arange(extent), np.arange(extent)) % extent
    angle = 2.0 * math.pi / extent * grid
    cosine, sine = np.cos(angle), sign * np.sin(angle)
    table = np.block([[cosine, sine], [-sine, cosine]])
    high, low = split_table(table)
    upper = np.concatenate([high, low], axis=1)
    lower = np.concatenate([high, np.zeros_like(low)], axis=1)
    return np.concatenate([upper, lower], axis=0)


def left_table(extent, sign):
    grid = np.outer(np.arange(extent), np.arange(extent)) % extent
    angle = 2.0 * math.pi / extent * grid
    high, low = split_table(np.concatenate([np.cos(angle), sign * np.sin(angle)], axis=0))
    return np.concatenate([high, high, low], axis=1)


def halves(value):
    high = value.astype(jnp.bfloat16)
    low = (value - high.astype(jnp.float32)).astype(jnp.bfloat16)
    return high, low


def right_product(value, table):
    lanes = value.shape[-1]
    high, low = halves(value)
    both = jnp.dot(
        jnp.concatenate([high, low], axis=1), table, preferred_element_type=jnp.float32
    )
    return both[:, :lanes] + both[:, lanes:]


def left_product(first, second, table):
    rows, lanes = first.shape
    high, low = halves(jnp.concatenate([first, second], axis=1))
    stacked = jnp.concatenate([high, low, high], axis=0)
    both = jnp.dot(table, stacked, preferred_element_type=jnp.float32)
    return tuple(
        both[:rows, cut : cut + lanes] - turn(both[rows:, cut : cut + lanes])
        for cut in (0, lanes)
    )


def spread_parts(value):
    lanes = value.shape[-1]
    swapped = pltpu.roll(value, lanes // 2, value.ndim - 1)
    lower = lax.broadcasted_iota(jnp.int32, value.shape, value.ndim - 1) < lanes // 2
    return jnp.where(lower, value, swapped), jnp.where(lower, swapped, value)


def forward_group(group, orbital_grid, partner_grid, work, right, left):
    rows, lanes = orbital_grid.shape[1:]
    span = pl.ds(group * GROUP, GROUP)
    orbital = orbital_grid[span].reshape(GROUP * rows, lanes)
    real, imag = spread_parts(partner_grid[span].reshape(GROUP * rows, lanes))
    density = real * orbital + imag * turn(orbital)
    lines = right_product(density, right[...])
    planes = []
    for pair in range(GROUP // 2):
        start = 2 * pair * rows
        planes += left_product(
            lines[start : start + rows], lines[start + rows : start + 2 * rows], left[...]
        )
    stacked = jnp.stack(planes, axis=0)
    work[:, span, :] = jnp.swapaxes(stacked, 0, 1)


def backward_group(group, partner_grid, partial, work, right, left):
    rows, lanes = partner_grid.shape[1:]
    span = pl.ds(group * GROUP, GROUP)
    planes = jnp.swapaxes(work[:, span, :], 0, 1)
    lines = []
    for pair in range(GROUP // 2):
        lines += left_product(planes[2 * pair], planes[2 * pair + 1], left[...])
    field = right_product(jnp.concatenate(lines, axis=0), right[...])
    real, imag = spread_parts(partner_grid[span].reshape(GROUP * rows, lanes))
    partial[span] = (real * field - imag * turn(field)).reshape(GROUP, rows, lanes)


def fill_screen(shift, screen):
    columns, extent, lanes = screen.shape
    first = frequency(lax.broadcasted_iota(jnp.int32, (extent, lanes), 0), extent)
    third_place = lax.broadcasted_iota(jnp.int32, (extent, lanes), 1)
    third_place = jnp.where(third_place < lanes // 2, third_place, third_place - lanes // 2)
    third = frequency(third_place, extent)
    base = (first + shift[0]) ** 2 + (third + shift[2]) ** 2 + SCREEN_SQUARE
    scale = FOUR_PI / (float(extent) * float(columns) * float(lanes // 2))

    def one_column(column, carry):
        second = jnp.where(column < columns // 2, column, column - columns)
        offset = (second.astype(jnp.float32) + shift[1]) ** 2
        screen[column] = scale / (base + offset)
        return carry

    lax.fori_loop(0, columns, one_column, 0, unroll=2)


def middle_pairs(screen, work, forward, inverse):
    columns = work.shape[0]

    def one_pair(pair, carry):
        spectra = left_product(work[2 * pair], work[2 * pair + 1], forward[...])
        scaled = [spectra[which] * screen[2 * pair + which] for which in range(2)]
        fields = left_product(scaled[0], scaled[1], inverse[...])
        work[2 * pair] = fields[0]
        work[2 * pair + 1] = fields[1]
        return carry

    lax.fori_loop(0, columns // 2, one_pair, 0, unroll=16)


def exchange_kernel(
    bands,
    ranks,
    shift_table,
    shift_index,
    orbital_home,
    partner_home,
    right_forward_home,
    right_inverse_home,
    left_forward_home,
    left_inverse_home,
    potential,
    projector,
    orbital_grid,
    partner_grid,
    work,
    partial,
    partner,
    detour,
    near,
    outgoing,
    arriving,
    passed,
    others,
    tallies,
    own_sums,
    all_sums,
    right_forward,
    right_inverse,
    left_forward,
    left_inverse,
    load_sem,
    gather_send,
    detour_send,
    detour_recv,
    onward_send,
    chain_send,
    partner_recv,
    grid_send,
    grid_recv,
    other_send,
    other_recv,
    near_send,
    near_recv,
    far_send,
    far_recv,
    up_send,
    up_recv,
    sum_send,
    sum_recv,
):
    planes, rows, lanes = potential.shape
    chunks = bands
    piece = planes // chunks
    per_group = GROUP // piece
    halves_count = planes // GROUP
    last = bands - 1
    cuts = 2 * chunks
    slice_size = planes // cuts
    direct = 4 * cuts // 8
    lag = cuts // 4
    held_back = 2 * cuts // 8
    band = lax.axis_index("band")
    rank = lax.axis_index("fft")
    beside = rank + 1 - 2 * (rank % 2)
    across = (rank + 2) % ranks
    beside_across = (beside + 2) % ranks
    slabs = (rank, beside, across, beside_across)
    home = 2 * (rank % 2) + (rank // 2 + rank % 2) % 2
    keeper = 2 * ((band // 2 + band % 2) % 2) + band // 2

    def both(*conditions):
        return functools.reduce(jnp.logical_and, conditions)

    def either(*conditions):
        return functools.reduce(jnp.logical_or, conditions)

    at_home = band == home
    at_end = either(band == 0, band == last)
    early = either(at_home, band == 1, band == last - 1)
    low_side = rank < ranks // 2
    takes_detour = both(at_end, low_side)
    gives_detour = both(jnp.logical_not(at_end), low_side)

    def span(index):
        return pl.ds(index * piece, piece)

    def cut_span(cut):
        return pl.ds(cut * slice_size, slice_size)

    def slab(index):
        return pl.ds(index * planes, planes)

    def window(index, chunk):
        return pl.ds(index * planes + chunk * piece, piece)

    own_slab = pltpu.make_async_copy(orbital_home, orbital_grid.at[slab(rank)], load_sem.at[1])
    partner_load = pltpu.make_async_copy(partner_home, partner, load_sem.at[0])
    home_load = pltpu.make_async_copy(partner_home, partner_grid.at[slab(rank)], load_sem.at[2])
    table_loads = [
        pltpu.make_async_copy(source, here, load_sem.at[3 + number])
        for number, (source, here) in enumerate(
            (
                (right_forward_home, right_forward),
                (left_forward_home, left_forward),
                (right_inverse_home, right_inverse),
                (left_inverse_home, left_inverse),
            )
        )
    ]
    partner_load.start()

    @pl.when(at_home)
    def _():
        home_load.start()

    own_slab.start()
    for load in table_loads:
        load.start()
    greet(
        [
            {"band": (band + step) % bands, "fft": (rank + turn_by) % ranks}
            for step in range(bands)
            for turn_by in range(ranks)
            if step or turn_by
        ]
    )

    def gather_copy(chunk):
        return remote(
            partner.at[span(chunk)],
            partner_grid.at[window(rank, chunk)],
            gather_send.at[chunk],
            partner_recv.at[rank, chunk],
            {"fft": keeper},
        )

    def detour_copy(chunk):
        return remote(
            partner.at[span(chunk)],
            detour.at[chunk],
            detour_send.at[chunk],
            detour_recv.at[chunk],
            {"band": last * (band - 1)},
        )

    def onward_copy(chunk):
        return remote(
            detour.at[chunk],
            partner_grid.at[window(rank, chunk)],
            onward_send.at[chunk],
            partner_recv.at[rank, chunk],
            {"fft": ranks // 2 + band // last},
        )

    def chain_copy(way, turn_to, chunk):
        place = partner_grid.at[window(slabs[turn_to], chunk)]
        return remote(
            place,
            place,
            chain_send.at[way, turn_to, chunk],
            partner_recv.at[slabs[turn_to], chunk],
            {"band": band + 1 - 2 * way},
        )

    def passes(way, turn_to):
        if way == 0:
            go = both(band >= home, band < last)
            short = both(band == last - 1, rank == ranks - 1)
        else:
            go = both(band <= home, band > 0)
            short = both(band == 1, rank == ranks // 2)
        return both(go, jnp.logical_not(short)) if turn_to > 1 else go

    def arrive(turn_to, chunk):
        def wait():
            chain_copy(0, turn_to, chunk).wait_recv()

        if turn_to:
            wait()
        else:
            pl.when(jnp.logical_not(at_home))(wait)

    def step(turn_to, chunk):
        arrive(turn_to, chunk)
        for way in (0, 1):

            @pl.when(passes(way, turn_to))
            def _():
                chain_copy(way, turn_to, chunk).start()

    tail = [(turn_to, half) for half in range(halves_count) for turn_to in (2, 3)]

    def of_half(half):
        return range(half * per_group, (half + 1) * per_group)

    partner_load.wait()
    for chunk in range(chunks):

        @pl.when(jnp.logical_not(at_home))
        def _():
            gather_copy(chunk).start()

        @pl.when(gives_detour)
        def _():
            detour_copy(chunk).start()

    @pl.when(at_home)
    def _():
        home_load.wait()

    own_slab.wait()
    own_orbital = orbital_grid.at[slab(rank)]
    to_across = remote(own_orbital, own_orbital, grid_send.at[0], grid_recv.at[0], {"fft": across})
    to_beside = remote(own_orbital, own_orbital, grid_send.at[1], grid_recv.at[1], {"fft": beside})
    other_orbital = orbital_grid.at[slab(across)]
    onward = remote(
        other_orbital, other_orbital, grid_send.at[2], grid_recv.at[2], {"fft": beside}
    )
    to_across.start()
    to_beside.start()

    def take_detour(condition, chunk):
        @pl.when(both(takes_detour, condition))
        def _():
            detour_copy(chunk).wait_recv()
            onward_copy(chunk).start()

    for turn_to in (0, 1):
        for chunk in range(chunks):
            step(turn_to, chunk)
            if turn_to == 1:
                take_detour(jnp.logical_not(at_home), chunk)

    def other_copy(slot, where, source=own_orbital):
        return remote(
            source,
            others.at[slot],
            other_send.at[slot, where],
            other_recv.at[slot],
            {"band": where},
        )

    def forward(group):
        forward_group(group, orbital_grid, partner_grid, work, right_forward, left_forward)

    def forward_near(index):
        forward(
            (rank + index // halves_count * (beside - rank)) * halves_count + index % halves_count
        )

    def tabulate():
        chosen = shift_index[home]
        fill_screen([shift_table[axis, chosen] for axis in range(3)], partial)

    for load in table_loads:
        load.wait()
    to_beside.wait_recv()

    @pl.when(early)
    def _():
        for number, (turn_to, half) in enumerate(tail):
            for chunk in of_half(half):
                if turn_to == 2:
                    take_detour(at_home, chunk)
            if number == len(tail) - 2:

                @pl.when(jnp.logical_not(at_home))
                def _():
                    to_across.wait_recv()
                    onward.start()

            for chunk in of_half(half):
                step(turn_to, chunk)
            forward_near(number)
            if number == 1:
                tabulate()

    @pl.when(band == 2)
    def _():
        other_copy(0, 1).start()

    @pl.when(band == last)
    def _():
        other_copy(1, 2).start()

    @pl.when(either(at_home, at_end))
    def _():
        to_across.wait_recv()
        onward.start()

    @pl.when(jnp.logical_not(early))
    def _():
        def one_group(index, carry):
            forward_near(index)
            return carry

        lax.fori_loop(0, 2 * halves_count, one_group, 0)
        tabulate()

    onward.wait_recv()
    for turn_to, half in tail:

        @pl.when(jnp.logical_not(early))
        def _():
            for chunk in of_half(half):
                arrive(turn_to, chunk)

        forward(slabs[turn_to] * halves_count + half)

    middle_pairs(partial, work, left_forward, left_inverse)

    @pl.when(band == 2)
    def _():
        other_copy(1, 2).wait_recv()
        other_copy(1, 1, others.at[1]).start()

    def backward(index, half):
        backward_group(
            index * halves_count + half, partner_grid, partial, work, right_inverse, left_inverse
        )

    def near_copy(which, index, half):
        return remote(
            partial.at[pl.ds(index * planes + half * GROUP, GROUP)],
            near.at[which, pl.ds(half * GROUP, GROUP)],
            near_send.at[which, half],
            near_recv.at[which, half],
            {"fft": beside},
        )

    def far_copy(cut):
        return remote(
            outgoing.at[cut_span(cut)],
            arriving.at[cut_span(cut)],
            far_send.at[cut],
            far_recv.at[cut],
            {"fft": across},
        )

    def up_copy(owner, cut, own=False):
        held = passed.at[owner, cut_span(cut)]
        return remote(
            potential.at[cut_span(cut)] if own else held,
            held,
            up_send.at[owner, cut],
            up_recv.at[owner, cut],
            {"band": band + 1},
        )

    def slice_of(index, cut):
        return pl.ds(index * planes + cut * slice_size, slice_size)

    per_half = cuts // halves_count
    def halves_of_cuts(half):
        return range(half * per_half, (half + 1) * per_half)

    def send_half(half):
        backward(beside_across, half)
        near_copy(1, beside_across, half).start()
        backward(across, half)
        near_copy(1, beside_across, half).wait_recv()
        for cut in halves_of_cuts(half):
            outgoing[cut_span(cut)] = partial[slice_of(across, cut)] + near[1, cut_span(cut)]
            far_copy(cut).start()
        backward(beside, half)
        near_copy(0, beside, half).start()

    zero = jnp.zeros((8, lanes), jnp.float32)
    for number in range(tallies.shape[0]):
        tallies[number] = zero

    def inner(pairs, right, start, stop):
        slots = [2 * slot + half for slot, _ in pairs for half in range(2)]

        def accumulate(plane, sums):
            straight = right(plane)
            sides = (straight, turn(straight))
            values = [left(plane) for _, left in pairs]
            return tuple(
                running
                + jnp.sum((values[n // 2] * sides[n % 2]).reshape(rows // 8, 8, lanes), axis=0)
                for n, running in enumerate(sums)
            )

        sums = lax.fori_loop(
            start,
            stop,
            accumulate,
            tuple(tallies[slot] for slot in slots),
            unroll=min(4, stop - start),
        )
        for slot, value in zip(slots, sums):
            tallies[slot] = value

    def own_potential(plane):
        return potential[plane]

    def first_potential(plane):
        return passed[0, plane]

    def own_values(plane):
        return orbital_grid[rank * planes + plane]

    def other_values(slot):
        return lambda plane: others[slot, plane]

    def finish(cut):
        far_copy(cut).wait_recv()
        potential[cut_span(cut)] = (
            partial[slice_of(rank, cut)] + near[0, cut_span(cut)]
        ) + arriving[cut_span(cut)]

        @pl.when(band < last - 1 if cut >= direct else band < last)
        def _():
            up_copy(band, cut, True).start()

        inner([(0, own_values)], own_potential, cut * slice_size, (cut + 1) * slice_size)
        if 0 <= cut - lag < direct:

            @pl.when(band == 2)
            def _():
                lift_on(1, cut - lag)

    def lift_on(member, cut):
        up_copy(member, cut).wait_recv()
        up_copy(member, cut).start()

    for half in range(halves_count):
        send_half(half)
        if half == 0:
            backward(rank, half)
            near_copy(0, beside, half).wait_recv()
            continue
        for number, cut in enumerate(halves_of_cuts(half - 1)):
            finish(cut)
            if number == per_half // 2 - 1:
                backward(rank, half)
        near_copy(0, beside, half).wait_recv()
    for cut in halves_of_cuts(halves_count - 1):
        finish(cut)

    @pl.when(band == 1)
    def _():
        def pass_on(cut):
            up_copy(0, cut).wait_recv()
            if cut < cuts - held_back:
                up_copy(0, cut).start()

        def with_first(start, stop):
            inner(
                [(3, own_values), (4, other_values(0)), (5, other_values(1))],
                first_potential,
                start * slice_size,
                stop * slice_size,
            )

        for cut in range(per_half):
            pass_on(cut)
        other_copy(0, 1).wait_recv()
        other_copy(1, 1).wait_recv()
        inner([(1, other_values(0)), (2, other_values(1))], own_potential, 0, planes)
        with_first(0, per_half)
        for cut in range(per_half, cuts):
            pass_on(cut)
            with_first(cut, cut + 1)

    @pl.when(band == 2)
    def _():
        inner([(2, other_values(1))], own_potential, 0, planes)

    entries = [(i, l) for i in range(bands) for l in range(i + 1)]
    places = (
        band * (band + 1) // 2 + band,
        entries.index((2, 1)),
        entries.index((last, 0)) + band,
        entries.index((1, 0)),
        entries.index((2, 0)),
        entries.index((last, 0)),
    )
    position = lax.broadcasted_iota(jnp.int32, (8, lanes), 1)
    packed = zero
    for slot, place in enumerate(places):
        for half in range(2):
            value = jnp.sum(tallies[2 * slot + half], axis=1, keepdims=True)
            packed = packed + jnp.where(position == 2 * place + half, value, 0.0)
    own_sums[...] = packed
    sum_copies = []
    for step_by in range(bands):
        for turn_by in range(ranks):
            if step_by == 0 and turn_by == 0:
                continue
            copy = remote(
                own_sums,
                all_sums.at[band, rank],
                sum_send.at[step_by, turn_by],
                sum_recv.at[step_by, turn_by],
                {"band": (band + step_by) % bands, "fft": (rank + turn_by) % ranks},
            )
            copy.start()
            sum_copies.append(copy)
    all_sums[band, rank] = packed

    @pl.when(band == 1)
    def _():
        for cut in range(cuts - held_back, cuts):
            up_copy(0, cut).start()

    @pl.when(band == 2)
    def _():
        for cut in range(cuts - lag, direct):
            lift_on(1, cut)
        for cut in range(direct):
            lift_on(0, cut)

    for chunk in range(chunks):

        @pl.when(jnp.logical_not(at_home))
        def _():
            gather_copy(chunk).wait_send()

        @pl.when(gives_detour)
        def _():
            detour_copy(chunk).wait_send()

        @pl.when(takes_detour)
        def _():
            onward_copy(chunk).wait_send()

        for turn_to in range(len(slabs)):
            for way in (0, 1):

                @pl.when(passes(way, turn_to))
                def _():
                    chain_copy(way, turn_to, chunk).wait_send()

    @pl.when(band == 2)
    def _():
        other_copy(0, 1).wait_send()
        other_copy(1, 1).wait_send()

    @pl.when(band == last)
    def _():
        other_copy(1, 2).wait_send()

    for half in range(halves_count):
        near_copy(0, beside, half).wait_send()
        near_copy(1, beside_across, half).wait_send()
    to_across.wait_send()
    to_beside.wait_send()
    onward.wait_send()

    for cut in range(cuts):
        far_copy(cut).wait_send()

    for copy in sum_copies:
        copy.wait()
    total = zero
    for one_band in range(bands):
        for one_rank in range(ranks):
            total = total + all_sums[one_band, one_rank]
    total = jnp.broadcast_to(jnp.sum(total, axis=0, keepdims=True), (8, lanes))
    volume = float(lanes // 2) * float(rows) * float(planes * ranks)
    matrix = [[None] * bands for _ in range(bands)]
    for number, (i, l) in enumerate(entries):
        values = [
            jnp.broadcast_to(
                jnp.sum(jnp.where(position == 2 * number + half, total, 0.0), axis=1, keepdims=True),
                (8, lanes),
            )
            / volume
            for half in range(2)
        ]
        matrix[i][l] = (values[0], values[1])
    inverse = small_factor_inverse(matrix)

    def combine(row, own, members, start, stop, put):
        def one_plane(plane, carry):
            sum_straight = jnp.zeros((rows, lanes), jnp.float32)
            sum_turned = jnp.zeros((rows, lanes), jnp.float32)
            for m in members:
                block = potential[plane] if m is None else passed[m, plane]
                real, imag = inverse[row][own if m is None else m]
                sum_straight = sum_straight + real[:1] * block
                sum_turned = sum_turned + imag[:1] * block
            put(plane, sum_straight + turn(sum_turned))
            return carry

        lax.fori_loop(start, stop, one_plane, 0, unroll=min(4, stop - start))

    def put_whole(plane, value):
        projector[plane] = value

    def put_more(plane, value):
        projector[plane] = projector[plane] + value

    def put_lifted(plane, value):
        passed[2, plane] = value

    for row in range(2):

        @pl.when(band == row)
        def _():
            combine(row, row, [None, 0][: row + 1], 0, planes, put_whole)

    @pl.when(band == 2)
    def _():
        for cut in range(direct, cuts):
            up_copy(1, cut).wait_recv()
        for cut in range(direct, cuts):
            up_copy(0, cut).wait_recv()
            combine(
                last, 2, (0, 1, None), cut * slice_size, (cut + 1) * slice_size, put_lifted
            )
            up_copy(2, cut).start()
        combine(2, 2, (0, 1, None), 0, planes, put_whole)

    @pl.when(band == last)
    def _():
        for member in (2, 1):
            for cut in range(direct):
                up_copy(member, cut).wait_recv()
        combine(last, last, (1, 2, None), 0, direct * slice_size, put_whole)
        combine(last, last, (None,), direct * slice_size, planes, put_whole)
        for cut in range(direct):
            up_copy(0, cut).wait_recv()
            combine(last, last, (0,), cut * slice_size, (cut + 1) * slice_size, put_more)
        for cut in range(direct, cuts):
            up_copy(2, cut).wait_recv()
            projector[cut_span(cut)] = projector[cut_span(cut)] + passed[2, cut_span(cut)]

    for cut in range(cuts):
        @pl.when(band < last)
        def _():
            up_copy(band, cut, True).wait_send()

        if cut < direct:

            @pl.when(band == 2)
            def _():
                up_copy(1, cut).wait_send()

        @pl.when(band == 1 if cut >= direct else either(band == 1, band == 2))
        def _():
            up_copy(0, cut).wait_send()


def exchange(bands, ranks, orbital, partner, shift_table, shift_index):
    planes, rows, lanes = orbital.shape
    chunks = bands
    halves_count = planes // GROUP
    vmem = pl.BlockSpec(memory_space=pltpu.VMEM)
    smem = pl.BlockSpec(memory_space=pltpu.SMEM)
    out = pltpu.VMEM((planes, rows, lanes), jnp.float32)
    grid = pltpu.VMEM((ranks * planes, rows, lanes), jnp.float32)
    slab = pltpu.VMEM((planes, rows, lanes), jnp.float32)
    quarters = pltpu.VMEM((chunks, planes // chunks, rows, lanes), jnp.float32)

    def slab_list(count):
        return pltpu.VMEM((count, planes, rows, lanes), jnp.float32)

    dma = pltpu.SemaphoreType.DMA
    tables = [
        jnp.asarray(table)
        for table in (
            right_table(rows, -1.0),
            right_table(rows, 1.0),
            left_table(rows, -1.0),
            left_table(rows, 1.0),
        )
    ]
    return pl.pallas_call(
        functools.partial(exchange_kernel, bands, ranks),
        name="exchange",
        out_shape=(out, out),
        in_specs=[smem, smem] + [pl.BlockSpec(memory_space=pl.ANY)] * 6,
        out_specs=(vmem, vmem),
        scratch_shapes=[
            grid,
            grid,
            grid,
            grid,
            slab,
            quarters,
            slab_list(2),
            slab,
            slab,
            slab_list(bands - 1),
            slab_list(2),
            pltpu.VMEM((12, 8, lanes), jnp.float32),
            pltpu.VMEM((8, lanes), jnp.float32),
            pltpu.VMEM((bands, ranks, 8, lanes), jnp.float32),
        ]
        + [pltpu.VMEM(table.shape, table.dtype) for table in tables]
        + [
            dma((7,)),
            dma((chunks,)),
            dma((chunks,)),
            dma((chunks,)),
            dma((chunks,)),
            dma((2, ranks, chunks)),
            dma((ranks, chunks)),
            dma((3,)),
            dma((3,)),
            dma((2, bands)),
            dma((2,)),
            dma((2, halves_count)),
            dma((2, halves_count)),
            dma((2 * chunks,)),
            dma((2 * chunks,)),
            dma((bands, 2 * chunks)),
            dma((bands, 2 * chunks)),
            dma((bands, ranks)),
            dma((bands, ranks)),
        ],
        compiler_params=pltpu.CompilerParams(
            collective_id=0, has_side_effects=True, vmem_limit_bytes=60 * 1024 * 1024
        ),
    )(shift_table.T, shift_index, orbital, partner, *tables)


def paired_body(bands, ranks, orbitals, partners, shift_table, shift_index):
    potential, projector = exchange(
        bands, ranks, orbitals[0], partners[0], shift_table, shift_index
    )
    return (potential[None], projector[None])


def body(orbitals, partners, shift_table, shift_index):
    bands = lax.axis_size("band")
    ranks = lax.axis_size("fft")
    count, planes, rows, lanes = orbitals.shape
    grid_bytes = ranks * planes * rows * lanes * 4
    paired = (
        count == 1
        and ranks == 4
        and bands == ranks
        and planes % (2 * bands) == 0
        and planes % GROUP == 0
        and GROUP % (planes // bands) == 0
        and lanes == 2 * rows
        and lanes == 128
        and grid_bytes <= 2 * 1024 * 1024
    )
    if paired:
        return paired_body(bands, ranks, orbitals, partners, shift_table, shift_index)
    return general_body(orbitals, partners, shift_table, shift_index)


def solution(mesh):
    in_specs = (
        P(("kgrp", "band"), "fft", None, None),
        P(("kgrp", "band"), "fft", None, None),
        P(),
        P("kgrp"),
    )
    out_specs = (P(("kgrp", "band"), "fft", None, None), P(("kgrp", "band"), "fft", None, None))
    return jax.shard_map(body, mesh=mesh, in_specs=in_specs, out_specs=out_specs, check_vma=False)
```

```python
import functools
import math

import jax
import jax.numpy as jnp
import numpy as np
from jax import lax
from jax.experimental import pallas as pl
from jax.experimental.pallas import tpu as pltpu
from jax.sharding import PartitionSpec as P

HIGHEST = lax.Precision.HIGHEST
HIGH = lax.Precision.HIGH
MESH = pl.DeviceIdType.MESH
GROUP = 8
SCREEN_SQUARE = 0.25
FOUR_PI = 4.0 * math.pi


def angle_pair(extent, sign):
    positions = jnp.arange(extent, dtype=jnp.int32)
    product = positions[:, None] * positions[None, :] % extent
    angle = 2.0 * math.pi / extent * product.astype(jnp.float32)
    return (jnp.cos(angle), sign * jnp.sin(angle))


def last_table(extent, sign):
    cosine, sine = angle_pair(extent, sign)
    upper = jnp.concatenate([cosine, sine], axis=1)
    lower = jnp.concatenate([-sine, cosine], axis=1)
    return jnp.concatenate([upper, lower], axis=0)


def middle_table(extent, sign):
    cosine, sine = angle_pair(extent, sign)
    return jnp.stack([jnp.stack([cosine, -sine], -1), jnp.stack([sine, cosine], -1)], 1)


def along_last(field, table):
    shape = field.shape
    flat = field.reshape(-1, shape[-1])
    return jnp.dot(flat, table, precision=HIGH).reshape(shape)


def along_axis(field, table, axis_number):
    shape = field.shape
    extent = shape[-1] // 2
    split = field.reshape(shape[0], shape[1], shape[2], 2, extent)
    if axis_number == 1:
        result = jnp.einsum("kcnd,pnbdz->pkbcz", table, split, precision=HIGH)
    else:
        result = jnp.einsum("kcnd,pandz->pakcz", table, split, precision=HIGH)
    return result.reshape(shape)


def times_conj(left, right):
    extent = left.shape[-1] // 2
    left_real, left_imag = (left[..., :extent], left[..., extent:])
    right_real, right_imag = (right[..., :extent], right[..., extent:])
    return jnp.concatenate(
        [
            left_real * right_real + left_imag * right_imag,
            left_real * right_imag - left_imag * right_real,
        ],
        axis=-1,
    )


def times(left, right):
    extent = left.shape[-1] // 2
    left_real, left_imag = (left[..., :extent], left[..., extent:])
    right_real, right_imag = (right[..., :extent], right[..., extent:])
    return jnp.concatenate(
        [
            left_real * right_real - left_imag * right_imag,
            left_real * right_imag + left_imag * right_real,
        ],
        axis=-1,
    )


def rotate(field):
    extent = field.shape[-1] // 2
    return jnp.concatenate([field[..., extent:], -field[..., :extent]], axis=-1)


def frequency(positions, extent):
    return jnp.where(positions < extent // 2, positions, positions - extent).astype(jnp.float32)


def kernel_block(qvectors, y_count, extent):
    first_freq = frequency(jnp.arange(extent, dtype=jnp.int32), extent)
    second_freq = frequency(jnp.arange(y_count, dtype=jnp.int32), extent)
    third_freq = frequency(jnp.arange(2 * extent, dtype=jnp.int32) % extent, extent)
    first_part = (first_freq[None, :] + qvectors[:, 0:1]) ** 2
    second_part = (second_freq[None, :] + qvectors[:, 1:2]) ** 2
    third_part = (third_freq[None, :] + qvectors[:, 2:3]) ** 2
    denominator = (
        first_part[:, :, None, None]
        + second_part[:, None, :, None]
        + third_part[:, None, None, :]
        + SCREEN_SQUARE
    )
    return FOUR_PI / extent**3 / denominator


def shifts_for(shift_table, shift_index, start_at, length):
    picked = lax.dynamic_slice_in_dim(shift_index, start_at, length)
    onehot = (picked[:, None] == jnp.arange(shift_table.shape[0], dtype=jnp.int32)[None, :]).astype(
        jnp.float32
    )
    return jnp.dot(onehot, shift_table, precision=HIGHEST)


def factor_inverse(over_real, over_imag):
    matrix_order = over_real.shape[0]
    positions = jnp.arange(matrix_order, dtype=jnp.int32)
    zero_start = jnp.zeros_like(over_real)

    def chol_step(column, lowers):
        lower_real, lower_imag = lowers
        row_real = lower_real[column]
        row_imag = lower_imag[column]
        resid_real = over_real[:, column] - (
            jnp.dot(lower_real, row_real, precision=HIGHEST)
            + jnp.dot(lower_imag, row_imag, precision=HIGHEST)
        )
        resid_imag = over_imag[:, column] - (
            jnp.dot(lower_imag, row_real, precision=HIGHEST)
            - jnp.dot(lower_real, row_imag, precision=HIGHEST)
        )
        pivot_value = jnp.sqrt(resid_real[column])
        below_diag = positions > column
        at_diag = positions == column
        new_real = jnp.where(
            below_diag, resid_real / pivot_value, jnp.where(at_diag, pivot_value, 0.0)
        )
        new_imag = jnp.where(below_diag, resid_imag / pivot_value, 0.0)
        chosen = positions[None, :] == column
        return (
            jnp.where(chosen, new_real[:, None], lower_real),
            jnp.where(chosen, new_imag[:, None], lower_imag),
        )

    lower_real, lower_imag = lax.fori_loop(0, matrix_order, chol_step, (zero_start, zero_start))

    def solve_step(row_index, inverses):
        inv_real, inv_imag = inverses
        row_real = lower_real[row_index]
        row_imag = lower_imag[row_index]
        sum_real = jnp.dot(row_real, inv_real, precision=HIGHEST) - jnp.dot(
            row_imag, inv_imag, precision=HIGHEST
        )
        sum_imag = jnp.dot(row_real, inv_imag, precision=HIGHEST) + jnp.dot(
            row_imag, inv_real, precision=HIGHEST
        )
        unit_row = (positions == row_index).astype(over_real.dtype)
        pivot_value = lower_real[row_index, row_index]
        new_real = (unit_row - sum_real) / pivot_value
        new_imag = -sum_imag / pivot_value
        chosen = positions[:, None] == row_index
        return (
            jnp.where(chosen, new_real[None, :], inv_real),
            jnp.where(chosen, new_imag[None, :], inv_imag),
        )

    return lax.fori_loop(0, matrix_order, solve_step, (zero_start, zero_start))


def general_body(orbitals, partners, shift_table, shift_index):
    extent = orbitals.shape[2]
    band_count = orbitals.shape[0]
    tables = (
        last_table(extent, -1.0),
        middle_table(extent, -1.0),
        last_table(extent, 1.0),
        middle_table(extent, 1.0),
    )
    my_band = lax.axis_index("band")
    forward_last, forward_mid, inverse_last, inverse_mid = tables
    full_orbitals = lax.all_gather(orbitals, "fft", axis=1, tiled=True)
    every_slab = lax.all_gather(partners, "band", axis=0, tiled=True)
    own_grids = lax.all_to_all(every_slab, "fft", split_axis=0, concat_axis=1, tiled=True)
    own_count = own_grids.shape[0]
    qvectors = shifts_for(shift_table, shift_index, lax.axis_index("fft") * own_count, own_count)

    def one_partner(member, running):
        single = lax.dynamic_slice_in_dim(own_grids, member, 1, 0)
        kernel = kernel_block(lax.dynamic_slice_in_dim(qvectors, member, 1, 0), extent, extent)
        density = times_conj(single, full_orbitals)
        spectrum = (
            along_axis(
                along_axis(along_last(density, forward_last), forward_mid, 2), forward_mid, 1
            )
            * kernel
        )
        field = along_last(
            along_axis(along_axis(spectrum, inverse_mid, 1), inverse_mid, 2), inverse_last
        )
        return running + times(single, field)

    partial_value = lax.fori_loop(
        0, own_count, one_partner, jnp.zeros(full_orbitals.shape, jnp.float32)
    )
    potential = lax.psum_scatter(partial_value, "fft", scatter_dimension=1, tiled=True)
    every_pot = lax.all_gather(potential, "band", axis=0, tiled=True)
    turned = rotate(every_pot)
    total_bands = every_pot.shape[0]
    flat_orbitals = orbitals.reshape(band_count, -1)
    flat_pot = every_pot.reshape(total_bands, -1)
    flat_turned = turned.reshape(total_bands, -1)
    volume = float(extent**3)
    rows_real = jnp.einsum("ik,jk->ij", flat_orbitals, flat_pot, precision=HIGHEST) / volume
    rows_imag = jnp.einsum("ik,jk->ij", flat_orbitals, flat_turned, precision=HIGHEST) / volume
    start_row = my_band * band_count
    summed_real, summed_imag = lax.psum((rows_real, rows_imag), "fft")
    over_real, over_imag = (
        lax.all_gather(summed_real, "band", axis=0, tiled=True),
        lax.all_gather(summed_imag, "band", axis=0, tiled=True),
    )
    inv_real, inv_imag = factor_inverse(over_real, over_imag)
    coef_real = lax.dynamic_slice_in_dim(inv_real, start_row, band_count, 0)
    coef_imag = lax.dynamic_slice_in_dim(inv_imag, start_row, band_count, 0)
    projector = jnp.dot(coef_real, flat_pot, precision=HIGHEST) + jnp.dot(
        coef_imag, flat_turned, precision=HIGHEST
    )
    return (potential, projector.reshape(orbitals.shape))


def remote(source, target, send_sem, recv_sem, where):
    return pltpu.make_async_remote_copy(
        src_ref=source,
        dst_ref=target,
        send_sem=send_sem,
        recv_sem=recv_sem,
        device_id=where,
        device_id_type=MESH,
    )


def greet(others):
    barrier = pltpu.get_barrier_semaphore()
    for other in others:
        pl.semaphore_signal(barrier, inc=1, device_id=other, device_id_type=MESH)
    pl.semaphore_wait(barrier, len(others))


def turn(block):
    lanes = block.shape[-1]
    swapped = pltpu.roll(block, lanes // 2, block.ndim - 1)
    position = lax.broadcasted_iota(jnp.int32, block.shape, block.ndim - 1)
    return jnp.where(position < lanes // 2, swapped, -swapped)


def small_factor_inverse(matrix):
    order = len(matrix)
    lower = [[None] * order for _ in range(order)]
    for column in range(order):
        residual = []
        for row in range(column, order):
            real, imag = matrix[row][column]
            for k in range(column):
                a, b = lower[row][k]
                c, d = lower[column][k]
                real = real - (a * c + b * d)
                imag = imag - (b * c - a * d)
            residual.append((real, imag))
        pivot = jnp.sqrt(residual[0][0])
        lower[column][column] = (pivot, jnp.zeros_like(pivot))
        for row in range(column + 1, order):
            real, imag = residual[row - column]
            lower[row][column] = (real / pivot, imag / pivot)
    inverse = [[None] * order for _ in range(order)]
    for row in range(order):
        pivot = lower[row][row][0]
        inverse[row][row] = (1.0 / pivot, jnp.zeros_like(pivot))
        for column in range(row):
            real = jnp.zeros_like(pivot)
            imag = jnp.zeros_like(pivot)
            for k in range(column, row):
                a, b = lower[row][k]
                c, d = inverse[k][column]
                real = real - (a * c - b * d)
                imag = imag - (a * d + b * c)
            inverse[row][column] = (real / pivot, imag / pivot)
    return inverse


def split_table(table):
    high = table.astype(jnp.bfloat16)
    low = (table - high.astype(np.float64)).astype(jnp.bfloat16)
    return high, low


def right_table(extent, sign):
    grid = np.outer(np.arange(extent), np.arange(extent)) % extent
    angle = 2.0 * math.pi / extent * grid
    cosine, sine = np.cos(angle), sign * np.sin(angle)
    table = np.block([[cosine, sine], [-sine, cosine]])
    high, low = split_table(table)
    upper = np.concatenate([high, low], axis=1)
    lower = np.concatenate([high, np.zeros_like(low)], axis=1)
    return np.concatenate([upper, lower], axis=0)


def left_table(extent, sign):
    grid = np.outer(np.arange(extent), np.arange(extent)) % extent
    angle = 2.0 * math.pi / extent * grid
    high, low = split_table(np.concatenate([np.cos(angle), sign * np.sin(angle)], axis=0))
    return np.concatenate([high, high, low], axis=1)


def halves(value):
    high = value.astype(jnp.bfloat16)
    low = (value - high.astype(jnp.float32)).astype(jnp.bfloat16)
    return high, low


def right_product(value, table):
    lanes = value.shape[-1]
    high, low = halves(value)
    both = jnp.dot(
        jnp.concatenate([high, low], axis=1), table, preferred_element_type=jnp.float32
    )
    return both[:, :lanes] + both[:, lanes:]


def left_product(first, second, table):
    rows, lanes = first.shape
    high, low = halves(jnp.concatenate([first, second], axis=1))
    stacked = jnp.concatenate([high, low, high], axis=0)
    both = jnp.dot(table, stacked, preferred_element_type=jnp.float32)
    return tuple(
        both[:rows, cut : cut + lanes] - turn(both[rows:, cut : cut + lanes])
        for cut in (0, lanes)
    )


def spread_parts(value):
    lanes = value.shape[-1]
    swapped = pltpu.roll(value, lanes // 2, value.ndim - 1)
    lower = lax.broadcasted_iota(jnp.int32, value.shape, value.ndim - 1) < lanes // 2
    return jnp.where(lower, value, swapped), jnp.where(lower, swapped, value)


def forward_group(group, orbital_grid, partner_grid, work, right, left):
    rows, lanes = orbital_grid.shape[1:]
    span = pl.ds(group * GROUP, GROUP)
    orbital = orbital_grid[span].reshape(GROUP * rows, lanes)
    real, imag = spread_parts(partner_grid[span].reshape(GROUP * rows, lanes))
    density = real * orbital + imag * turn(orbital)
    lines = right_product(density, right[...])
    planes = []
    for pair in range(GROUP // 2):
        start = 2 * pair * rows
        planes += left_product(
            lines[start : start + rows], lines[start + rows : start + 2 * rows], left[...]
        )
    stacked = jnp.stack(planes, axis=0)
    work[:, span, :] = jnp.swapaxes(stacked, 0, 1)


def backward_group(group, partner_grid, partial, work, right, left):
    rows, lanes = partner_grid.shape[1:]
    span = pl.ds(group * GROUP, GROUP)
    planes = jnp.swapaxes(work[:, span, :], 0, 1)
    lines = []
    for pair in range(GROUP // 2):
        lines += left_product(planes[2 * pair], planes[2 * pair + 1], left[...])
    field = right_product(jnp.concatenate(lines, axis=0), right[...])
    real, imag = spread_parts(partner_grid[span].reshape(GROUP * rows, lanes))
    partial[span] = (real * field - imag * turn(field)).reshape(GROUP, rows, lanes)


def fill_screen(shift, screen):
    columns, extent, lanes = screen.shape
    first = frequency(lax.broadcasted_iota(jnp.int32, (extent, lanes), 0), extent)
    third_place = lax.broadcasted_iota(jnp.int32, (extent, lanes), 1)
    third_place = jnp.where(third_place < lanes // 2, third_place, third_place - lanes // 2)
    third = frequency(third_place, extent)
    base = (first + shift[0]) ** 2 + (third + shift[2]) ** 2 + SCREEN_SQUARE
    scale = FOUR_PI / (float(extent) * float(columns) * float(lanes // 2))

    def one_column(column, carry):
        second = jnp.where(column < columns // 2, column, column - columns)
        offset = (second.astype(jnp.float32) + shift[1]) ** 2
        screen[column] = scale / (base + offset)
        return carry

    lax.fori_loop(0, columns, one_column, 0, unroll=2)


def middle_pairs(screen, work, forward, inverse):
    columns = work.shape[0]

    def one_pair(pair, carry):
        spectra = left_product(work[2 * pair], work[2 * pair + 1], forward[...])
        scaled = [spectra[which] * screen[2 * pair + which] for which in range(2)]
        fields = left_product(scaled[0], scaled[1], inverse[...])
        work[2 * pair] = fields[0]
        work[2 * pair + 1] = fields[1]
        return carry

    lax.fori_loop(0, columns // 2, one_pair, 0, unroll=16)


def exchange_kernel(
    bands,
    ranks,
    shift_table,
    shift_index,
    orbital_home,
    partner_home,
    right_forward_home,
    right_inverse_home,
    left_forward_home,
    left_inverse_home,
    potential,
    projector,
    orbital_grid,
    partner_grid,
    work,
    partial,
    partner,
    detour,
    near,
    outgoing,
    arriving,
    passed,
    others,
    tops,
    tallies,
    own_sums,
    all_sums,
    right_forward,
    right_inverse,
    left_forward,
    left_inverse,
    load_sem,
    gather_send,
    detour_send,
    detour_recv,
    onward_send,
    chain_send,
    partner_recv,
    grid_send,
    grid_recv,
    other_send,
    other_recv,
    third_send,
    third_recv,
    top_send,
    top_recv,
    near_send,
    near_recv,
    far_send,
    far_recv,
    up_send,
    up_recv,
    sum_send,
    sum_recv,
):
    planes, rows, lanes = potential.shape
    chunks = bands
    piece = planes // chunks
    per_group = GROUP // piece
    halves_count = planes // GROUP
    last = bands - 1
    cuts = 2 * chunks
    slice_size = planes // cuts
    direct = 4 * cuts // 8
    lag = cuts // 4
    held_back = 2 * cuts // 8
    top = 4 * cuts // 8
    split = (cuts - top) * slice_size
    band = lax.axis_index("band")
    rank = lax.axis_index("fft")
    beside = rank + 1 - 2 * (rank % 2)
    across = (rank + 2) % ranks
    beside_across = (beside + 2) % ranks
    slabs = (rank, beside, across, beside_across)
    home = 2 * (rank % 2) + (rank // 2 + rank % 2) % 2
    keeper = 2 * ((band // 2 + band % 2) % 2) + band // 2

    def both(*conditions):
        return functools.reduce(jnp.logical_and, conditions)

    def either(*conditions):
        return functools.reduce(jnp.logical_or, conditions)

    at_home = band == home
    at_end = either(band == 0, band == last)
    early = either(at_home, band == 1, band == last - 1)
    low_side = rank < ranks // 2
    takes_detour = both(at_end, low_side)
    gives_detour = both(jnp.logical_not(at_end), low_side)

    def span(index):
        return pl.ds(index * piece, piece)

    def cut_span(cut):
        return pl.ds(cut * slice_size, slice_size)

    def slab(index):
        return pl.ds(index * planes, planes)

    def window(index, chunk):
        return pl.ds(index * planes + chunk * piece, piece)

    own_slab = pltpu.make_async_copy(orbital_home, orbital_grid.at[slab(rank)], load_sem.at[1])
    partner_load = pltpu.make_async_copy(partner_home, partner, load_sem.at[0])
    home_load = pltpu.make_async_copy(partner_home, partner_grid.at[slab(rank)], load_sem.at[2])
    table_loads = [
        pltpu.make_async_copy(source, here, load_sem.at[3 + number])
        for number, (source, here) in enumerate(
            (
                (right_forward_home, right_forward),
                (left_forward_home, left_forward),
                (right_inverse_home, right_inverse),
                (left_inverse_home, left_inverse),
            )
        )
    ]
    partner_load.start()

    @pl.when(at_home)
    def _():
        home_load.start()

    own_slab.start()
    for load in table_loads:
        load.start()
    greet(
        [
            {"band": (band + step) % bands, "fft": (rank + turn_by) % ranks}
            for step in range(bands)
            for turn_by in range(ranks)
            if step or turn_by
        ]
    )

    def gather_copy(chunk):
        return remote(
            partner.at[span(chunk)],
            partner_grid.at[window(rank, chunk)],
            gather_send.at[chunk],
            partner_recv.at[rank, chunk],
            {"fft": keeper},
        )

    def detour_copy(chunk):
        return remote(
            partner.at[span(chunk)],
            detour.at[chunk],
            detour_send.at[chunk],
            detour_recv.at[chunk],
            {"band": last * (band - 1)},
        )

    def onward_copy(chunk):
        return remote(
            detour.at[chunk],
            partner_grid.at[window(rank, chunk)],
            onward_send.at[chunk],
            partner_recv.at[rank, chunk],
            {"fft": ranks // 2 + band // last},
        )

    def chain_copy(way, turn_to, chunk):
        place = partner_grid.at[window(slabs[turn_to], chunk)]
        return remote(
            place,
            place,
            chain_send.at[way, turn_to, chunk],
            partner_recv.at[slabs[turn_to], chunk],
            {"band": band + 1 - 2 * way},
        )

    def passes(way, turn_to):
        if way == 0:
            go = both(band >= home, band < last)
            short = both(band == last - 1, rank == ranks - 1)
        else:
            go = both(band <= home, band > 0)
            short = both(band == 1, rank == ranks // 2)
        return both(go, jnp.logical_not(short)) if turn_to > 1 else go

    def arrive(turn_to, chunk):
        def wait():
            chain_copy(0, turn_to, chunk).wait_recv()

        if turn_to:
            wait()
        else:
            pl.when(jnp.logical_not(at_home))(wait)

    def step(turn_to, chunk):
        arrive(turn_to, chunk)
        for way in (0, 1):

            @pl.when(passes(way, turn_to))
            def _():
                chain_copy(way, turn_to, chunk).start()

    tail = [(turn_to, half) for half in range(halves_count) for turn_to in (2, 3)]

    def of_half(half):
        return range(half * per_group, (half + 1) * per_group)

    partner_load.wait()
    for chunk in range(chunks):

        @pl.when(jnp.logical_not(at_home))
        def _():
            gather_copy(chunk).start()

        @pl.when(gives_detour)
        def _():
            detour_copy(chunk).start()

    @pl.when(at_home)
    def _():
        home_load.wait()

    own_slab.wait()
    own_orbital = orbital_grid.at[slab(rank)]
    to_across = remote(own_orbital, own_orbital, grid_send.at[0], grid_recv.at[0], {"fft": across})
    to_beside = remote(own_orbital, own_orbital, grid_send.at[1], grid_recv.at[1], {"fft": beside})
    other_orbital = orbital_grid.at[slab(across)]
    onward = remote(
        other_orbital, other_orbital, grid_send.at[2], grid_recv.at[2], {"fft": beside}
    )
    to_across.start()
    to_beside.start()

    def take_detour(condition, chunk):
        @pl.when(both(takes_detour, condition))
        def _():
            detour_copy(chunk).wait_recv()
            onward_copy(chunk).start()

    for turn_to in (0, 1):
        for chunk in range(chunks):
            step(turn_to, chunk)
            if turn_to == 1:
                take_detour(jnp.logical_not(at_home), chunk)

    def other_copy(slot, where, source=own_orbital):
        return remote(
            source,
            others.at[slot],
            other_send.at[slot, where],
            other_recv.at[slot],
            {"band": where},
        )

    def third_copy(number):
        place = pl.ds(split, planes - split) if number == 0 else pl.ds(0, split)
        held = others.at[1, place]
        return remote(
            held, held, third_send.at[number], third_recv.at[number], {"band": 1}
        )

    def top_copy(member):
        rest = pl.ds(split, planes - split)
        source = (
            orbital_grid.at[pl.ds(rank * planes + split, planes - split)]
            if member == 0
            else others.at[member - 1, rest]
        )
        return remote(
            source,
            tops.at[member],
            top_send.at[member],
            top_recv.at[member],
            {"band": 0},
        )

    def forward(group):
        forward_group(group, orbital_grid, partner_grid, work, right_forward, left_forward)

    def forward_near(index):
        forward(
            (rank + index // halves_count * (beside - rank)) * halves_count + index % halves_count
        )

    def tabulate():
        chosen = shift_index[home]
        fill_screen([shift_table[axis, chosen] for axis in range(3)], partial)

    for load in table_loads:
        load.wait()
    to_beside.wait_recv()

    @pl.when(early)
    def _():
        for number, (turn_to, half) in enumerate(tail):
            for chunk in of_half(half):
                if turn_to == 2:
                    take_detour(at_home, chunk)
            if number == len(tail) - 2:

                @pl.when(jnp.logical_not(at_home))
                def _():
                    to_across.wait_recv()
                    onward.start()

            for chunk in of_half(half):
                step(turn_to, chunk)
            forward_near(number)
            if number == 1:
                tabulate()

    @pl.when(band == 2)
    def _():
        other_copy(0, 1).start()

    @pl.when(band == last)
    def _():
        other_copy(1, 2).start()

    @pl.when(either(at_home, at_end))
    def _():
        to_across.wait_recv()
        onward.start()

    @pl.when(jnp.logical_not(early))
    def _():
        def one_group(index, carry):
            forward_near(index)
            return carry

        lax.fori_loop(0, 2 * halves_count, one_group, 0)
        tabulate()

    onward.wait_recv()
    for turn_to, half in tail:

        @pl.when(jnp.logical_not(early))
        def _():
            for chunk in of_half(half):
                arrive(turn_to, chunk)

        forward(slabs[turn_to] * halves_count + half)

    middle_pairs(partial, work, left_forward, left_inverse)

    @pl.when(band == 2)
    def _():
        other_copy(1, 2).wait_recv()
        for number in range(2):
            third_copy(number).start()

    def backward(index, half):
        backward_group(
            index * halves_count + half, partner_grid, partial, work, right_inverse, left_inverse
        )

    def near_copy(which, index, half):
        return remote(
            partial.at[pl.ds(index * planes + half * GROUP, GROUP)],
            near.at[which, pl.ds(half * GROUP, GROUP)],
            near_send.at[which, half],
            near_recv.at[which, half],
            {"fft": beside},
        )

    def far_copy(cut):
        return remote(
            outgoing.at[cut_span(cut)],
            arriving.at[cut_span(cut)],
            far_send.at[cut],
            far_recv.at[cut],
            {"fft": across},
        )

    def up_copy(owner, cut, own=False):
        held = passed.at[owner, cut_span(cut)]
        return remote(
            potential.at[cut_span(cut)] if own else held,
            held,
            up_send.at[owner, cut],
            up_recv.at[owner, cut],
            {"band": band + 1},
        )

    def slice_of(index, cut):
        return pl.ds(index * planes + cut * slice_size, slice_size)

    per_half = cuts // halves_count
    def halves_of_cuts(half):
        return range(half * per_half, (half + 1) * per_half)

    def send_half(half):
        backward(beside_across, half)
        near_copy(1, beside_across, half).start()
        backward(across, half)
        near_copy(1, beside_across, half).wait_recv()
        for cut in halves_of_cuts(half):
            outgoing[cut_span(cut)] = partial[slice_of(across, cut)] + near[1, cut_span(cut)]
            far_copy(cut).start()
        backward(beside, half)
        near_copy(0, beside, half).start()

    zero = jnp.zeros((8, lanes), jnp.float32)
    for number in range(tallies.shape[0]):
        tallies[number] = zero

    def inner(pairs, right, start, stop):
        slots = [2 * slot + half for slot, _ in pairs for half in range(2)]

        def accumulate(plane, sums):
            straight = right(plane)
            sides = (straight, turn(straight))
            values = [left(plane) for _, left in pairs]
            return tuple(
                running
                + jnp.sum((values[n // 2] * sides[n % 2]).reshape(rows // 8, 8, lanes), axis=0)
                for n, running in enumerate(sums)
            )

        sums = lax.fori_loop(
            start,
            stop,
            accumulate,
            tuple(tallies[slot] for slot in slots),
            unroll=min(4, stop - start),
        )
        for slot, value in zip(slots, sums):
            tallies[slot] = value

    def own_potential(plane):
        return potential[plane]

    def first_potential(plane):
        return passed[0, plane]

    def own_values(plane):
        return orbital_grid[rank * planes + plane]

    def other_values(slot):
        return lambda plane: others[slot, plane]

    def finish(cut):
        far_copy(cut).wait_recv()
        potential[cut_span(cut)] = (
            partial[slice_of(rank, cut)] + near[0, cut_span(cut)]
        ) + arriving[cut_span(cut)]

        sends = band < last - 1 if cut >= direct else band < last

        @pl.when(both(sends, band > 0) if cut >= cuts - held_back else sends)
        def _():
            up_copy(band, cut, True).start()

        inner([(0, own_values)], own_potential, cut * slice_size, (cut + 1) * slice_size)
        if 0 <= cut - lag < direct:

            @pl.when(band == 2)
            def _():
                lift_on(1, cut - lag)

        if cut == cuts // 2:

            @pl.when(band == 1)
            def _():
                other_copy(0, 1).wait_recv()
                top_copy(1).start()

    def lift_on(member, cut):
        up_copy(member, cut).wait_recv()
        up_copy(member, cut).start()

    for half in range(halves_count):
        send_half(half)
        if half == 0:

            @pl.when(band == 1)
            def _():
                top_copy(0).start()

            backward(rank, half)
            near_copy(0, beside, half).wait_recv()
            continue
        for number, cut in enumerate(halves_of_cuts(half - 1)):
            finish(cut)
            if number == per_half // 2 - 1:
                backward(rank, half)
        near_copy(0, beside, half).wait_recv()
    for cut in halves_of_cuts(halves_count - 1):
        finish(cut)

    @pl.when(band == 1)
    def _():
        def pass_on(cut):
            up_copy(0, cut).wait_recv()
            up_copy(0, cut).start()

        def with_first(start, stop):
            inner(
                [(3, own_values), (4, other_values(0)), (5, other_values(1))],
                first_potential,
                start * slice_size,
                stop * slice_size,
            )

        third_copy(0).wait_recv()
        top_copy(2).start()
        for cut in range(per_half):
            pass_on(cut)
        third_copy(1).wait_recv()
        inner([(1, other_values(0)), (2, other_values(1))], own_potential, 0, planes)
        with_first(0, per_half)
        for cut in range(per_half, cuts - top):
            pass_on(cut)
            with_first(cut, cut + 1)

    @pl.when(band == 2)
    def _():
        inner([(2, other_values(1))], own_potential, 0, planes)

    @pl.when(band == 0)
    def _():
        for member in range(3):
            top_copy(member).wait_recv()
        inner(
            [
                (3 + member, lambda plane, member=member: tops[member, plane - split])
                for member in range(3)
            ],
            own_potential,
            split,
            planes,
        )

    entries = [(i, l) for i in range(bands) for l in range(i + 1)]
    places = (
        band * (band + 1) // 2 + band,
        entries.index((2, 1)),
        entries.index((last, 0)) + band,
        entries.index((1, 0)),
        entries.index((2, 0)),
        entries.index((last, 0)),
    )
    position = lax.broadcasted_iota(jnp.int32, (8, lanes), 1)
    packed = zero
    for slot, place in enumerate(places):
        for half in range(2):
            value = jnp.sum(tallies[2 * slot + half], axis=1, keepdims=True)
            packed = packed + jnp.where(position == 2 * place + half, value, 0.0)
    own_sums[...] = packed
    sum_copies = []
    for step_by in range(bands):
        for turn_by in range(ranks):
            if step_by == 0 and turn_by == 0:
                continue
            copy = remote(
                own_sums,
                all_sums.at[band, rank],
                sum_send.at[step_by, turn_by],
                sum_recv.at[step_by, turn_by],
                {"band": (band + step_by) % bands, "fft": (rank + turn_by) % ranks},
            )
            copy.start()
            sum_copies.append(copy)
    all_sums[band, rank] = packed

    @pl.when(band == 0)
    def _():
        for cut in range(cuts - held_back, cuts):
            up_copy(0, cut, True).start()

    @pl.when(band == 1)
    def _():
        for cut in range(cuts - top, cuts):
            up_copy(0, cut).wait_recv()
            up_copy(0, cut).start()

    @pl.when(band == 2)
    def _():
        for cut in range(cuts - lag, direct):
            lift_on(1, cut)
        for cut in range(direct):
            lift_on(0, cut)

    for chunk in range(chunks):

        @pl.when(jnp.logical_not(at_home))
        def _():
            gather_copy(chunk).wait_send()

        @pl.when(gives_detour)
        def _():
            detour_copy(chunk).wait_send()

        @pl.when(takes_detour)
        def _():
            onward_copy(chunk).wait_send()

        for turn_to in range(len(slabs)):
            for way in (0, 1):

                @pl.when(passes(way, turn_to))
                def _():
                    chain_copy(way, turn_to, chunk).wait_send()

    @pl.when(band == 2)
    def _():
        other_copy(0, 1).wait_send()
        for number in range(2):
            third_copy(number).wait_send()

    @pl.when(band == 1)
    def _():
        for member in range(3):
            top_copy(member).wait_send()

    @pl.when(band == last)
    def _():
        other_copy(1, 2).wait_send()

    for half in range(halves_count):
        near_copy(0, beside, half).wait_send()
        near_copy(1, beside_across, half).wait_send()
    to_across.wait_send()
    to_beside.wait_send()
    onward.wait_send()

    for cut in range(cuts):
        far_copy(cut).wait_send()

    for copy in sum_copies:
        copy.wait()
    total = zero
    for one_band in range(bands):
        for one_rank in range(ranks):
            total = total + all_sums[one_band, one_rank]
    total = jnp.broadcast_to(jnp.sum(total, axis=0, keepdims=True), (8, lanes))
    volume = float(lanes // 2) * float(rows) * float(planes * ranks)
    matrix = [[None] * bands for _ in range(bands)]
    for number, (i, l) in enumerate(entries):
        values = [
            jnp.broadcast_to(
                jnp.sum(jnp.where(position == 2 * number + half, total, 0.0), axis=1, keepdims=True),
                (8, lanes),
            )
            / volume
            for half in range(2)
        ]
        matrix[i][l] = (values[0], values[1])
    inverse = small_factor_inverse(matrix)

    def combine(row, own, members, start, stop, put):
        def one_plane(plane, carry):
            sum_straight = jnp.zeros((rows, lanes), jnp.float32)
            sum_turned = jnp.zeros((rows, lanes), jnp.float32)
            for m in members:
                block = potential[plane] if m is None else passed[m, plane]
                real, imag = inverse[row][own if m is None else m]
                sum_straight = sum_straight + real[:1] * block
                sum_turned = sum_turned + imag[:1] * block
            put(plane, sum_straight + turn(sum_turned))
            return carry

        lax.fori_loop(start, stop, one_plane, 0, unroll=min(4, stop - start))

    def put_whole(plane, value):
        projector[plane] = value

    def put_more(plane, value):
        projector[plane] = projector[plane] + value

    def put_lifted(plane, value):
        passed[2, plane] = value

    for row in range(2):

        @pl.when(band == row)
        def _():
            combine(row, row, [None, 0][: row + 1], 0, planes, put_whole)

    @pl.when(band == 2)
    def _():
        for cut in range(direct, cuts):
            up_copy(1, cut).wait_recv()
        for cut in range(direct, cuts):
            up_copy(0, cut).wait_recv()
            combine(
                last, 2, (0, 1, None), cut * slice_size, (cut + 1) * slice_size, put_lifted
            )
            up_copy(2, cut).start()
        combine(2, 2, (0, 1, None), 0, planes, put_whole)

    @pl.when(band == last)
    def _():
        for member in (2, 1):
            for cut in range(direct):
                up_copy(member, cut).wait_recv()
        combine(last, last, (1, 2, None), 0, direct * slice_size, put_whole)
        combine(last, last, (None,), direct * slice_size, planes, put_whole)
        for cut in range(direct):
            up_copy(0, cut).wait_recv()
            combine(last, last, (0,), cut * slice_size, (cut + 1) * slice_size, put_more)
        for cut in range(direct, cuts):
            up_copy(2, cut).wait_recv()
            projector[cut_span(cut)] = projector[cut_span(cut)] + passed[2, cut_span(cut)]

    for cut in range(cuts):
        @pl.when(band < last)
        def _():
            up_copy(band, cut, True).wait_send()

        if cut < direct:

            @pl.when(band == 2)
            def _():
                up_copy(1, cut).wait_send()

        @pl.when(band == 1 if cut >= direct else either(band == 1, band == 2))
        def _():
            up_copy(0, cut).wait_send()


def exchange(bands, ranks, orbital, partner, shift_table, shift_index):
    planes, rows, lanes = orbital.shape
    chunks = bands
    halves_count = planes // GROUP
    vmem = pl.BlockSpec(memory_space=pltpu.VMEM)
    smem = pl.BlockSpec(memory_space=pltpu.SMEM)
    out = pltpu.VMEM((planes, rows, lanes), jnp.float32)
    grid = pltpu.VMEM((ranks * planes, rows, lanes), jnp.float32)
    slab = pltpu.VMEM((planes, rows, lanes), jnp.float32)
    quarters = pltpu.VMEM((chunks, planes // chunks, rows, lanes), jnp.float32)

    def slab_list(count):
        return pltpu.VMEM((count, planes, rows, lanes), jnp.float32)

    dma = pltpu.SemaphoreType.DMA
    tables = [
        jnp.asarray(table)
        for table in (
            right_table(rows, -1.0),
            right_table(rows, 1.0),
            left_table(rows, -1.0),
            left_table(rows, 1.0),
        )
    ]
    return pl.pallas_call(
        functools.partial(exchange_kernel, bands, ranks),
        name="exchange",
        out_shape=(out, out),
        in_specs=[smem, smem] + [pl.BlockSpec(memory_space=pl.ANY)] * 6,
        out_specs=(vmem, vmem),
        scratch_shapes=[
            grid,
            grid,
            grid,
            grid,
            slab,
            quarters,
            slab_list(2),
            slab,
            slab,
            slab_list(bands - 1),
            slab_list(2),
            pltpu.VMEM((3, 4 * (planes // (2 * chunks)), rows, lanes), jnp.float32),
            pltpu.VMEM((12, 8, lanes), jnp.float32),
            pltpu.VMEM((8, lanes), jnp.float32),
            pltpu.VMEM((bands, ranks, 8, lanes), jnp.float32),
        ]
        + [pltpu.VMEM(table.shape, table.dtype) for table in tables]
        + [
            dma((7,)),
            dma((chunks,)),
            dma((chunks,)),
            dma((chunks,)),
            dma((chunks,)),
            dma((2, ranks, chunks)),
            dma((ranks, chunks)),
            dma((3,)),
            dma((3,)),
            dma((2, bands)),
            dma((2,)),
            dma((2,)),
            dma((2,)),
            dma((3,)),
            dma((3,)),
            dma((2, halves_count)),
            dma((2, halves_count)),
            dma((2 * chunks,)),
            dma((2 * chunks,)),
            dma((bands, 2 * chunks)),
            dma((bands, 2 * chunks)),
            dma((bands, ranks)),
            dma((bands, ranks)),
        ],
        compiler_params=pltpu.CompilerParams(
            collective_id=0, has_side_effects=True, vmem_limit_bytes=60 * 1024 * 1024
        ),
    )(shift_table.T, shift_index, orbital, partner, *tables)


def paired_body(bands, ranks, orbitals, partners, shift_table, shift_index):
    potential, projector = exchange(
        bands, ranks, orbitals[0], partners[0], shift_table, shift_index
    )
    return (potential[None], projector[None])


def body(orbitals, partners, shift_table, shift_index):
    bands = lax.axis_size("band")
    ranks = lax.axis_size("fft")
    count, planes, rows, lanes = orbitals.shape
    grid_bytes = ranks * planes * rows * lanes * 4
    paired = (
        count == 1
        and ranks == 4
        and bands == ranks
        and planes % (2 * bands) == 0
        and planes % GROUP == 0
        and GROUP % (planes // bands) == 0
        and lanes == 2 * rows
        and lanes == 128
        and grid_bytes <= 2 * 1024 * 1024
    )
    if paired:
        return paired_body(bands, ranks, orbitals, partners, shift_table, shift_index)
    return general_body(orbitals, partners, shift_table, shift_index)


def solution(mesh):
    in_specs = (
        P(("kgrp", "band"), "fft", None, None),
        P(("kgrp", "band"), "fft", None, None),
        P(),
        P("kgrp"),
    )
    out_specs = (P(("kgrp", "band"), "fft", None, None), P(("kgrp", "band"), "fft", None, None))
    return jax.shard_map(body, mesh=mesh, in_specs=in_specs, out_specs=out_specs, check_vma=False)
```

```python
import functools
import math

import jax
import jax.numpy as jnp
import numpy as np
from jax import lax
from jax.experimental import pallas as pl
from jax.experimental.pallas import tpu as pltpu
from jax.sharding import PartitionSpec as P

HIGHEST = lax.Precision.HIGHEST
HIGH = lax.Precision.HIGH
MESH = pl.DeviceIdType.MESH
GROUP = 8
SCREEN_SQUARE = 0.25
FOUR_PI = 4.0 * math.pi


def angle_pair(extent, sign):
    positions = jnp.arange(extent, dtype=jnp.int32)
    product = positions[:, None] * positions[None, :] % extent
    angle = 2.0 * math.pi / extent * product.astype(jnp.float32)
    return (jnp.cos(angle), sign * jnp.sin(angle))


def last_table(extent, sign):
    cosine, sine = angle_pair(extent, sign)
    upper = jnp.concatenate([cosine, sine], axis=1)
    lower = jnp.concatenate([-sine, cosine], axis=1)
    return jnp.concatenate([upper, lower], axis=0)


def middle_table(extent, sign):
    cosine, sine = angle_pair(extent, sign)
    return jnp.stack([jnp.stack([cosine, -sine], -1), jnp.stack([sine, cosine], -1)], 1)


def along_last(field, table):
    shape = field.shape
    flat = field.reshape(-1, shape[-1])
    return jnp.dot(flat, table, precision=HIGH).reshape(shape)


def along_axis(field, table, axis_number):
    shape = field.shape
    extent = shape[-1] // 2
    split = field.reshape(shape[0], shape[1], shape[2], 2, extent)
    if axis_number == 1:
        result = jnp.einsum("kcnd,pnbdz->pkbcz", table, split, precision=HIGH)
    else:
        result = jnp.einsum("kcnd,pandz->pakcz", table, split, precision=HIGH)
    return result.reshape(shape)


def times_conj(left, right):
    extent = left.shape[-1] // 2
    left_real, left_imag = (left[..., :extent], left[..., extent:])
    right_real, right_imag = (right[..., :extent], right[..., extent:])
    return jnp.concatenate(
        [
            left_real * right_real + left_imag * right_imag,
            left_real * right_imag - left_imag * right_real,
        ],
        axis=-1,
    )


def times(left, right):
    extent = left.shape[-1] // 2
    left_real, left_imag = (left[..., :extent], left[..., extent:])
    right_real, right_imag = (right[..., :extent], right[..., extent:])
    return jnp.concatenate(
        [
            left_real * right_real - left_imag * right_imag,
            left_real * right_imag + left_imag * right_real,
        ],
        axis=-1,
    )


def rotate(field):
    extent = field.shape[-1] // 2
    return jnp.concatenate([field[..., extent:], -field[..., :extent]], axis=-1)


def frequency(positions, extent):
    return jnp.where(positions < extent // 2, positions, positions - extent).astype(jnp.float32)


def kernel_block(qvectors, y_count, extent):
    first_freq = frequency(jnp.arange(extent, dtype=jnp.int32), extent)
    second_freq = frequency(jnp.arange(y_count, dtype=jnp.int32), extent)
    third_freq = frequency(jnp.arange(2 * extent, dtype=jnp.int32) % extent, extent)
    first_part = (first_freq[None, :] + qvectors[:, 0:1]) ** 2
    second_part = (second_freq[None, :] + qvectors[:, 1:2]) ** 2
    third_part = (third_freq[None, :] + qvectors[:, 2:3]) ** 2
    denominator = (
        first_part[:, :, None, None]
        + second_part[:, None, :, None]
        + third_part[:, None, None, :]
        + SCREEN_SQUARE
    )
    return FOUR_PI / extent**3 / denominator


def shifts_for(shift_table, shift_index, start_at, length):
    picked = lax.dynamic_slice_in_dim(shift_index, start_at, length)
    onehot = (picked[:, None] == jnp.arange(shift_table.shape[0], dtype=jnp.int32)[None, :]).astype(
        jnp.float32
    )
    return jnp.dot(onehot, shift_table, precision=HIGHEST)


def factor_inverse(over_real, over_imag):
    matrix_order = over_real.shape[0]
    positions = jnp.arange(matrix_order, dtype=jnp.int32)
    zero_start = jnp.zeros_like(over_real)

    def chol_step(column, lowers):
        lower_real, lower_imag = lowers
        row_real = lower_real[column]
        row_imag = lower_imag[column]
        resid_real = over_real[:, column] - (
            jnp.dot(lower_real, row_real, precision=HIGHEST)
            + jnp.dot(lower_imag, row_imag, precision=HIGHEST)
        )
        resid_imag = over_imag[:, column] - (
            jnp.dot(lower_imag, row_real, precision=HIGHEST)
            - jnp.dot(lower_real, row_imag, precision=HIGHEST)
        )
        pivot_value = jnp.sqrt(resid_real[column])
        below_diag = positions > column
        at_diag = positions == column
        new_real = jnp.where(
            below_diag, resid_real / pivot_value, jnp.where(at_diag, pivot_value, 0.0)
        )
        new_imag = jnp.where(below_diag, resid_imag / pivot_value, 0.0)
        chosen = positions[None, :] == column
        return (
            jnp.where(chosen, new_real[:, None], lower_real),
            jnp.where(chosen, new_imag[:, None], lower_imag),
        )

    lower_real, lower_imag = lax.fori_loop(0, matrix_order, chol_step, (zero_start, zero_start))

    def solve_step(row_index, inverses):
        inv_real, inv_imag = inverses
        row_real = lower_real[row_index]
        row_imag = lower_imag[row_index]
        sum_real = jnp.dot(row_real, inv_real, precision=HIGHEST) - jnp.dot(
            row_imag, inv_imag, precision=HIGHEST
        )
        sum_imag = jnp.dot(row_real, inv_imag, precision=HIGHEST) + jnp.dot(
            row_imag, inv_real, precision=HIGHEST
        )
        unit_row = (positions == row_index).astype(over_real.dtype)
        pivot_value = lower_real[row_index, row_index]
        new_real = (unit_row - sum_real) / pivot_value
        new_imag = -sum_imag / pivot_value
        chosen = positions[:, None] == row_index
        return (
            jnp.where(chosen, new_real[None, :], inv_real),
            jnp.where(chosen, new_imag[None, :], inv_imag),
        )

    return lax.fori_loop(0, matrix_order, solve_step, (zero_start, zero_start))


def general_body(orbitals, partners, shift_table, shift_index):
    extent = orbitals.shape[2]
    band_count = orbitals.shape[0]
    tables = (
        last_table(extent, -1.0),
        middle_table(extent, -1.0),
        last_table(extent, 1.0),
        middle_table(extent, 1.0),
    )
    my_band = lax.axis_index("band")
    forward_last, forward_mid, inverse_last, inverse_mid = tables
    full_orbitals = lax.all_gather(orbitals, "fft", axis=1, tiled=True)
    every_slab = lax.all_gather(partners, "band", axis=0, tiled=True)
    own_grids = lax.all_to_all(every_slab, "fft", split_axis=0, concat_axis=1, tiled=True)
    own_count = own_grids.shape[0]
    qvectors = shifts_for(shift_table, shift_index, lax.axis_index("fft") * own_count, own_count)

    def one_partner(member, running):
        single = lax.dynamic_slice_in_dim(own_grids, member, 1, 0)
        kernel = kernel_block(lax.dynamic_slice_in_dim(qvectors, member, 1, 0), extent, extent)
        density = times_conj(single, full_orbitals)
        spectrum = (
            along_axis(
                along_axis(along_last(density, forward_last), forward_mid, 2), forward_mid, 1
            )
            * kernel
        )
        field = along_last(
            along_axis(along_axis(spectrum, inverse_mid, 1), inverse_mid, 2), inverse_last
        )
        return running + times(single, field)

    partial_value = lax.fori_loop(
        0, own_count, one_partner, jnp.zeros(full_orbitals.shape, jnp.float32)
    )
    potential = lax.psum_scatter(partial_value, "fft", scatter_dimension=1, tiled=True)
    every_pot = lax.all_gather(potential, "band", axis=0, tiled=True)
    turned = rotate(every_pot)
    total_bands = every_pot.shape[0]
    flat_orbitals = orbitals.reshape(band_count, -1)
    flat_pot = every_pot.reshape(total_bands, -1)
    flat_turned = turned.reshape(total_bands, -1)
    volume = float(extent**3)
    rows_real = jnp.einsum("ik,jk->ij", flat_orbitals, flat_pot, precision=HIGHEST) / volume
    rows_imag = jnp.einsum("ik,jk->ij", flat_orbitals, flat_turned, precision=HIGHEST) / volume
    start_row = my_band * band_count
    summed_real, summed_imag = lax.psum((rows_real, rows_imag), "fft")
    over_real, over_imag = (
        lax.all_gather(summed_real, "band", axis=0, tiled=True),
        lax.all_gather(summed_imag, "band", axis=0, tiled=True),
    )
    inv_real, inv_imag = factor_inverse(over_real, over_imag)
    coef_real = lax.dynamic_slice_in_dim(inv_real, start_row, band_count, 0)
    coef_imag = lax.dynamic_slice_in_dim(inv_imag, start_row, band_count, 0)
    projector = jnp.dot(coef_real, flat_pot, precision=HIGHEST) + jnp.dot(
        coef_imag, flat_turned, precision=HIGHEST
    )
    return (potential, projector.reshape(orbitals.shape))


def remote(source, target, send_sem, recv_sem, where):
    return pltpu.make_async_remote_copy(
        src_ref=source,
        dst_ref=target,
        send_sem=send_sem,
        recv_sem=recv_sem,
        device_id=where,
        device_id_type=MESH,
    )


def greet(others):
    barrier = pltpu.get_barrier_semaphore()
    for other in others:
        pl.semaphore_signal(barrier, inc=1, device_id=other, device_id_type=MESH)
    pl.semaphore_wait(barrier, len(others))


def turn(block):
    lanes = block.shape[-1]
    swapped = pltpu.roll(block, lanes // 2, block.ndim - 1)
    position = lax.broadcasted_iota(jnp.int32, block.shape, block.ndim - 1)
    return jnp.where(position < lanes // 2, swapped, -swapped)


def small_factor_inverse(matrix):
    order = len(matrix)
    lower = [[None] * order for _ in range(order)]
    for column in range(order):
        residual = []
        for row in range(column, order):
            real, imag = matrix[row][column]
            for k in range(column):
                a, b = lower[row][k]
                c, d = lower[column][k]
                real = real - (a * c + b * d)
                imag = imag - (b * c - a * d)
            residual.append((real, imag))
        pivot = jnp.sqrt(residual[0][0])
        lower[column][column] = (pivot, jnp.zeros_like(pivot))
        for row in range(column + 1, order):
            real, imag = residual[row - column]
            lower[row][column] = (real / pivot, imag / pivot)
    inverse = [[None] * order for _ in range(order)]
    for row in range(order):
        pivot = lower[row][row][0]
        inverse[row][row] = (1.0 / pivot, jnp.zeros_like(pivot))
        for column in range(row):
            real = jnp.zeros_like(pivot)
            imag = jnp.zeros_like(pivot)
            for k in range(column, row):
                a, b = lower[row][k]
                c, d = inverse[k][column]
                real = real - (a * c - b * d)
                imag = imag - (a * d + b * c)
            inverse[row][column] = (real / pivot, imag / pivot)
    return inverse


def split_table(table):
    high = table.astype(jnp.bfloat16)
    low = (table - high.astype(np.float64)).astype(jnp.bfloat16)
    return high, low


def right_table(extent, sign):
    grid = np.outer(np.arange(extent), np.arange(extent)) % extent
    angle = 2.0 * math.pi / extent * grid
    cosine, sine = np.cos(angle), sign * np.sin(angle)
    table = np.block([[cosine, sine], [-sine, cosine]])
    high, low = split_table(table)
    upper = np.concatenate([high, low], axis=1)
    lower = np.concatenate([high, np.zeros_like(low)], axis=1)
    return np.concatenate([upper, lower], axis=0)


def left_table(extent, sign):
    grid = np.outer(np.arange(extent), np.arange(extent)) % extent
    angle = 2.0 * math.pi / extent * grid
    high, low = split_table(np.concatenate([np.cos(angle), sign * np.sin(angle)], axis=0))
    return np.concatenate([high, high, low], axis=1)


def halves(value):
    high = value.astype(jnp.bfloat16)
    low = (value - high.astype(jnp.float32)).astype(jnp.bfloat16)
    return high, low


def right_product(value, table):
    lanes = value.shape[-1]
    high, low = halves(value)
    both = jnp.dot(
        jnp.concatenate([high, low], axis=1), table, preferred_element_type=jnp.float32
    )
    return both[:, :lanes] + both[:, lanes:]


def left_product(first, second, table):
    rows, lanes = first.shape
    high, low = halves(jnp.concatenate([first, second], axis=1))
    stacked = jnp.concatenate([high, low, high], axis=0)
    both = jnp.dot(table, stacked, preferred_element_type=jnp.float32)
    return tuple(
        both[:rows, cut : cut + lanes] - turn(both[rows:, cut : cut + lanes])
        for cut in (0, lanes)
    )


def spread_parts(value):
    lanes = value.shape[-1]
    swapped = pltpu.roll(value, lanes // 2, value.ndim - 1)
    lower = lax.broadcasted_iota(jnp.int32, value.shape, value.ndim - 1) < lanes // 2
    return jnp.where(lower, value, swapped), jnp.where(lower, swapped, value)


def forward_group(group, orbital_grid, partner_grid, work, right, left):
    rows, lanes = orbital_grid.shape[1:]
    span = pl.ds(group * GROUP, GROUP)
    orbital = orbital_grid[span].reshape(GROUP * rows, lanes)
    real, imag = spread_parts(partner_grid[span].reshape(GROUP * rows, lanes))
    density = real * orbital + imag * turn(orbital)
    lines = right_product(density, right[...])
    planes = []
    for pair in range(GROUP // 2):
        start = 2 * pair * rows
        planes += left_product(
            lines[start : start + rows], lines[start + rows : start + 2 * rows], left[...]
        )
    stacked = jnp.stack(planes, axis=0)
    work[:, span, :] = jnp.swapaxes(stacked, 0, 1)


def backward_group(group, partner_grid, partial, work, right, left):
    rows, lanes = partner_grid.shape[1:]
    span = pl.ds(group * GROUP, GROUP)
    planes = jnp.swapaxes(work[:, span, :], 0, 1)
    lines = []
    for pair in range(GROUP // 2):
        lines += left_product(planes[2 * pair], planes[2 * pair + 1], left[...])
    field = right_product(jnp.concatenate(lines, axis=0), right[...])
    real, imag = spread_parts(partner_grid[span].reshape(GROUP * rows, lanes))
    partial[span] = (real * field - imag * turn(field)).reshape(GROUP, rows, lanes)


def fill_screen(shift, screen):
    columns, extent, lanes = screen.shape
    first = frequency(lax.broadcasted_iota(jnp.int32, (extent, lanes), 0), extent)
    third_place = lax.broadcasted_iota(jnp.int32, (extent, lanes), 1)
    third_place = jnp.where(third_place < lanes // 2, third_place, third_place - lanes // 2)
    third = frequency(third_place, extent)
    base = (first + shift[0]) ** 2 + (third + shift[2]) ** 2 + SCREEN_SQUARE
    scale = FOUR_PI / (float(extent) * float(columns) * float(lanes // 2))

    def one_column(column, carry):
        second = jnp.where(column < columns // 2, column, column - columns)
        offset = (second.astype(jnp.float32) + shift[1]) ** 2
        screen[column] = scale / (base + offset)
        return carry

    lax.fori_loop(0, columns, one_column, 0, unroll=2)


def middle_pairs(screen, work, forward, inverse):
    columns = work.shape[0]

    def one_pair(pair, carry):
        spectra = left_product(work[2 * pair], work[2 * pair + 1], forward[...])
        scaled = [spectra[which] * screen[2 * pair + which] for which in range(2)]
        fields = left_product(scaled[0], scaled[1], inverse[...])
        work[2 * pair] = fields[0]
        work[2 * pair + 1] = fields[1]
        return carry

    lax.fori_loop(0, columns // 2, one_pair, 0, unroll=32)


def exchange_kernel(
    bands,
    ranks,
    shift_table,
    shift_index,
    orbital_home,
    partner_home,
    right_forward_home,
    right_inverse_home,
    left_forward_home,
    left_inverse_home,
    potential,
    projector,
    orbital_grid,
    partner_grid,
    work,
    partial,
    partner,
    detour,
    near,
    outgoing,
    arriving,
    passed,
    others,
    tops,
    tallies,
    own_sums,
    all_sums,
    right_forward,
    right_inverse,
    left_forward,
    left_inverse,
    load_sem,
    gather_send,
    detour_send,
    detour_recv,
    onward_send,
    chain_send,
    partner_recv,
    grid_send,
    grid_recv,
    other_send,
    other_recv,
    third_send,
    third_recv,
    top_send,
    top_recv,
    near_send,
    near_recv,
    far_send,
    far_recv,
    up_send,
    up_recv,
    sum_send,
    sum_recv,
):
    planes, rows, lanes = potential.shape
    chunks = bands
    piece = planes // chunks
    per_group = GROUP // piece
    halves_count = planes // GROUP
    last = bands - 1
    cuts = 2 * chunks
    slice_size = planes // cuts
    direct = 4 * cuts // 8
    lag = cuts // 4
    held_back = 2 * cuts // 8
    top = 4 * cuts // 8
    split = (cuts - top) * slice_size
    band = lax.axis_index("band")
    rank = lax.axis_index("fft")
    beside = rank + 1 - 2 * (rank % 2)
    across = (rank + 2) % ranks
    beside_across = (beside + 2) % ranks
    slabs = (rank, beside, across, beside_across)
    home = 2 * (rank % 2) + (rank // 2 + rank % 2) % 2
    keeper = 2 * ((band // 2 + band % 2) % 2) + band // 2

    def both(*conditions):
        return functools.reduce(jnp.logical_and, conditions)

    def either(*conditions):
        return functools.reduce(jnp.logical_or, conditions)

    at_home = band == home
    at_end = either(band == 0, band == last)
    early = either(at_home, band == 1, band == last - 1)
    low_side = rank < ranks // 2
    takes_detour = both(at_end, low_side)
    gives_detour = both(jnp.logical_not(at_end), low_side)

    def span(index):
        return pl.ds(index * piece, piece)

    def cut_span(cut):
        return pl.ds(cut * slice_size, slice_size)

    def slab(index):
        return pl.ds(index * planes, planes)

    def window(index, chunk):
        return pl.ds(index * planes + chunk * piece, piece)

    own_slab = pltpu.make_async_copy(orbital_home, orbital_grid.at[slab(rank)], load_sem.at[1])
    partner_load = pltpu.make_async_copy(partner_home, partner, load_sem.at[0])
    home_load = pltpu.make_async_copy(partner_home, partner_grid.at[slab(rank)], load_sem.at[2])
    table_loads = [
        pltpu.make_async_copy(source, here, load_sem.at[3 + number])
        for number, (source, here) in enumerate(
            (
                (right_forward_home, right_forward),
                (left_forward_home, left_forward),
                (right_inverse_home, right_inverse),
                (left_inverse_home, left_inverse),
            )
        )
    ]
    partner_load.start()

    @pl.when(at_home)
    def _():
        home_load.start()

    own_slab.start()
    for load in table_loads:
        load.start()
    greet(
        [
            {"band": (band + step) % bands, "fft": (rank + turn_by) % ranks}
            for step in range(bands)
            for turn_by in range(ranks)
            if step or turn_by
        ]
    )

    def gather_copy(chunk):
        return remote(
            partner.at[span(chunk)],
            partner_grid.at[window(rank, chunk)],
            gather_send.at[chunk],
            partner_recv.at[rank, chunk],
            {"fft": keeper},
        )

    def detour_copy(chunk):
        return remote(
            partner.at[span(chunk)],
            detour.at[chunk],
            detour_send.at[chunk],
            detour_recv.at[chunk],
            {"band": last * (band - 1)},
        )

    def onward_copy(chunk):
        return remote(
            detour.at[chunk],
            partner_grid.at[window(rank, chunk)],
            onward_send.at[chunk],
            partner_recv.at[rank, chunk],
            {"fft": ranks // 2 + band // last},
        )

    def chain_copy(way, turn_to, chunk):
        place = partner_grid.at[window(slabs[turn_to], chunk)]
        return remote(
            place,
            place,
            chain_send.at[way, turn_to, chunk],
            partner_recv.at[slabs[turn_to], chunk],
            {"band": band + 1 - 2 * way},
        )

    def passes(way, turn_to):
        if way == 0:
            go = both(band >= home, band < last)
            short = both(band == last - 1, rank == ranks - 1)
        else:
            go = both(band <= home, band > 0)
            short = both(band == 1, rank == ranks // 2)
        return both(go, jnp.logical_not(short)) if turn_to > 1 else go

    def arrive(turn_to, chunk):
        def wait():
            chain_copy(0, turn_to, chunk).wait_recv()

        if turn_to:
            wait()
        else:
            pl.when(jnp.logical_not(at_home))(wait)

    def step(turn_to, chunk):
        arrive(turn_to, chunk)
        for way in (0, 1):

            @pl.when(passes(way, turn_to))
            def _():
                chain_copy(way, turn_to, chunk).start()

    tail = [(turn_to, half) for half in range(halves_count) for turn_to in (2, 3)]

    def of_half(half):
        return range(half * per_group, (half + 1) * per_group)

    partner_load.wait()
    for chunk in range(chunks):

        @pl.when(jnp.logical_not(at_home))
        def _():
            gather_copy(chunk).start()

        @pl.when(gives_detour)
        def _():
            detour_copy(chunk).start()

    @pl.when(at_home)
    def _():
        home_load.wait()

    own_slab.wait()
    own_orbital = orbital_grid.at[slab(rank)]
    to_across = remote(own_orbital, own_orbital, grid_send.at[0], grid_recv.at[0], {"fft": across})
    to_beside = remote(own_orbital, own_orbital, grid_send.at[1], grid_recv.at[1], {"fft": beside})
    other_orbital = orbital_grid.at[slab(across)]
    onward = remote(
        other_orbital, other_orbital, grid_send.at[2], grid_recv.at[2], {"fft": beside}
    )
    to_across.start()
    to_beside.start()

    def take_detour(condition, chunk):
        @pl.when(both(takes_detour, condition))
        def _():
            detour_copy(chunk).wait_recv()
            onward_copy(chunk).start()

    for turn_to in (0, 1):
        for chunk in range(chunks):
            step(turn_to, chunk)
            if turn_to == 1:
                take_detour(jnp.logical_not(at_home), chunk)

    def other_copy(slot, where, source=own_orbital):
        return remote(
            source,
            others.at[slot],
            other_send.at[slot, where],
            other_recv.at[slot],
            {"band": where},
        )

    def third_copy(number):
        place = pl.ds(split, planes - split) if number == 0 else pl.ds(0, split)
        held = others.at[1, place]
        return remote(
            held, held, third_send.at[number], third_recv.at[number], {"band": 1}
        )

    def top_copy(member):
        rest = pl.ds(split, planes - split)
        source = (
            orbital_grid.at[pl.ds(rank * planes + split, planes - split)]
            if member == 0
            else others.at[member - 1, rest]
        )
        return remote(
            source,
            tops.at[member],
            top_send.at[member],
            top_recv.at[member],
            {"band": 0},
        )

    def forward(group):
        forward_group(group, orbital_grid, partner_grid, work, right_forward, left_forward)

    def forward_near(index):
        forward(
            (rank + index // halves_count * (beside - rank)) * halves_count + index % halves_count
        )

    def tabulate():
        chosen = shift_index[home]
        fill_screen([shift_table[axis, chosen] for axis in range(3)], partial)

    for load in table_loads:
        load.wait()
    to_beside.wait_recv()

    @pl.when(early)
    def _():
        for number, (turn_to, half) in enumerate(tail):
            for chunk in of_half(half):
                if turn_to == 2:
                    take_detour(at_home, chunk)
            if number == len(tail) - 2:

                @pl.when(jnp.logical_not(at_home))
                def _():
                    to_across.wait_recv()
                    onward.start()

            for chunk in of_half(half):
                step(turn_to, chunk)
            forward_near(number)
            if number == 1:
                tabulate()

    @pl.when(band == 2)
    def _():
        other_copy(0, 1).start()

    @pl.when(band == last)
    def _():
        other_copy(1, 2).start()

    @pl.when(either(at_home, at_end))
    def _():
        to_across.wait_recv()
        onward.start()

    @pl.when(jnp.logical_not(early))
    def _():
        def one_group(index, carry):
            forward_near(index)
            return carry

        lax.fori_loop(0, 2 * halves_count, one_group, 0)
        tabulate()

    onward.wait_recv()
    for turn_to, half in tail:

        @pl.when(jnp.logical_not(early))
        def _():
            for chunk in of_half(half):
                arrive(turn_to, chunk)

        forward(slabs[turn_to] * halves_count + half)

    middle_pairs(partial, work, left_forward, left_inverse)

    @pl.when(band == 2)
    def _():
        other_copy(1, 2).wait_recv()
        for number in range(2):
            third_copy(number).start()

    def backward(index, half):
        backward_group(
            index * halves_count + half, partner_grid, partial, work, right_inverse, left_inverse
        )

    def near_copy(which, index, half):
        return remote(
            partial.at[pl.ds(index * planes + half * GROUP, GROUP)],
            near.at[which, pl.ds(half * GROUP, GROUP)],
            near_send.at[which, half],
            near_recv.at[which, half],
            {"fft": beside},
        )

    def far_copy(cut):
        return remote(
            outgoing.at[cut_span(cut)],
            arriving.at[cut_span(cut)],
            far_send.at[cut],
            far_recv.at[cut],
            {"fft": across},
        )

    def up_copy(owner, cut, own=False):
        held = passed.at[owner, cut_span(cut)]
        return remote(
            potential.at[cut_span(cut)] if own else held,
            held,
            up_send.at[owner, cut],
            up_recv.at[owner, cut],
            {"band": band + 1},
        )

    def slice_of(index, cut):
        return pl.ds(index * planes + cut * slice_size, slice_size)

    per_half = cuts // halves_count
    def halves_of_cuts(half):
        return range(half * per_half, (half + 1) * per_half)

    def send_half(half):
        backward(beside_across, half)
        near_copy(1, beside_across, half).start()
        backward(across, half)
        near_copy(1, beside_across, half).wait_recv()
        for cut in halves_of_cuts(half):
            outgoing[cut_span(cut)] = partial[slice_of(across, cut)] + near[1, cut_span(cut)]
            far_copy(cut).start()
        backward(beside, half)
        near_copy(0, beside, half).start()

    zero = jnp.zeros((8, lanes), jnp.float32)
    for number in range(tallies.shape[0]):
        tallies[number] = zero

    def inner(pairs, right, start, stop):
        slots = [2 * slot + half for slot, _ in pairs for half in range(2)]

        def accumulate(plane, sums):
            straight = right(plane)
            sides = (straight, turn(straight))
            values = [left(plane) for _, left in pairs]
            return tuple(
                running
                + jnp.sum((values[n // 2] * sides[n % 2]).reshape(rows // 8, 8, lanes), axis=0)
                for n, running in enumerate(sums)
            )

        sums = lax.fori_loop(
            start,
            stop,
            accumulate,
            tuple(tallies[slot] for slot in slots),
            unroll=min(4, stop - start),
        )
        for slot, value in zip(slots, sums):
            tallies[slot] = value

    def own_potential(plane):
        return potential[plane]

    def first_potential(plane):
        return passed[0, plane]

    def own_values(plane):
        return orbital_grid[rank * planes + plane]

    def other_values(slot):
        return lambda plane: others[slot, plane]

    def finish(cut):
        far_copy(cut).wait_recv()
        potential[cut_span(cut)] = (
            partial[slice_of(rank, cut)] + near[0, cut_span(cut)]
        ) + arriving[cut_span(cut)]

        sends = band < last - 1 if cut >= direct else band < last

        @pl.when(both(sends, band > 0) if cut >= cuts - held_back else sends)
        def _():
            up_copy(band, cut, True).start()

        inner([(0, own_values)], own_potential, cut * slice_size, (cut + 1) * slice_size)
        if 0 <= cut - lag < direct:

            @pl.when(band == 2)
            def _():
                lift_on(1, cut - lag)

        if cut == cuts // 2:

            @pl.when(band == 1)
            def _():
                other_copy(0, 1).wait_recv()
                top_copy(1).start()

    def lift_on(member, cut):
        up_copy(member, cut).wait_recv()
        up_copy(member, cut).start()

    for half in range(halves_count):
        send_half(half)
        if half == 0:

            @pl.when(band == 1)
            def _():
                top_copy(0).start()

            backward(rank, half)
            near_copy(0, beside, half).wait_recv()
            continue
        for number, cut in enumerate(halves_of_cuts(half - 1)):
            finish(cut)
            if number == per_half // 2 - 1:
                backward(rank, half)
        near_copy(0, beside, half).wait_recv()
    for cut in halves_of_cuts(halves_count - 1):
        finish(cut)

    @pl.when(band == 1)
    def _():
        def pass_on(cut):
            up_copy(0, cut).wait_recv()
            up_copy(0, cut).start()

        def with_first(start, stop):
            inner(
                [(3, own_values), (4, other_values(0)), (5, other_values(1))],
                first_potential,
                start * slice_size,
                stop * slice_size,
            )

        third_copy(0).wait_recv()
        top_copy(2).start()
        for cut in range(per_half):
            pass_on(cut)
        third_copy(1).wait_recv()
        inner([(1, other_values(0)), (2, other_values(1))], own_potential, 0, planes)
        with_first(0, per_half)
        for cut in range(per_half, cuts - top):
            pass_on(cut)
            with_first(cut, cut + 1)

    @pl.when(band == 2)
    def _():
        inner([(2, other_values(1))], own_potential, 0, planes)

    @pl.when(band == 0)
    def _():
        for member in range(3):
            top_copy(member).wait_recv()
        inner(
            [
                (3 + member, lambda plane, member=member: tops[member, plane - split])
                for member in range(3)
            ],
            own_potential,
            split,
            planes,
        )

    entries = [(i, l) for i in range(bands) for l in range(i + 1)]
    places = (
        band * (band + 1) // 2 + band,
        entries.index((2, 1)),
        entries.index((last, 0)) + band,
        entries.index((1, 0)),
        entries.index((2, 0)),
        entries.index((last, 0)),
    )
    position = lax.broadcasted_iota(jnp.int32, (8, lanes), 1)
    packed = zero
    for slot, place in enumerate(places):
        for half in range(2):
            value = jnp.sum(tallies[2 * slot + half], axis=1, keepdims=True)
            packed = packed + jnp.where(position == 2 * place + half, value, 0.0)
    own_sums[...] = packed
    sum_copies = []
    for step_by in range(bands):
        for turn_by in range(ranks):
            if step_by == 0 and turn_by == 0:
                continue
            copy = remote(
                own_sums,
                all_sums.at[band, rank],
                sum_send.at[step_by, turn_by],
                sum_recv.at[step_by, turn_by],
                {"band": (band + step_by) % bands, "fft": (rank + turn_by) % ranks},
            )
            copy.start()
            sum_copies.append(copy)
    all_sums[band, rank] = packed

    @pl.when(band == 0)
    def _():
        for cut in range(cuts - held_back, cuts):
            up_copy(0, cut, True).start()

    @pl.when(band == 1)
    def _():
        for cut in range(cuts - top, cuts):
            up_copy(0, cut).wait_recv()
            up_copy(0, cut).start()

    @pl.when(band == 2)
    def _():
        for cut in range(cuts - lag, direct):
            lift_on(1, cut)
        for cut in range(direct):
            lift_on(0, cut)

    for chunk in range(chunks):

        @pl.when(jnp.logical_not(at_home))
        def _():
            gather_copy(chunk).wait_send()

        @pl.when(gives_detour)
        def _():
            detour_copy(chunk).wait_send()

        @pl.when(takes_detour)
        def _():
            onward_copy(chunk).wait_send()

        for turn_to in range(len(slabs)):
            for way in (0, 1):

                @pl.when(passes(way, turn_to))
                def _():
                    chain_copy(way, turn_to, chunk).wait_send()

    @pl.when(band == 2)
    def _():
        other_copy(0, 1).wait_send()
        for number in range(2):
            third_copy(number).wait_send()

    @pl.when(band == 1)
    def _():
        for member in range(3):
            top_copy(member).wait_send()

    @pl.when(band == last)
    def _():
        other_copy(1, 2).wait_send()

    for half in range(halves_count):
        near_copy(0, beside, half).wait_send()
        near_copy(1, beside_across, half).wait_send()
    to_across.wait_send()
    to_beside.wait_send()
    onward.wait_send()

    for cut in range(cuts):
        far_copy(cut).wait_send()

    for copy in sum_copies:
        copy.wait()
    total = zero
    for one_band in range(bands):
        for one_rank in range(ranks):
            total = total + all_sums[one_band, one_rank]
    total = jnp.broadcast_to(jnp.sum(total, axis=0, keepdims=True), (8, lanes))
    volume = float(lanes // 2) * float(rows) * float(planes * ranks)
    matrix = [[None] * bands for _ in range(bands)]
    for number, (i, l) in enumerate(entries):
        values = [
            jnp.broadcast_to(
                jnp.sum(jnp.where(position == 2 * number + half, total, 0.0), axis=1, keepdims=True),
                (8, lanes),
            )
            / volume
            for half in range(2)
        ]
        matrix[i][l] = (values[0], values[1])
    inverse = small_factor_inverse(matrix)

    def combine(row, own, members, start, stop, put):
        def one_plane(plane, carry):
            sum_straight = jnp.zeros((rows, lanes), jnp.float32)
            sum_turned = jnp.zeros((rows, lanes), jnp.float32)
            for m in members:
                block = potential[plane] if m is None else passed[m, plane]
                real, imag = inverse[row][own if m is None else m]
                sum_straight = sum_straight + real[:1] * block
                sum_turned = sum_turned + imag[:1] * block
            put(plane, sum_straight + turn(sum_turned))
            return carry

        lax.fori_loop(start, stop, one_plane, 0, unroll=min(4, stop - start))

    def put_whole(plane, value):
        projector[plane] = value

    def put_more(plane, value):
        projector[plane] = projector[plane] + value

    def put_lifted(plane, value):
        passed[2, plane] = value

    for row in range(2):

        @pl.when(band == row)
        def _():
            combine(row, row, [None, 0][: row + 1], 0, planes, put_whole)

    @pl.when(band == 2)
    def _():
        for cut in range(direct, cuts):
            up_copy(1, cut).wait_recv()
        for cut in range(direct, cuts):
            up_copy(0, cut).wait_recv()
            combine(
                last, 2, (0, 1, None), cut * slice_size, (cut + 1) * slice_size, put_lifted
            )
            up_copy(2, cut).start()
        combine(2, 2, (0, 1, None), 0, planes, put_whole)

    @pl.when(band == last)
    def _():
        for member in (2, 1):
            for cut in range(direct):
                up_copy(member, cut).wait_recv()
        combine(last, last, (1, 2, None), 0, direct * slice_size, put_whole)
        combine(last, last, (None,), direct * slice_size, planes, put_whole)
        for cut in range(direct):
            up_copy(0, cut).wait_recv()
            combine(last, last, (0,), cut * slice_size, (cut + 1) * slice_size, put_more)
        for cut in range(direct, cuts):
            up_copy(2, cut).wait_recv()
            projector[cut_span(cut)] = projector[cut_span(cut)] + passed[2, cut_span(cut)]

    for cut in range(cuts):
        @pl.when(band < last)
        def _():
            up_copy(band, cut, True).wait_send()

        if cut < direct:

            @pl.when(band == 2)
            def _():
                up_copy(1, cut).wait_send()

        @pl.when(band == 1 if cut >= direct else either(band == 1, band == 2))
        def _():
            up_copy(0, cut).wait_send()


def exchange(bands, ranks, orbital, partner, shift_table, shift_index):
    planes, rows, lanes = orbital.shape
    chunks = bands
    halves_count = planes // GROUP
    vmem = pl.BlockSpec(memory_space=pltpu.VMEM)
    smem = pl.BlockSpec(memory_space=pltpu.SMEM)
    out = pltpu.VMEM((planes, rows, lanes), jnp.float32)
    grid = pltpu.VMEM((ranks * planes, rows, lanes), jnp.float32)
    slab = pltpu.VMEM((planes, rows, lanes), jnp.float32)
    quarters = pltpu.VMEM((chunks, planes // chunks, rows, lanes), jnp.float32)

    def slab_list(count):
        return pltpu.VMEM((count, planes, rows, lanes), jnp.float32)

    dma = pltpu.SemaphoreType.DMA
    tables = [
        jnp.asarray(table)
        for table in (
            right_table(rows, -1.0),
            right_table(rows, 1.0),
            left_table(rows, -1.0),
            left_table(rows, 1.0),
        )
    ]
    return pl.pallas_call(
        functools.partial(exchange_kernel, bands, ranks),
        name="exchange",
        out_shape=(out, out),
        in_specs=[smem, smem] + [pl.BlockSpec(memory_space=pl.ANY)] * 6,
        out_specs=(vmem, vmem),
        scratch_shapes=[
            grid,
            grid,
            grid,
            grid,
            slab,
            quarters,
            slab_list(2),
            slab,
            slab,
            slab_list(bands - 1),
            slab_list(2),
            pltpu.VMEM((3, 4 * (planes // (2 * chunks)), rows, lanes), jnp.float32),
            pltpu.VMEM((12, 8, lanes), jnp.float32),
            pltpu.VMEM((8, lanes), jnp.float32),
            pltpu.VMEM((bands, ranks, 8, lanes), jnp.float32),
        ]
        + [pltpu.VMEM(table.shape, table.dtype) for table in tables]
        + [
            dma((7,)),
            dma((chunks,)),
            dma((chunks,)),
            dma((chunks,)),
            dma((chunks,)),
            dma((2, ranks, chunks)),
            dma((ranks, chunks)),
            dma((3,)),
            dma((3,)),
            dma((2, bands)),
            dma((2,)),
            dma((2,)),
            dma((2,)),
            dma((3,)),
            dma((3,)),
            dma((2, halves_count)),
            dma((2, halves_count)),
            dma((2 * chunks,)),
            dma((2 * chunks,)),
            dma((bands, 2 * chunks)),
            dma((bands, 2 * chunks)),
            dma((bands, ranks)),
            dma((bands, ranks)),
        ],
        compiler_params=pltpu.CompilerParams(
            collective_id=0, has_side_effects=True, vmem_limit_bytes=60 * 1024 * 1024
        ),
    )(shift_table.T, shift_index, orbital, partner, *tables)


def settle_kernel(potential, projector, potential_home, projector_home, sem):
    copies = [
        pltpu.make_async_copy(here, home, sem.at[number])
        for number, (here, home) in enumerate(
            ((potential, potential_home), (projector, projector_home))
        )
    ]
    for copy in copies:
        copy.start()
    for copy in copies:
        copy.wait()


def settle(potential, projector):
    out = jax.ShapeDtypeStruct(potential.shape, jnp.float32)
    return pl.pallas_call(
        settle_kernel,
        name="settle",
        out_shape=(out, out),
        in_specs=[pl.BlockSpec(memory_space=pltpu.VMEM)] * 2,
        out_specs=(pl.BlockSpec(memory_space=pl.ANY),) * 2,
        scratch_shapes=[pltpu.SemaphoreType.DMA((2,))],
    )(*[pltpu.with_memory_space_constraint(value, pltpu.VMEM) for value in (potential, projector)])


def paired_body(bands, ranks, orbitals, partners, shift_table, shift_index):
    potential, projector = settle(
        *exchange(bands, ranks, orbitals[0], partners[0], shift_table, shift_index)
    )
    return (potential[None], projector[None])


def body(orbitals, partners, shift_table, shift_index):
    bands = lax.axis_size("band")
    ranks = lax.axis_size("fft")
    count, planes, rows, lanes = orbitals.shape
    grid_bytes = ranks * planes * rows * lanes * 4
    paired = (
        count == 1
        and ranks == 4
        and bands == ranks
        and planes % (2 * bands) == 0
        and planes % GROUP == 0
        and GROUP % (planes // bands) == 0
        and lanes == 2 * rows
        and lanes == 128
        and grid_bytes <= 2 * 1024 * 1024
    )
    if paired:
        return paired_body(bands, ranks, orbitals, partners, shift_table, shift_index)
    return general_body(orbitals, partners, shift_table, shift_index)


def solution(mesh):
    in_specs = (
        P(("kgrp", "band"), "fft", None, None),
        P(("kgrp", "band"), "fft", None, None),
        P(),
        P("kgrp"),
    )
    out_specs = (P(("kgrp", "band"), "fft", None, None), P(("kgrp", "band"), "fft", None, None))
    return jax.shard_map(body, mesh=mesh, in_specs=in_specs, out_specs=out_specs, check_vma=False)
```

```python
import functools
import math

import jax
import jax.numpy as jnp
import numpy as np
from jax import lax
from jax.experimental import pallas as pl
from jax.experimental.pallas import tpu as pltpu
from jax.sharding import PartitionSpec as P

HIGHEST = lax.Precision.HIGHEST
HIGH = lax.Precision.HIGH
MESH = pl.DeviceIdType.MESH
GROUP = 8
SCREEN_SQUARE = 0.25
FOUR_PI = 4.0 * math.pi


def angle_pair(extent, sign):
    positions = jnp.arange(extent, dtype=jnp.int32)
    product = positions[:, None] * positions[None, :] % extent
    angle = 2.0 * math.pi / extent * product.astype(jnp.float32)
    return (jnp.cos(angle), sign * jnp.sin(angle))


def last_table(extent, sign):
    cosine, sine = angle_pair(extent, sign)
    upper = jnp.concatenate([cosine, sine], axis=1)
    lower = jnp.concatenate([-sine, cosine], axis=1)
    return jnp.concatenate([upper, lower], axis=0)


def middle_table(extent, sign):
    cosine, sine = angle_pair(extent, sign)
    return jnp.stack([jnp.stack([cosine, -sine], -1), jnp.stack([sine, cosine], -1)], 1)


def along_last(field, table):
    shape = field.shape
    flat = field.reshape(-1, shape[-1])
    return jnp.dot(flat, table, precision=HIGH).reshape(shape)


def along_axis(field, table, axis_number):
    shape = field.shape
    extent = shape[-1] // 2
    split = field.reshape(shape[0], shape[1], shape[2], 2, extent)
    if axis_number == 1:
        result = jnp.einsum("kcnd,pnbdz->pkbcz", table, split, precision=HIGH)
    else:
        result = jnp.einsum("kcnd,pandz->pakcz", table, split, precision=HIGH)
    return result.reshape(shape)


def times_conj(left, right):
    extent = left.shape[-1] // 2
    left_real, left_imag = (left[..., :extent], left[..., extent:])
    right_real, right_imag = (right[..., :extent], right[..., extent:])
    return jnp.concatenate(
        [
            left_real * right_real + left_imag * right_imag,
            left_real * right_imag - left_imag * right_real,
        ],
        axis=-1,
    )


def times(left, right):
    extent = left.shape[-1] // 2
    left_real, left_imag = (left[..., :extent], left[..., extent:])
    right_real, right_imag = (right[..., :extent], right[..., extent:])
    return jnp.concatenate(
        [
            left_real * right_real - left_imag * right_imag,
            left_real * right_imag + left_imag * right_real,
        ],
        axis=-1,
    )


def rotate(field):
    extent = field.shape[-1] // 2
    return jnp.concatenate([field[..., extent:], -field[..., :extent]], axis=-1)


def frequency(positions, extent):
    return jnp.where(positions < extent // 2, positions, positions - extent).astype(jnp.float32)


def kernel_block(qvectors, y_count, extent):
    first_freq = frequency(jnp.arange(extent, dtype=jnp.int32), extent)
    second_freq = frequency(jnp.arange(y_count, dtype=jnp.int32), extent)
    third_freq = frequency(jnp.arange(2 * extent, dtype=jnp.int32) % extent, extent)
    first_part = (first_freq[None, :] + qvectors[:, 0:1]) ** 2
    second_part = (second_freq[None, :] + qvectors[:, 1:2]) ** 2
    third_part = (third_freq[None, :] + qvectors[:, 2:3]) ** 2
    denominator = (
        first_part[:, :, None, None]
        + second_part[:, None, :, None]
        + third_part[:, None, None, :]
        + SCREEN_SQUARE
    )
    return FOUR_PI / extent**3 / denominator


def shifts_for(shift_table, shift_index, start_at, length):
    picked = lax.dynamic_slice_in_dim(shift_index, start_at, length)
    onehot = (picked[:, None] == jnp.arange(shift_table.shape[0], dtype=jnp.int32)[None, :]).astype(
        jnp.float32
    )
    return jnp.dot(onehot, shift_table, precision=HIGHEST)


def factor_inverse(over_real, over_imag):
    matrix_order = over_real.shape[0]
    positions = jnp.arange(matrix_order, dtype=jnp.int32)
    zero_start = jnp.zeros_like(over_real)

    def chol_step(column, lowers):
        lower_real, lower_imag = lowers
        row_real = lower_real[column]
        row_imag = lower_imag[column]
        resid_real = over_real[:, column] - (
            jnp.dot(lower_real, row_real, precision=HIGHEST)
            + jnp.dot(lower_imag, row_imag, precision=HIGHEST)
        )
        resid_imag = over_imag[:, column] - (
            jnp.dot(lower_imag, row_real, precision=HIGHEST)
            - jnp.dot(lower_real, row_imag, precision=HIGHEST)
        )
        pivot_value = jnp.sqrt(resid_real[column])
        below_diag = positions > column
        at_diag = positions == column
        new_real = jnp.where(
            below_diag, resid_real / pivot_value, jnp.where(at_diag, pivot_value, 0.0)
        )
        new_imag = jnp.where(below_diag, resid_imag / pivot_value, 0.0)
        chosen = positions[None, :] == column
        return (
            jnp.where(chosen, new_real[:, None], lower_real),
            jnp.where(chosen, new_imag[:, None], lower_imag),
        )

    lower_real, lower_imag = lax.fori_loop(0, matrix_order, chol_step, (zero_start, zero_start))

    def solve_step(row_index, inverses):
        inv_real, inv_imag = inverses
        row_real = lower_real[row_index]
        row_imag = lower_imag[row_index]
        sum_real = jnp.dot(row_real, inv_real, precision=HIGHEST) - jnp.dot(
            row_imag, inv_imag, precision=HIGHEST
        )
        sum_imag = jnp.dot(row_real, inv_imag, precision=HIGHEST) + jnp.dot(
            row_imag, inv_real, precision=HIGHEST
        )
        unit_row = (positions == row_index).astype(over_real.dtype)
        pivot_value = lower_real[row_index, row_index]
        new_real = (unit_row - sum_real) / pivot_value
        new_imag = -sum_imag / pivot_value
        chosen = positions[:, None] == row_index
        return (
            jnp.where(chosen, new_real[None, :], inv_real),
            jnp.where(chosen, new_imag[None, :], inv_imag),
        )

    return lax.fori_loop(0, matrix_order, solve_step, (zero_start, zero_start))


def general_body(orbitals, partners, shift_table, shift_index):
    extent = orbitals.shape[2]
    band_count = orbitals.shape[0]
    tables = (
        last_table(extent, -1.0),
        middle_table(extent, -1.0),
        last_table(extent, 1.0),
        middle_table(extent, 1.0),
    )
    my_band = lax.axis_index("band")
    forward_last, forward_mid, inverse_last, inverse_mid = tables
    full_orbitals = lax.all_gather(orbitals, "fft", axis=1, tiled=True)
    every_slab = lax.all_gather(partners, "band", axis=0, tiled=True)
    own_grids = lax.all_to_all(every_slab, "fft", split_axis=0, concat_axis=1, tiled=True)
    own_count = own_grids.shape[0]
    qvectors = shifts_for(shift_table, shift_index, lax.axis_index("fft") * own_count, own_count)

    def one_partner(member, running):
        single = lax.dynamic_slice_in_dim(own_grids, member, 1, 0)
        kernel = kernel_block(lax.dynamic_slice_in_dim(qvectors, member, 1, 0), extent, extent)
        density = times_conj(single, full_orbitals)
        spectrum = (
            along_axis(
                along_axis(along_last(density, forward_last), forward_mid, 2), forward_mid, 1
            )
            * kernel
        )
        field = along_last(
            along_axis(along_axis(spectrum, inverse_mid, 1), inverse_mid, 2), inverse_last
        )
        return running + times(single, field)

    partial_value = lax.fori_loop(
        0, own_count, one_partner, jnp.zeros(full_orbitals.shape, jnp.float32)
    )
    potential = lax.psum_scatter(partial_value, "fft", scatter_dimension=1, tiled=True)
    every_pot = lax.all_gather(potential, "band", axis=0, tiled=True)
    turned = rotate(every_pot)
    total_bands = every_pot.shape[0]
    flat_orbitals = orbitals.reshape(band_count, -1)
    flat_pot = every_pot.reshape(total_bands, -1)
    flat_turned = turned.reshape(total_bands, -1)
    volume = float(extent**3)
    rows_real = jnp.einsum("ik,jk->ij", flat_orbitals, flat_pot, precision=HIGHEST) / volume
    rows_imag = jnp.einsum("ik,jk->ij", flat_orbitals, flat_turned, precision=HIGHEST) / volume
    start_row = my_band * band_count
    summed_real, summed_imag = lax.psum((rows_real, rows_imag), "fft")
    over_real, over_imag = (
        lax.all_gather(summed_real, "band", axis=0, tiled=True),
        lax.all_gather(summed_imag, "band", axis=0, tiled=True),
    )
    inv_real, inv_imag = factor_inverse(over_real, over_imag)
    coef_real = lax.dynamic_slice_in_dim(inv_real, start_row, band_count, 0)
    coef_imag = lax.dynamic_slice_in_dim(inv_imag, start_row, band_count, 0)
    projector = jnp.dot(coef_real, flat_pot, precision=HIGHEST) + jnp.dot(
        coef_imag, flat_turned, precision=HIGHEST
    )
    return (potential, projector.reshape(orbitals.shape))


def remote(source, target, send_sem, recv_sem, where):
    return pltpu.make_async_remote_copy(
        src_ref=source,
        dst_ref=target,
        send_sem=send_sem,
        recv_sem=recv_sem,
        device_id=where,
        device_id_type=MESH,
    )


def greet(others):
    barrier = pltpu.get_barrier_semaphore()
    for other in others:
        pl.semaphore_signal(barrier, inc=1, device_id=other, device_id_type=MESH)
    pl.semaphore_wait(barrier, len(others))


def turn(block):
    lanes = block.shape[-1]
    swapped = pltpu.roll(block, lanes // 2, block.ndim - 1)
    position = lax.broadcasted_iota(jnp.int32, block.shape, block.ndim - 1)
    return jnp.where(position < lanes // 2, swapped, -swapped)


def small_factor_inverse(matrix):
    order = len(matrix)
    lower = [[None] * order for _ in range(order)]
    for column in range(order):
        residual = []
        for row in range(column, order):
            real, imag = matrix[row][column]
            for k in range(column):
                a, b = lower[row][k]
                c, d = lower[column][k]
                real = real - (a * c + b * d)
                imag = imag - (b * c - a * d)
            residual.append((real, imag))
        pivot = jnp.sqrt(residual[0][0])
        lower[column][column] = (pivot, jnp.zeros_like(pivot))
        for row in range(column + 1, order):
            real, imag = residual[row - column]
            lower[row][column] = (real / pivot, imag / pivot)
    inverse = [[None] * order for _ in range(order)]
    for row in range(order):
        pivot = lower[row][row][0]
        inverse[row][row] = (1.0 / pivot, jnp.zeros_like(pivot))
        for column in range(row):
            real = jnp.zeros_like(pivot)
            imag = jnp.zeros_like(pivot)
            for k in range(column, row):
                a, b = lower[row][k]
                c, d = inverse[k][column]
                real = real - (a * c - b * d)
                imag = imag - (a * d + b * c)
            inverse[row][column] = (real / pivot, imag / pivot)
    return inverse


def split_table(table):
    high = table.astype(jnp.bfloat16)
    low = (table - high.astype(np.float64)).astype(jnp.bfloat16)
    return high, low


def right_table(extent, sign):
    grid = np.outer(np.arange(extent), np.arange(extent)) % extent
    angle = 2.0 * math.pi / extent * grid
    cosine, sine = np.cos(angle), sign * np.sin(angle)
    table = np.block([[cosine, sine], [-sine, cosine]])
    high, low = split_table(table)
    upper = np.concatenate([high, low], axis=1)
    lower = np.concatenate([high, np.zeros_like(low)], axis=1)
    return np.concatenate([upper, lower], axis=0)


def left_table(extent, sign):
    grid = np.outer(np.arange(extent), np.arange(extent)) % extent
    angle = 2.0 * math.pi / extent * grid
    high, low = split_table(np.concatenate([np.cos(angle), sign * np.sin(angle)], axis=0))
    return np.concatenate([high, high, low], axis=1)


def halves(value):
    high = value.astype(jnp.bfloat16)
    low = (value - high.astype(jnp.float32)).astype(jnp.bfloat16)
    return high, low


def right_product(value, table):
    lanes = value.shape[-1]
    high, low = halves(value)
    both = jnp.dot(
        jnp.concatenate([high, low], axis=1), table, preferred_element_type=jnp.float32
    )
    return both[:, :lanes] + both[:, lanes:]


def left_product(first, second, table):
    rows, lanes = first.shape
    high, low = halves(jnp.concatenate([first, second], axis=1))
    stacked = jnp.concatenate([high, low, high], axis=0)
    both = jnp.dot(table, stacked, preferred_element_type=jnp.float32)
    return tuple(
        both[:rows, cut : cut + lanes] - turn(both[rows:, cut : cut + lanes])
        for cut in (0, lanes)
    )


def spread_parts(value):
    lanes = value.shape[-1]
    swapped = pltpu.roll(value, lanes // 2, value.ndim - 1)
    lower = lax.broadcasted_iota(jnp.int32, value.shape, value.ndim - 1) < lanes // 2
    return jnp.where(lower, value, swapped), jnp.where(lower, swapped, value)


def forward_group(group, orbital_grid, partner_grid, work, right, left):
    rows, lanes = orbital_grid.shape[1:]
    span = pl.ds(group * GROUP, GROUP)
    orbital = orbital_grid[span].reshape(GROUP * rows, lanes)
    real, imag = spread_parts(partner_grid[span].reshape(GROUP * rows, lanes))
    density = real * orbital + imag * turn(orbital)
    lines = right_product(density, right[...])
    planes = []
    for pair in range(GROUP // 2):
        start = 2 * pair * rows
        planes += left_product(
            lines[start : start + rows], lines[start + rows : start + 2 * rows], left[...]
        )
    stacked = jnp.stack(planes, axis=0)
    work[:, span, :] = jnp.swapaxes(stacked, 0, 1)


def backward_group(group, partner_grid, partial, work, right, left):
    rows, lanes = partner_grid.shape[1:]
    span = pl.ds(group * GROUP, GROUP)
    planes = jnp.swapaxes(work[:, span, :], 0, 1)
    lines = []
    for pair in range(GROUP // 2):
        lines += left_product(planes[2 * pair], planes[2 * pair + 1], left[...])
    field = right_product(jnp.concatenate(lines, axis=0), right[...])
    real, imag = spread_parts(partner_grid[span].reshape(GROUP * rows, lanes))
    partial[span] = (real * field - imag * turn(field)).reshape(GROUP, rows, lanes)


def fill_screen(shift, screen):
    columns, extent, lanes = screen.shape
    first = frequency(lax.broadcasted_iota(jnp.int32, (extent, lanes), 0), extent)
    third_place = lax.broadcasted_iota(jnp.int32, (extent, lanes), 1)
    third_place = jnp.where(third_place < lanes // 2, third_place, third_place - lanes // 2)
    third = frequency(third_place, extent)
    base = (first + shift[0]) ** 2 + (third + shift[2]) ** 2 + SCREEN_SQUARE
    scale = FOUR_PI / (float(extent) * float(columns) * float(lanes // 2))

    def one_column(column, carry):
        second = jnp.where(column < columns // 2, column, column - columns)
        offset = (second.astype(jnp.float32) + shift[1]) ** 2
        screen[column] = scale / (base + offset)
        return carry

    lax.fori_loop(0, columns, one_column, 0, unroll=2)


def middle_pairs(screen, work, forward, inverse):
    columns = work.shape[0]

    def one_pair(pair, carry):
        spectra = left_product(work[2 * pair], work[2 * pair + 1], forward[...])
        scaled = [spectra[which] * screen[2 * pair + which] for which in range(2)]
        fields = left_product(scaled[0], scaled[1], inverse[...])
        work[2 * pair] = fields[0]
        work[2 * pair + 1] = fields[1]
        return carry

    lax.fori_loop(0, columns // 2, one_pair, 0, unroll=32)


def exchange_kernel(
    bands,
    ranks,
    shift_table,
    shift_index,
    orbital_home,
    partner_home,
    right_forward_home,
    right_inverse_home,
    left_forward_home,
    left_inverse_home,
    potential,
    projector,
    orbital_grid,
    partner_grid,
    work,
    partial,
    partner,
    detour,
    near,
    outgoing,
    arriving,
    passed,
    others,
    tops,
    tallies,
    own_sums,
    all_sums,
    right_forward,
    right_inverse,
    left_forward,
    left_inverse,
    load_sem,
    gather_send,
    detour_send,
    detour_recv,
    onward_send,
    chain_send,
    partner_recv,
    grid_send,
    grid_recv,
    other_send,
    other_recv,
    third_send,
    third_recv,
    top_send,
    top_recv,
    near_send,
    near_recv,
    far_send,
    far_recv,
    up_send,
    up_recv,
    sum_send,
    sum_recv,
):
    planes, rows, lanes = potential.shape
    chunks = bands
    piece = planes // chunks
    per_group = GROUP // piece
    halves_count = planes // GROUP
    last = bands - 1
    cuts = 2 * chunks
    slice_size = planes // cuts
    direct = 4 * cuts // 8
    lag = cuts // 4
    held_back = 2 * cuts // 8
    top = 4 * cuts // 8
    split = (cuts - top) * slice_size
    band = lax.axis_index("band")
    rank = lax.axis_index("fft")
    beside = rank + 1 - 2 * (rank % 2)
    across = (rank + 2) % ranks
    beside_across = (beside + 2) % ranks
    slabs = (rank, beside, across, beside_across)
    home = 2 * (rank % 2) + (rank // 2 + rank % 2) % 2
    keeper = 2 * ((band // 2 + band % 2) % 2) + band // 2

    def both(*conditions):
        return functools.reduce(jnp.logical_and, conditions)

    def either(*conditions):
        return functools.reduce(jnp.logical_or, conditions)

    at_home = band == home
    at_end = either(band == 0, band == last)
    early = either(at_home, band == 1, band == last - 1)
    low_side = rank < ranks // 2
    takes_detour = both(at_end, low_side)
    gives_detour = both(jnp.logical_not(at_end), low_side)

    def span(index):
        return pl.ds(index * piece, piece)

    def cut_span(cut):
        return pl.ds(cut * slice_size, slice_size)

    def slab(index):
        return pl.ds(index * planes, planes)

    def window(index, chunk):
        return pl.ds(index * planes + chunk * piece, piece)

    own_slab = pltpu.make_async_copy(orbital_home, orbital_grid.at[slab(rank)], load_sem.at[1])
    partner_load = pltpu.make_async_copy(partner_home, partner, load_sem.at[0])
    home_load = pltpu.make_async_copy(partner_home, partner_grid.at[slab(rank)], load_sem.at[2])
    table_loads = [
        pltpu.make_async_copy(source, here, load_sem.at[3 + number])
        for number, (source, here) in enumerate(
            (
                (right_forward_home, right_forward),
                (left_forward_home, left_forward),
                (right_inverse_home, right_inverse),
                (left_inverse_home, left_inverse),
            )
        )
    ]
    partner_load.start()

    @pl.when(at_home)
    def _():
        home_load.start()

    own_slab.start()
    for load in table_loads:
        load.start()
    greet(
        [
            {"band": (band + step) % bands, "fft": (rank + turn_by) % ranks}
            for step in range(bands)
            for turn_by in range(ranks)
            if step or turn_by
        ]
    )

    def gather_copy(chunk):
        return remote(
            partner.at[span(chunk)],
            partner_grid.at[window(rank, chunk)],
            gather_send.at[chunk],
            partner_recv.at[rank, chunk],
            {"fft": keeper},
        )

    def detour_copy(chunk):
        return remote(
            partner.at[span(chunk)],
            detour.at[chunk],
            detour_send.at[chunk],
            detour_recv.at[chunk],
            {"band": last * (band - 1)},
        )

    def onward_copy(chunk):
        return remote(
            detour.at[chunk],
            partner_grid.at[window(rank, chunk)],
            onward_send.at[chunk],
            partner_recv.at[rank, chunk],
            {"fft": ranks // 2 + band // last},
        )

    def chain_copy(way, turn_to, chunk):
        place = partner_grid.at[window(slabs[turn_to], chunk)]
        return remote(
            place,
            place,
            chain_send.at[way, turn_to, chunk],
            partner_recv.at[slabs[turn_to], chunk],
            {"band": band + 1 - 2 * way},
        )

    def passes(way, turn_to):
        if way == 0:
            go = both(band >= home, band < last)
            short = both(band == last - 1, rank == ranks - 1)
        else:
            go = both(band <= home, band > 0)
            short = both(band == 1, rank == ranks // 2)
        return both(go, jnp.logical_not(short)) if turn_to > 1 else go

    def arrive(turn_to, chunk):
        def wait():
            chain_copy(0, turn_to, chunk).wait_recv()

        if turn_to:
            wait()
        else:
            pl.when(jnp.logical_not(at_home))(wait)

    def step(turn_to, chunk):
        arrive(turn_to, chunk)
        for way in (0, 1):

            @pl.when(passes(way, turn_to))
            def _():
                chain_copy(way, turn_to, chunk).start()

    tail = [(turn_to, half) for half in range(halves_count) for turn_to in (2, 3)]

    def of_half(half):
        return range(half * per_group, (half + 1) * per_group)

    own_slab.wait()
    own_orbital = orbital_grid.at[slab(rank)]
    to_across = remote(own_orbital, own_orbital, grid_send.at[0], grid_recv.at[0], {"fft": across})
    to_beside = remote(own_orbital, own_orbital, grid_send.at[1], grid_recv.at[1], {"fft": beside})
    other_orbital = orbital_grid.at[slab(across)]
    onward = remote(
        other_orbital, other_orbital, grid_send.at[2], grid_recv.at[2], {"fft": beside}
    )
    pl.when(jnp.logical_not(at_end))(to_across.start)
    partner_load.wait()
    for chunk in range(chunks):

        @pl.when(jnp.logical_not(at_home))
        def _():
            gather_copy(chunk).start()

        @pl.when(gives_detour)
        def _():
            detour_copy(chunk).start()

    @pl.when(at_home)
    def _():
        home_load.wait()

    pl.when(at_end)(to_across.start)
    to_beside.start()

    def take_detour(condition, chunk):
        @pl.when(both(takes_detour, condition))
        def _():
            detour_copy(chunk).wait_recv()
            onward_copy(chunk).start()

    for turn_to in (0, 1):
        for chunk in range(chunks):
            step(turn_to, chunk)
            if turn_to == 1:
                take_detour(jnp.logical_not(at_home), chunk)

    def other_copy(slot, where, source=own_orbital):
        return remote(
            source,
            others.at[slot],
            other_send.at[slot, where],
            other_recv.at[slot],
            {"band": where},
        )

    def third_copy(number):
        place = pl.ds(split, planes - split) if number == 0 else pl.ds(0, split)
        held = others.at[1, place]
        return remote(
            held, held, third_send.at[number], third_recv.at[number], {"band": 1}
        )

    def top_copy(member):
        rest = pl.ds(split, planes - split)
        source = (
            orbital_grid.at[pl.ds(rank * planes + split, planes - split)]
            if member == 0
            else others.at[member - 1, rest]
        )
        return remote(
            source,
            tops.at[member],
            top_send.at[member],
            top_recv.at[member],
            {"band": 0},
        )

    def forward(group):
        forward_group(group, orbital_grid, partner_grid, work, right_forward, left_forward)

    def forward_near(index):
        forward(
            (rank + index // halves_count * (beside - rank)) * halves_count + index % halves_count
        )

    def tabulate():
        chosen = shift_index[home]
        fill_screen([shift_table[axis, chosen] for axis in range(3)], partial)

    for load in table_loads:
        load.wait()
    to_beside.wait_recv()

    @pl.when(early)
    def _():
        for number, (turn_to, half) in enumerate(tail):
            for chunk in of_half(half):
                if turn_to == 2:
                    take_detour(at_home, chunk)
            if number == 0:

                @pl.when(jnp.logical_not(at_home))
                def _():
                    to_across.wait_recv()
                    onward.start()

            for chunk in of_half(half):
                step(turn_to, chunk)
            forward_near(number)
            if number == 1:
                tabulate()

    @pl.when(band == 2)
    def _():
        other_copy(0, 1).start()

    @pl.when(band == last)
    def _():
        other_copy(1, 2).start()

    @pl.when(either(at_home, at_end))
    def _():
        to_across.wait_recv()
        onward.start()

    @pl.when(jnp.logical_not(early))
    def _():
        def one_group(index, carry):
            forward_near(index)
            return carry

        lax.fori_loop(0, 2 * halves_count, one_group, 0)
        tabulate()

    onward.wait_recv()
    for turn_to, half in tail:

        @pl.when(jnp.logical_not(early))
        def _():
            for chunk in of_half(half):
                arrive(turn_to, chunk)

        forward(slabs[turn_to] * halves_count + half)

    middle_pairs(partial, work, left_forward, left_inverse)

    @pl.when(band == 2)
    def _():
        other_copy(1, 2).wait_recv()
        for number in range(2):
            third_copy(number).start()

    def backward(index, half):
        backward_group(
            index * halves_count + half, partner_grid, partial, work, right_inverse, left_inverse
        )

    def near_copy(which, index, half):
        return remote(
            partial.at[pl.ds(index * planes + half * GROUP, GROUP)],
            near.at[which, pl.ds(half * GROUP, GROUP)],
            near_send.at[which, half],
            near_recv.at[which, half],
            {"fft": beside},
        )

    def far_copy(cut):
        return remote(
            outgoing.at[cut_span(cut)],
            arriving.at[cut_span(cut)],
            far_send.at[cut],
            far_recv.at[cut],
            {"fft": across},
        )

    def up_copy(owner, cut, own=False):
        held = passed.at[owner, cut_span(cut)]
        return remote(
            potential.at[cut_span(cut)] if own else held,
            held,
            up_send.at[owner, cut],
            up_recv.at[owner, cut],
            {"band": band + 1},
        )

    def slice_of(index, cut):
        return pl.ds(index * planes + cut * slice_size, slice_size)

    per_half = cuts // halves_count
    def halves_of_cuts(half):
        return range(half * per_half, (half + 1) * per_half)

    def send_half(half):
        backward(beside_across, half)
        near_copy(1, beside_across, half).start()
        backward(across, half)
        near_copy(1, beside_across, half).wait_recv()
        for cut in halves_of_cuts(half):
            outgoing[cut_span(cut)] = partial[slice_of(across, cut)] + near[1, cut_span(cut)]
            far_copy(cut).start()
        backward(beside, half)
        near_copy(0, beside, half).start()

    zero = jnp.zeros((8, lanes), jnp.float32)
    for number in range(tallies.shape[0]):
        tallies[number] = zero

    def inner(pairs, right, start, stop):
        slots = [2 * slot + half for slot, _ in pairs for half in range(2)]

        def accumulate(plane, sums):
            straight = right(plane)
            sides = (straight, turn(straight))
            values = [left(plane) for _, left in pairs]
            return tuple(
                running
                + jnp.sum((values[n // 2] * sides[n % 2]).reshape(rows // 8, 8, lanes), axis=0)
                for n, running in enumerate(sums)
            )

        sums = lax.fori_loop(
            start,
            stop,
            accumulate,
            tuple(tallies[slot] for slot in slots),
            unroll=min(4, stop - start),
        )
        for slot, value in zip(slots, sums):
            tallies[slot] = value

    def own_potential(plane):
        return potential[plane]

    def first_potential(plane):
        return passed[0, plane]

    def own_values(plane):
        return orbital_grid[rank * planes + plane]

    def other_values(slot):
        return lambda plane: others[slot, plane]

    def finish(cut):
        far_copy(cut).wait_recv()
        potential[cut_span(cut)] = (
            partial[slice_of(rank, cut)] + near[0, cut_span(cut)]
        ) + arriving[cut_span(cut)]

        sends = band < last - 1 if cut >= direct else band < last

        @pl.when(both(sends, band > 0) if cut >= cuts - held_back else sends)
        def _():
            up_copy(band, cut, True).start()

        inner([(0, own_values)], own_potential, cut * slice_size, (cut + 1) * slice_size)
        if 0 <= cut - lag < direct:

            @pl.when(band == 2)
            def _():
                lift_on(1, cut - lag)

        if cut == cuts // 2:

            @pl.when(band == 1)
            def _():
                other_copy(0, 1).wait_recv()
                top_copy(1).start()

    def lift_on(member, cut):
        up_copy(member, cut).wait_recv()
        up_copy(member, cut).start()

    for half in range(halves_count):
        send_half(half)
        if half == 0:

            @pl.when(band == 1)
            def _():
                top_copy(0).start()

            backward(rank, half)
            near_copy(0, beside, half).wait_recv()
            continue
        for number, cut in enumerate(halves_of_cuts(half - 1)):
            finish(cut)
            if number == per_half // 2 - 1:
                backward(rank, half)
        near_copy(0, beside, half).wait_recv()
    for cut in halves_of_cuts(halves_count - 1):
        finish(cut)

    @pl.when(band == 1)
    def _():
        def pass_on(cut):
            up_copy(0, cut).wait_recv()
            up_copy(0, cut).start()

        def with_first(start, stop):
            inner(
                [(3, own_values), (4, other_values(0)), (5, other_values(1))],
                first_potential,
                start * slice_size,
                stop * slice_size,
            )

        third_copy(0).wait_recv()
        top_copy(2).start()
        for cut in range(per_half):
            pass_on(cut)
        third_copy(1).wait_recv()
        inner([(1, other_values(0)), (2, other_values(1))], own_potential, 0, planes)
        with_first(0, per_half)
        for cut in range(per_half, cuts - top):
            pass_on(cut)
            with_first(cut, cut + 1)

    @pl.when(band == 2)
    def _():
        inner([(2, other_values(1))], own_potential, 0, planes)

    @pl.when(band == 0)
    def _():
        for member in range(3):
            top_copy(member).wait_recv()
        inner(
            [
                (3 + member, lambda plane, member=member: tops[member, plane - split])
                for member in range(3)
            ],
            own_potential,
            split,
            planes,
        )

    entries = [(i, l) for i in range(bands) for l in range(i + 1)]
    places = (
        band * (band + 1) // 2 + band,
        entries.index((2, 1)),
        entries.index((last, 0)) + band,
        entries.index((1, 0)),
        entries.index((2, 0)),
        entries.index((last, 0)),
    )
    position = lax.broadcasted_iota(jnp.int32, (8, lanes), 1)
    packed = zero
    for slot, place in enumerate(places):
        for half in range(2):
            value = jnp.sum(tallies[2 * slot + half], axis=1, keepdims=True)
            packed = packed + jnp.where(position == 2 * place + half, value, 0.0)
    own_sums[...] = packed
    sum_copies = []
    for step_by in range(bands):
        for turn_by in range(ranks):
            if step_by == 0 and turn_by == 0:
                continue
            copy = remote(
                own_sums,
                all_sums.at[band, rank],
                sum_send.at[step_by, turn_by],
                sum_recv.at[step_by, turn_by],
                {"band": (band + step_by) % bands, "fft": (rank + turn_by) % ranks},
            )
            copy.start()
            sum_copies.append(copy)
    all_sums[band, rank] = packed

    @pl.when(band == 0)
    def _():
        for cut in range(cuts - held_back, cuts):
            up_copy(0, cut, True).start()

    @pl.when(band == 1)
    def _():
        for cut in range(cuts - top, cuts):
            up_copy(0, cut).wait_recv()
            up_copy(0, cut).start()

    @pl.when(band == 2)
    def _():
        for cut in range(cuts - lag, direct):
            lift_on(1, cut)
        for cut in range(direct):
            lift_on(0, cut)

    for chunk in range(chunks):

        @pl.when(jnp.logical_not(at_home))
        def _():
            gather_copy(chunk).wait_send()

        @pl.when(gives_detour)
        def _():
            detour_copy(chunk).wait_send()

        @pl.when(takes_detour)
        def _():
            onward_copy(chunk).wait_send()

        for turn_to in range(len(slabs)):
            for way in (0, 1):

                @pl.when(passes(way, turn_to))
                def _():
                    chain_copy(way, turn_to, chunk).wait_send()

    @pl.when(band == 2)
    def _():
        other_copy(0, 1).wait_send()
        for number in range(2):
            third_copy(number).wait_send()

    @pl.when(band == 1)
    def _():
        for member in range(3):
            top_copy(member).wait_send()

    @pl.when(band == last)
    def _():
        other_copy(1, 2).wait_send()

    for half in range(halves_count):
        near_copy(0, beside, half).wait_send()
        near_copy(1, beside_across, half).wait_send()
    to_across.wait_send()
    to_beside.wait_send()
    onward.wait_send()

    for cut in range(cuts):
        far_copy(cut).wait_send()

    for copy in sum_copies:
        copy.wait()
    total = zero
    for one_band in range(bands):
        for one_rank in range(ranks):
            total = total + all_sums[one_band, one_rank]
    total = jnp.broadcast_to(jnp.sum(total, axis=0, keepdims=True), (8, lanes))
    volume = float(lanes // 2) * float(rows) * float(planes * ranks)
    matrix = [[None] * bands for _ in range(bands)]
    for number, (i, l) in enumerate(entries):
        values = [
            jnp.broadcast_to(
                jnp.sum(jnp.where(position == 2 * number + half, total, 0.0), axis=1, keepdims=True),
                (8, lanes),
            )
            / volume
            for half in range(2)
        ]
        matrix[i][l] = (values[0], values[1])
    inverse = small_factor_inverse(matrix)

    def combine(row, own, members, start, stop, put):
        def one_plane(plane, carry):
            sum_straight = jnp.zeros((rows, lanes), jnp.float32)
            sum_turned = jnp.zeros((rows, lanes), jnp.float32)
            for m in members:
                block = potential[plane] if m is None else passed[m, plane]
                real, imag = inverse[row][own if m is None else m]
                sum_straight = sum_straight + real[:1] * block
                sum_turned = sum_turned + imag[:1] * block
            put(plane, sum_straight + turn(sum_turned))
            return carry

        lax.fori_loop(start, stop, one_plane, 0, unroll=min(4, stop - start))

    def put_whole(plane, value):
        projector[plane] = value

    def put_more(plane, value):
        projector[plane] = projector[plane] + value

    def put_lifted(plane, value):
        passed[2, plane] = value

    for row in range(2):

        @pl.when(band == row)
        def _():
            combine(row, row, [None, 0][: row + 1], 0, planes, put_whole)

    @pl.when(band == 2)
    def _():
        for cut in range(direct, cuts):
            up_copy(1, cut).wait_recv()
        for cut in range(direct, cuts):
            up_copy(0, cut).wait_recv()
            combine(
                last, 2, (0, 1, None), cut * slice_size, (cut + 1) * slice_size, put_lifted
            )
            up_copy(2, cut).start()
        combine(2, 2, (0, 1, None), 0, planes, put_whole)

    @pl.when(band == last)
    def _():
        for member in (2, 1):
            for cut in range(direct):
                up_copy(member, cut).wait_recv()
        combine(last, last, (1, 2, None), 0, direct * slice_size, put_whole)
        combine(last, last, (None,), direct * slice_size, planes, put_whole)
        for cut in range(direct):
            up_copy(0, cut).wait_recv()
            combine(last, last, (0,), cut * slice_size, (cut + 1) * slice_size, put_more)
        for cut in range(direct, cuts):
            up_copy(2, cut).wait_recv()
            projector[cut_span(cut)] = projector[cut_span(cut)] + passed[2, cut_span(cut)]

    for cut in range(cuts):
        @pl.when(band < last)
        def _():
            up_copy(band, cut, True).wait_send()

        if cut < direct:

            @pl.when(band == 2)
            def _():
                up_copy(1, cut).wait_send()

        @pl.when(band == 1 if cut >= direct else either(band == 1, band == 2))
        def _():
            up_copy(0, cut).wait_send()


def exchange(bands, ranks, orbital, partner, shift_table, shift_index):
    planes, rows, lanes = orbital.shape
    chunks = bands
    halves_count = planes // GROUP
    vmem = pl.BlockSpec(memory_space=pltpu.VMEM)
    smem = pl.BlockSpec(memory_space=pltpu.SMEM)
    out = pltpu.VMEM((planes, rows, lanes), jnp.float32)
    grid = pltpu.VMEM((ranks * planes, rows, lanes), jnp.float32)
    slab = pltpu.VMEM((planes, rows, lanes), jnp.float32)
    quarters = pltpu.VMEM((chunks, planes // chunks, rows, lanes), jnp.float32)

    def slab_list(count):
        return pltpu.VMEM((count, planes, rows, lanes), jnp.float32)

    dma = pltpu.SemaphoreType.DMA
    tables = [
        jnp.asarray(table)
        for table in (
            right_table(rows, -1.0),
            right_table(rows, 1.0),
            left_table(rows, -1.0),
            left_table(rows, 1.0),
        )
    ]
    return pl.pallas_call(
        functools.partial(exchange_kernel, bands, ranks),
        name="exchange",
        out_shape=(out, out),
        in_specs=[smem, smem] + [pl.BlockSpec(memory_space=pl.ANY)] * 6,
        out_specs=(vmem, vmem),
        scratch_shapes=[
            grid,
            grid,
            grid,
            grid,
            slab,
            quarters,
            slab_list(2),
            slab,
            slab,
            slab_list(bands - 1),
            slab_list(2),
            pltpu.VMEM((3, 4 * (planes // (2 * chunks)), rows, lanes), jnp.float32),
            pltpu.VMEM((12, 8, lanes), jnp.float32),
            pltpu.VMEM((8, lanes), jnp.float32),
            pltpu.VMEM((bands, ranks, 8, lanes), jnp.float32),
        ]
        + [pltpu.VMEM(table.shape, table.dtype) for table in tables]
        + [
            dma((7,)),
            dma((chunks,)),
            dma((chunks,)),
            dma((chunks,)),
            dma((chunks,)),
            dma((2, ranks, chunks)),
            dma((ranks, chunks)),
            dma((3,)),
            dma((3,)),
            dma((2, bands)),
            dma((2,)),
            dma((2,)),
            dma((2,)),
            dma((3,)),
            dma((3,)),
            dma((2, halves_count)),
            dma((2, halves_count)),
            dma((2 * chunks,)),
            dma((2 * chunks,)),
            dma((bands, 2 * chunks)),
            dma((bands, 2 * chunks)),
            dma((bands, ranks)),
            dma((bands, ranks)),
        ],
        compiler_params=pltpu.CompilerParams(
            collective_id=0, has_side_effects=True, vmem_limit_bytes=60 * 1024 * 1024
        ),
    )(shift_table.T, shift_index, orbital, partner, *tables)


def settle_kernel(potential, projector, potential_home, projector_home, sem):
    copies = [
        pltpu.make_async_copy(here, home, sem.at[number])
        for number, (here, home) in enumerate(
            ((potential, potential_home), (projector, projector_home))
        )
    ]
    for copy in copies:
        copy.start()
    for copy in copies:
        copy.wait()


def settle(potential, projector):
    out = jax.ShapeDtypeStruct(potential.shape, jnp.float32)
    return pl.pallas_call(
        settle_kernel,
        name="settle",
        out_shape=(out, out),
        in_specs=[pl.BlockSpec(memory_space=pltpu.VMEM)] * 2,
        out_specs=(pl.BlockSpec(memory_space=pl.ANY),) * 2,
        scratch_shapes=[pltpu.SemaphoreType.DMA((2,))],
    )(*[pltpu.with_memory_space_constraint(value, pltpu.VMEM) for value in (potential, projector)])


def paired_body(bands, ranks, orbitals, partners, shift_table, shift_index):
    potential, projector = settle(
        *exchange(bands, ranks, orbitals[0], partners[0], shift_table, shift_index)
    )
    return (potential[None], projector[None])


def body(orbitals, partners, shift_table, shift_index):
    bands = lax.axis_size("band")
    ranks = lax.axis_size("fft")
    count, planes, rows, lanes = orbitals.shape
    grid_bytes = ranks * planes * rows * lanes * 4
    paired = (
        count == 1
        and ranks == 4
        and bands == ranks
        and planes % (2 * bands) == 0
        and planes % GROUP == 0
        and GROUP % (planes // bands) == 0
        and lanes == 2 * rows
        and lanes == 128
        and grid_bytes <= 2 * 1024 * 1024
    )
    if paired:
        return paired_body(bands, ranks, orbitals, partners, shift_table, shift_index)
    return general_body(orbitals, partners, shift_table, shift_index)


def solution(mesh):
    in_specs = (
        P(("kgrp", "band"), "fft", None, None),
        P(("kgrp", "band"), "fft", None, None),
        P(),
        P("kgrp"),
    )
    out_specs = (P(("kgrp", "band"), "fft", None, None), P(("kgrp", "band"), "fft", None, None))
    return jax.shard_map(body, mesh=mesh, in_specs=in_specs, out_specs=out_specs, check_vma=False)
```
